256 devices in a mesh: grid: 128 (over x, y_hi, z, core), band: 2 (over y_lo).
Axes of the slice: x: 4, y: 4 (y_hi: 2, y_lo: 2; y = y_hi * 2 + y_lo), z: 8, core: 2. Of those that a mesh axis runs over, the one named last changes fastest.
Arguments:
- left_bands: float32 [2, 8, 128, 128, 128], P(None, 'band', 'grid'), may hold values from -6 to 6
- right_bands: float32 [2, 4, 128, 128, 128], P(None, 'band', 'grid'), may hold values from -6 to 6
- sphere_index: int32 [16384], replicated, may hold values from 0 to 2097151, as said below
- right_order: int32 [4], replicated, may hold values from 0 to 3, each once
Outputs:
- pair_density: float32 [2, 8, 4, 16384], P(None, 'band', None, 'grid')
The draws below stay inside these ranges and needn't reach their ends.
Inputs may be any that keep to these rules, and one draw needn't show every extreme that they name: `sphere_index`: flat index (kz * 128 + ky) * 128 + kx; an index may repeat. In each aligned block of 128 entries, at most 1 entries share one value of ky, and some value is shared by exactly 1. `right_order`: each second band once.
All inputs are finite; a program needn't handle non-finite values.
Results may differ from the reference program's by a relative error of at most 0.00008.
Values sent between devices are 32-bit elements; how exact they have to be, the bound alone decides.
A program may use at most 128 MiB of HBM per device.

```python
import jax
import jax.numpy as jnp
from jax import lax

NG = 128
NX = 128
NGV = 16384
NL = 8
NR = 4
ZS = 1


def draw_sphere_index(key, part):
    devices = NG // ZS
    per_block = NGV // devices
    key_shift = jax.random.fold_in(key, 11)
    key_perm = jax.random.fold_in(key, 12)
    key_row = jax.random.fold_in(key, 13)
    key_plane = jax.random.fold_in(key, 14)
    key_column = jax.random.fold_in(key, 15)
    shifts = jax.random.randint(key_shift, (devices, 1), 0, devices)
    position = jnp.arange(per_block, dtype=jnp.int32)[None, :]
    source = (position + shifts) % devices
    block_keys = jax.random.split(key_perm, devices)
    orders = jax.vmap(lambda k: jax.random.permutation(k, per_block))(block_keys)
    source = jnp.take_along_axis(source, orders.astype(jnp.int32), axis=1).reshape(-1)
    wave_y = source * ZS + jax.random.randint(key_row, (NGV,), 0, ZS)
    wave_z = jax.random.randint(key_plane, (NGV,), 0, NG)
    wave_x = jax.random.randint(key_column, (NGV,), 0, NX)
    return ((wave_z * NG + wave_y) * NX + wave_x).astype(jnp.int32)


def levels(stream_key, shape, shards, low, top_value):
    def one(dim, parts):
        draws = jax.random.uniform(jax.random.fold_in(jax.random.fold_in(stream_key, 6), dim), (parts,), jnp.float32, low / len(shards), top_value / len(shards))
        return jnp.repeat(jnp.exp(draws), shape[dim] // parts).reshape((-1,) + (1,) * (len(shape) - dim - 1))

    factor_of = one(*shards[0])
    for cut in shards[1:]:
        factor_of = factor_of * one(*cut)
    return factor_of


def normal_values(stream_key, dims, scale, reach, cuts=(), kind=jnp.bfloat16):
    array = jax.random.normal(stream_key, dims, jnp.float32) * scale
    if len(cuts) > 0:
        array = levels(stream_key, dims, cuts, -0.22, 0.18) * array
    return jnp.clip(array, min=-reach, max=reach).astype(kind)


def setup_inputs(seed: int = 0) -> dict:
    key_list = jax.random.split(jax.random.key(seed), 5)
    return {
        "left_bands": normal_values(key_list[0], (2, NL, NG, NG, NX), 1.0, 6.0, ((1, 2), (2, 128)), jnp.float32),
        "right_bands": normal_values(key_list[1], (2, NR, NG, NG, NX), 1.0, 6.0, ((1, 2), (2, 128)), jnp.float32),
        "sphere_index": draw_sphere_index(jax.random.fold_in(key_list[4], 71), 0),
        "right_order": jax.random.permutation(key_list[3], NR).astype(jnp.int32),
    }


def reference(left_bands, right_bands, sphere_index, right_order):
    factor = 1.0 / (NG * NG * NX) ** 0.5

    def one_left(left_field):
        def one_right(column):
            right_field = lax.dynamic_index_in_dim(right_bands, column, 1, keepdims=False)
            real_part = left_field[0] * right_field[0] + left_field[1] * right_field[1]
            imag_part = left_field[0] * right_field[1] - left_field[1] * right_field[0]
            spectrum = jnp.fft.fftn(real_part + 1j * imag_part)
            picked = spectrum.reshape(-1)[sphere_index]
            return jnp.stack([jnp.real(picked), jnp.imag(picked)]).astype(jnp.float32) * factor

        return lax.map(one_right, right_order)

    result = lax.map(one_left, jnp.moveaxis(left_bands, 1, 0))
    return jnp.transpose(result, (2, 0, 1, 3))
```

```python
import functools
import math

import jax
import jax.numpy as jnp
from jax import lax
from jax.experimental import pallas as pl
from jax.experimental.pallas import tpu as pltpu
from jax.sharding import PartitionSpec as P
import numpy as np

NG = 128
NX = 128
NGV = 16384
AX, AH, AZ, AC = 4, 2, 8, 2
SIDE = AH * AZ * AC
QUARTER = SIDE * 8
HALF = QUARTER // 2
MESH = pl.DeviceIdType.MESH
F32 = jnp.float32
BF16 = jnp.bfloat16


def split(value):
    high = value.astype(BF16)
    return high, (value - high.astype(F32)).astype(BF16)


def dft_tables():
    counter = np.arange(NG)
    angles = (counter[:, None] * counter[None, :] % NG) * (2.0 * math.pi / NG)
    cosine, sine = np.cos(angles), np.sin(angles)

    def halves(table):
        high = table.astype(np.float32).astype(BF16)
        low = (table - high.astype(np.float64)).astype(np.float32).astype(BF16)
        return high, low

    high, low = halves(np.block([[cosine, -sine], [sine, cosine]]))
    along_x = np.concatenate([high, high, low], axis=0)
    high, low = halves(np.block([[cosine, sine], [-sine, cosine]]))
    along_y = np.concatenate([high, low, high], axis=1)
    trig = np.zeros((8, NG), np.float32)
    trig[0], trig[1] = cosine[1], sine[1]
    return along_x, along_y, trig


def lanes(value, index):
    return jnp.take_along_axis(value, index, axis=1, mode="promise_in_bounds")


def kernel(
    left_ref, right_ref, sphere_ref, along_x_ref, along_y_ref, trig_ref, out_ref, row_ref,
    lefts, rights, own_right, sphere, along_x, along_y, trig,
    ky_t, val_t, kx_of, phase, acc, send, from_a, from_b, from_c, x_sum, tiles,
    load_sem, pair_send, pair_recv, y_send, y_recv, x_send, x_recv, z_send, z_recv,
):
    g = lax.axis_index("grid")
    b = lax.axis_index("band")
    c = lax.rem(g, AC)
    j = lax.rem(g, SIDE)
    x = lax.div(g, SIDE)
    up = lax.rem(x + 1, AX)
    down = lax.rem(x + AX - 1, AX)
    across = lax.rem(x + 2, AX)

    loads = [
        pltpu.make_async_copy(sphere_ref, sphere, load_sem.at[0]),
        pltpu.make_async_copy(trig_ref, trig, load_sem.at[1]),
        pltpu.make_async_copy(right_ref, own_right, load_sem.at[2]),
        pltpu.make_async_copy(left_ref, lefts.at[c], load_sem.at[3]),
        pltpu.make_async_copy(right_ref.at[:, c], rights.at[0, c], load_sem.at[4]),
        pltpu.make_async_copy(along_x_ref, along_x, load_sem.at[5]),
        pltpu.make_async_copy(along_y_ref, along_y, load_sem.at[6]),
    ]
    for load in loads:
        load.start()

    barrier = pltpu.get_barrier_semaphore()

    def greet(grid, band):
        pl.semaphore_signal(barrier, inc=1, device_id=(grid, band), device_id_type=MESH)

    greet(g - c, 1 - b)
    greet(g - c + 1, 1 - b)
    greet(up * SIDE + j, b)
    greet(down * SIDE + j, b)

    @pl.loop(1, SIDE)
    def _(step):
        greet(x * SIDE + lax.rem(j + step, SIDE), b)

    loads[0].wait()
    loads[1].wait()
    flipped = sphere[...].T
    ky_t[...] = (flipped >> 7) & 127
    val_t[...] = ((flipped >> 14) << 7) | (flipped & 127)
    rows = lax.broadcasted_iota(jnp.int32, (NG, NG), 0)

    def place(p, table):
        return jnp.where(ky_t[pl.ds(p, 1), :] == rows, val_t[pl.ds(p, 1), :], table)

    table = lax.fori_loop(0, NG, place, jnp.zeros((NG, NG), jnp.int32), unroll=8)
    kx_of[...] = table & 127
    kz = table >> 7
    cosine = jnp.broadcast_to(trig[0:1, :], (NG, NG))
    sine = jnp.broadcast_to(trig[1:2, :], (NG, NG))
    for core in range(2):
        angle = (kz * (g - c + core)) & 127
        phase[core, 0] = lanes(cosine, angle)
        phase[core, 1] = lanes(sine, angle)
    row_ref[...] = jnp.broadcast_to((sphere[pl.ds(g, 1), :] >> 7) & 127, (8, NG))

    def transform(chunk, plane, combine):
        right_real = rights[chunk, plane, 0]
        right_imag = rights[chunk, plane, 1]
        index = kx_of[...]
        for half in range(2):
            columns = []
            for n in (2 * half, 2 * half + 1):
                left_real = lefts[plane, 0, n]
                left_imag = lefts[plane, 1, n]
                field = jnp.concatenate(
                    [
                        left_real * right_real + left_imag * right_imag,
                        left_real * right_imag - left_imag * right_real,
                    ],
                    axis=1,
                )
                high, low = split(field)
                moved = jnp.dot(
                    jnp.concatenate([high, low, high], axis=1),
                    along_x[...],
                    preferred_element_type=F32,
                )
                columns.append(jnp.concatenate([moved[:, :NX], moved[:, NX:]], axis=0))
            high, low = split(jnp.concatenate(columns, axis=1))
            plane_waves = jnp.dot(
                along_y[...],
                jnp.concatenate([high, high, low], axis=0),
                preferred_element_type=F32,
            )
            for at, n in enumerate((2 * half, 2 * half + 1)):
                real = lanes(plane_waves[:NG, at * NX : (at + 1) * NX], index)
                imag = lanes(plane_waves[NG:, at * NX : (at + 1) * NX], index)
                cosines, sines = phase[plane, 0], phase[plane, 1]
                combine(n, real * cosines + imag * sines)
                combine(n + 4, imag * cosines - real * sines)

    def keep(channel, value):
        acc[channel] = value

    def finish(chunk, channel, value):
        send[chunk, pl.ds(channel, NG, stride=8), :] = (acc[channel] + value).T

    for load in loads[2:]:
        load.wait()
    transform(0, c, keep)

    pl.semaphore_wait(barrier, SIDE - 1 + 4)

    def remote(source, target, sent, received, grid, band):
        return pltpu.make_async_remote_copy(
            src_ref=source, dst_ref=target, send_sem=sent, recv_sem=received,
            device_id=(grid, band), device_id_type=MESH,
        )

    to_other = [
        remote(own_right.at[:, m], rights.at[1, c], y_send.at[m], y_recv.at[c], g - c + m, 1 - b)
        for m in range(2)
    ]
    pair = g + 1 - 2 * c
    to_pair = [
        remote(lefts.at[c], lefts.at[c], pair_send.at[0], pair_recv.at[0], pair, b),
        remote(own_right.at[:, 1 - c], rights.at[0, c], pair_send.at[1], pair_recv.at[1], pair, b),
    ]
    for copy in to_pair + to_other:
        copy.start()
    for copy in to_pair:
        copy.wait_recv()
    transform(0, 1 - c, functools.partial(finish, 0))

    def part(chunk, quarter, half):
        start = pl.multiple_of(quarter * QUARTER + half * HALF, HALF)
        return send.at[chunk, pl.ds(start, HALF)]

    grid_up = up * SIDE + j
    grid_down = down * SIDE + j

    def x_copies(chunk):
        sent, received = x_send.at[chunk], x_recv.at[chunk]
        return [
            remote(part(chunk, across, 0), from_a.at[chunk, 0], sent.at[0], received.at[0], grid_up, b),
            remote(part(chunk, across, 1), from_a.at[chunk, 1], sent.at[1], received.at[1], grid_down, b),
            remote(part(chunk, up, 1), from_b.at[chunk, 0], sent.at[2], received.at[2], grid_up, b),
            remote(part(chunk, down, 0), from_b.at[chunk, 1], sent.at[3], received.at[3], grid_down, b),
            remote(part(chunk, up, 0), from_c.at[chunk, 0], sent.at[4], received.at[4], grid_up, b),
            remote(part(chunk, down, 1), from_c.at[chunk, 1], sent.at[5], received.at[5], grid_down, b),
        ]

    def x_first(copies):
        for copy in copies[:4]:
            copy.start()

    def x_second(chunk, copies):
        for way, quarter in enumerate((up, down)):
            copies[way].wait_recv()
            ref = part(chunk, quarter, way)
            ref[...] = ref[...] + from_a[chunk, way]
            copies[4 + way].start()

    def z_first(chunk, copies):
        for copy in copies[2:]:
            copy.wait_recv()
        for half in range(2):
            x_sum[chunk, pl.ds(half * HALF, HALF)] = (
                part(chunk, x, half)[...] + from_c[chunk, half] + from_b[chunk, 1 - half]
            )
        mine = pl.ds(pl.multiple_of(j * 8, 8), 8)
        tiles[chunk, mine] = x_sum[chunk, mine]

        @pl.loop(1, SIDE)
        def _(step):
            to = lax.rem(j + step, SIDE)
            theirs = pl.ds(pl.multiple_of(to * 8, 8), 8)
            remote(
                x_sum.at[chunk, theirs], tiles.at[chunk, mine],
                z_send.at[chunk], z_recv.at[chunk], x * SIDE + to, b,
            ).start()

    def z_wait(buffer, chunk, sem):
        many = buffer.at[chunk, pl.ds(0, (SIDE - 1) * 8)]
        pltpu.make_async_copy(many, many, sem.at[chunk]).wait()

    def z_last(chunk):
        z_wait(tiles, chunk, z_recv)
        for core in range(2):
            total = tiles[chunk, pl.ds(core * 8, 8)]
            for chip in range(1, SIDE // 2):
                total = total + tiles[chunk, pl.ds((2 * chip + core) * 8, 8)]
            out_ref[pl.ds((2 * chunk + core) * 8, 8), :] = total

    native = x_copies(0)
    distant = x_copies(1)
    x_first(native)
    x_second(0, native)

    def arrival(core):
        return remote(
            own_right.at[:, 0], rights.at[1, core], y_send.at[0], y_recv.at[core], g, 1 - b
        )

    arrival(0).wait_recv()
    transform(1, 0, keep)
    arrival(1).wait_recv()
    transform(1, 1, functools.partial(finish, 1))
    x_first(distant)
    z_first(0, native)
    x_second(1, distant)
    z_first(1, distant)
    z_last(0)
    z_last(1)

    for copy in to_pair + to_other + native + distant:
        copy.wait_send()
    for chunk in range(2):
        z_wait(x_sum, chunk, z_send)


def last_kernel(order_ref, sums_ref, row_ref, out_ref):
    index = row_ref[...]
    factor = 1.0 / (NG * NG * NX) ** 0.5
    for column in range(4):
        start = pl.multiple_of(order_ref[column] * 8, 8)
        value = lanes(sums_ref[pl.ds(start, 8), :], index) * factor
        out_ref[pl.ds(column, 8, stride=4), :] = value


def local(left_bands, right_bands, sphere_index, right_order):
    along_x, along_y, trig = dft_tables()
    hbm = pl.BlockSpec(memory_space=pltpu.HBM)
    vmem = pl.BlockSpec(memory_space=pltpu.VMEM)
    dma = pltpu.SemaphoreType.DMA
    sums, row = pl.pallas_call(
        kernel,
        name="pair_sums",
        out_shape=(
            jax.ShapeDtypeStruct((32, NG), F32),
            jax.ShapeDtypeStruct((8, NG), jnp.int32),
        ),
        in_specs=[hbm] * 6,
        out_specs=(vmem, vmem),
        scratch_shapes=[
            pltpu.VMEM((2, 2, 4, NG, NX), F32),
            pltpu.VMEM((2, 2, 2, NG, NX), F32),
            pltpu.VMEM((2, 2, NG, NX), F32),
            pltpu.VMEM((NG, NG), jnp.int32),
            pltpu.VMEM((6 * NG, 2 * NG), BF16),
            pltpu.VMEM((2 * NG, 6 * NG), BF16),
            pltpu.VMEM((8, NG), F32),
            pltpu.VMEM((NG, NG), jnp.int32),
            pltpu.VMEM((NG, NG), jnp.int32),
            pltpu.VMEM((NG, NG), jnp.int32),
            pltpu.VMEM((2, 2, NG, NG), F32),
            pltpu.VMEM((8, NG, NG), F32),
            pltpu.VMEM((2, AX * QUARTER, NG), F32),
            pltpu.VMEM((2, 2, HALF, NG), F32),
            pltpu.VMEM((2, 2, HALF, NG), F32),
            pltpu.VMEM((2, 2, HALF, NG), F32),
            pltpu.VMEM((2, QUARTER, NG), F32),
            pltpu.VMEM((2, QUARTER, NG), F32),
            dma((7,)), dma((2,)), dma((2,)), dma((2,)), dma((2,)),
            dma((2, 6)), dma((2, 6)), dma((2,)), dma((2,)),
        ],
        compiler_params=pltpu.CompilerParams(collective_id=0, has_side_effects=True),
    )(
        left_bands.reshape(2, 4, NG, NX),
        right_bands.reshape(2, 2, NG, NX),
        sphere_index.reshape(NG, NG),
        jnp.asarray(along_x),
        jnp.asarray(along_y),
        jnp.asarray(trig),
    )
    position = (right_order - lax.axis_index("band") * 2) % 4
    result = pl.pallas_call(
        last_kernel,
        name="place",
        out_shape=jax.ShapeDtypeStruct((32, NG), F32),
        in_specs=[pl.BlockSpec(memory_space=pltpu.SMEM), vmem, vmem],
        out_specs=vmem,
    )(position, sums, row)
    return result.reshape(2, 4, 4, NG)


def solution(mesh):
    placed = (P(None, "band", "grid", None, None), P(None, "band", "grid", None, None), P(), P())
    return jax.shard_map(
        local, mesh=mesh, in_specs=placed, out_specs=P(None, "band", None, "grid"), check_vma=False
    )
```

```python
import functools
import math

import jax
import jax.numpy as jnp
from jax import lax
from jax.experimental import pallas as pl
from jax.experimental.pallas import tpu as pltpu
from jax.sharding import PartitionSpec as P
import numpy as np

NG = 128
NX = 128
NGV = 16384
AX, AH, AZ, AC = 4, 2, 8, 2
SIDE = AH * AZ * AC
QUARTER = SIDE * 8
HALF = QUARTER // 2
MESH = pl.DeviceIdType.MESH
F32 = jnp.float32
BF16 = jnp.bfloat16


def split(value):
    high = value.astype(BF16)
    return high, (value - high.astype(F32)).astype(BF16)


def dft_tables():
    counter = np.arange(NG)
    angles = (counter[:, None] * counter[None, :] % NG) * (2.0 * math.pi / NG)
    cosine, sine = np.cos(angles), np.sin(angles)

    def halves(table):
        high = table.astype(np.float32).astype(BF16)
        low = (table - high.astype(np.float64)).astype(np.float32).astype(BF16)
        return high, low

    high, low = halves(np.block([[cosine, -sine], [sine, cosine]]))
    along_x = np.concatenate([high, high, low], axis=0)
    high, low = halves(np.block([[cosine, sine], [-sine, cosine]]))
    along_y = np.concatenate([high, low, high], axis=1)
    trig = np.zeros((8, NG), np.float32)
    trig[0], trig[1] = cosine[1], sine[1]
    return along_x, along_y, trig


def lanes(value, index):
    return jnp.take_along_axis(value, index, axis=1, mode="promise_in_bounds")


def kernel(
    order_ref, left_ref, right_ref, sphere_ref, along_x_ref, along_y_ref, trig_ref, out_ref,
    lefts, rights, own_right, sphere, along_x, along_y, trig,
    ky_t, val_t, kx_of, phase, acc, send, from_a, from_b, from_c, x_sum, tiles,
    load_sem, pair_send, pair_recv, y_send, y_recv, x_send, x_recv, z_send, z_recv, known,
):
    g = lax.axis_index("grid")
    b = lax.axis_index("band")
    c = lax.rem(g, AC)
    j = lax.rem(g, SIDE)
    x = lax.div(g, SIDE)
    up = lax.rem(x + 1, AX)
    down = lax.rem(x + AX - 1, AX)
    across = lax.rem(x + 2, AX)

    loads = [
        pltpu.make_async_copy(right_ref, own_right, load_sem.at[0]),
        pltpu.make_async_copy(left_ref, lefts.at[c], load_sem.at[1]),
        pltpu.make_async_copy(sphere_ref, sphere, load_sem.at[2]),
        pltpu.make_async_copy(trig_ref, trig, load_sem.at[3]),
        pltpu.make_async_copy(right_ref.at[:, c], rights.at[0, c], load_sem.at[4]),
        pltpu.make_async_copy(along_x_ref, along_x, load_sem.at[5]),
        pltpu.make_async_copy(along_y_ref, along_y, load_sem.at[6]),
    ]
    for load in loads:
        load.start()

    grid_up = up * SIDE + j
    grid_down = down * SIDE + j
    pair = g + 1 - 2 * c
    z = lax.rem(lax.div(g, AC), AZ)
    opposite = g + SIDE // 2 - SIDE * lax.rem(lax.div(g, SIDE // 2), AH)
    along_z = [g + AC * (lax.rem(z + step, AZ) - z) for step in (1, 2, AZ - 1, AZ - 2)]
    friends = along_z + [opposite, pair]
    barrier = pltpu.get_barrier_semaphore()

    def signal(sem, grid, band):
        pl.semaphore_signal(sem, inc=1, device_id=(grid, band), device_id_type=MESH)

    signal(barrier, g - c, 1 - b)
    signal(barrier, g - c + 1, 1 - b)
    signal(barrier, grid_up, b)
    signal(barrier, grid_down, b)
    for friend in friends:
        signal(barrier, friend, b)

    def tell(step):
        for friend in friends:
            signal(known.at[step], friend, b)

    def hear(step):
        pl.semaphore_wait(known.at[step], len(friends))

    def remote(source, target, sent, received, grid, band):
        return pltpu.make_async_remote_copy(
            src_ref=source, dst_ref=target, send_sem=sent, recv_sem=received,
            device_id=(grid, band), device_id_type=MESH,
        )

    to_other = [
        remote(own_right.at[:, m], rights.at[1, c], y_send.at[m], y_recv.at[c], g - c + m, 1 - b)
        for m in range(2)
    ]
    to_pair = [
        remote(lefts.at[c], lefts.at[c], pair_send.at[0], pair_recv.at[0], pair, b),
        remote(own_right.at[:, 1 - c], rights.at[0, c], pair_send.at[1], pair_recv.at[1], pair, b),
    ]
    loads[0].wait()
    loads[1].wait()
    pl.semaphore_wait(barrier, 4 + len(friends))

    @pl.when(c == 0)
    def _():
        for copy in to_other:
            copy.start()

    for copy in to_pair:
        copy.start()
    tell(0)

    loads[2].wait()
    loads[3].wait()
    flipped = sphere[...].T
    ky_t[...] = (flipped >> 7) & 127
    val_t[...] = ((flipped >> 14) << 7) | (flipped & 127)
    rows = lax.broadcasted_iota(jnp.int32, (NG, NG), 0)

    def place(p, table):
        return jnp.where(ky_t[pl.ds(p, 1), :] == rows, val_t[pl.ds(p, 1), :], table)

    table = lax.fori_loop(0, NG, place, jnp.zeros((NG, NG), jnp.int32), unroll=8)
    kx_of[...] = table & 127
    kz = table >> 7
    cosine = jnp.broadcast_to(trig[0:1, :], (NG, NG))
    sine = jnp.broadcast_to(trig[1:2, :], (NG, NG))
    for core in range(2):
        angle = (kz * (g - c + core)) & 127
        phase[core, 0] = lanes(cosine, angle)
        phase[core, 1] = lanes(sine, angle)

    @pl.when(c == 1)
    def _():
        for copy in to_other:
            copy.start()

    def transform(chunk, plane, combine):
        right_real = rights[chunk, plane, 0]
        right_imag = rights[chunk, plane, 1]
        index = kx_of[...]
        for half in range(2):
            columns = []
            for n in (2 * half, 2 * half + 1):
                left_real = lefts[plane, 0, n]
                left_imag = lefts[plane, 1, n]
                field = jnp.concatenate(
                    [
                        left_real * right_real + left_imag * right_imag,
                        left_real * right_imag - left_imag * right_real,
                    ],
                    axis=1,
                )
                high, low = split(field)
                moved = jnp.dot(
                    jnp.concatenate([high, low, high], axis=1),
                    along_x[...],
                    preferred_element_type=F32,
                )
                columns.append(jnp.concatenate([moved[:, :NX], moved[:, NX:]], axis=0))
            high, low = split(jnp.concatenate(columns, axis=1))
            plane_waves = jnp.dot(
                along_y[...],
                jnp.concatenate([high, high, low], axis=0),
                preferred_element_type=F32,
            )
            for at, n in enumerate((2 * half, 2 * half + 1)):
                real = lanes(plane_waves[:NG, at * NX : (at + 1) * NX], index)
                imag = lanes(plane_waves[NG:, at * NX : (at + 1) * NX], index)
                cosines, sines = phase[plane, 0], phase[plane, 1]
                combine(n, real * cosines + imag * sines)
                combine(n + 4, imag * cosines - real * sines)

    def keep(channel, value):
        acc[channel] = value

    def finish(chunk, channel, value):
        send[chunk, pl.ds(channel, NG, stride=8), :] = (acc[channel] + value).T

    for load in loads[4:]:
        load.wait()
    transform(0, c, keep)
    hear(0)
    tell(1)
    for copy in to_pair:
        copy.wait_recv()
    transform(0, 1 - c, functools.partial(finish, 0))

    def part(chunk, quarter, half):
        start = pl.multiple_of(quarter * QUARTER + half * HALF, HALF)
        return send.at[chunk, pl.ds(start, HALF)]

    def x_copies(chunk):
        sent, received = x_send.at[chunk], x_recv.at[chunk]
        return [
            remote(part(chunk, across, 0), from_a.at[chunk, 0], sent.at[0], received.at[0], grid_up, b),
            remote(part(chunk, across, 1), from_a.at[chunk, 1], sent.at[1], received.at[1], grid_down, b),
            remote(part(chunk, up, 1), from_b.at[chunk, 0], sent.at[2], received.at[2], grid_up, b),
            remote(part(chunk, down, 0), from_b.at[chunk, 1], sent.at[3], received.at[3], grid_down, b),
            remote(part(chunk, up, 0), from_c.at[chunk, 0], sent.at[4], received.at[4], grid_up, b),
            remote(part(chunk, down, 1), from_c.at[chunk, 1], sent.at[5], received.at[5], grid_down, b),
        ]

    def x_first(copies):
        for copy in copies[:4]:
            copy.start()

    def x_second(chunk, copies):
        for way, quarter in enumerate((up, down)):
            copies[way].wait_recv()
            ref = part(chunk, quarter, way)
            ref[...] = ref[...] + from_a[chunk, way]
            copies[4 + way].start()

    def z_first(chunk, copies):
        for copy in copies[2:]:
            copy.wait_recv()
        for half in range(2):
            x_sum[chunk, pl.ds(half * HALF, HALF)] = (
                part(chunk, x, half)[...] + from_c[chunk, half] + from_b[chunk, 1 - half]
            )
        mine = pl.ds(pl.multiple_of(j * 8, 8), 8)
        tiles[chunk, mine] = x_sum[chunk, mine]

        @pl.loop(1, SIDE)
        def _(step):
            to = lax.rem(j + step, SIDE)
            theirs = pl.ds(pl.multiple_of(to * 8, 8), 8)
            remote(
                x_sum.at[chunk, theirs], tiles.at[chunk, mine],
                z_send.at[chunk], z_recv.at[chunk], x * SIDE + to, b,
            ).start()

    def z_wait(buffer, chunk, sem):
        many = buffer.at[chunk, pl.ds(0, (SIDE - 1) * 8)]
        pltpu.make_async_copy(many, many, sem.at[chunk]).wait()

    index = jnp.broadcast_to((sphere[pl.ds(g, 1), :] >> 7) & 127, (8, NG))
    factor = 1.0 / (NG * NG * NX) ** 0.5

    def z_last(chunk):
        z_wait(tiles, chunk, z_recv)
        values = []
        for core in range(2):
            total = tiles[chunk, pl.ds(core * 8, 8)]
            for chip in range(1, SIDE // 2):
                total = total + tiles[chunk, pl.ds((2 * chip + core) * 8, 8)]
            values.append(lanes(total, index) * factor)
        return values

    native = x_copies(0)
    distant = x_copies(1)
    x_first(native)
    hear(1)
    tell(2)

    def arrival(core):
        return remote(
            own_right.at[:, 0], rights.at[1, core], y_send.at[0], y_recv.at[core], g, 1 - b
        )

    arrival(0).wait_recv()
    transform(1, 0, keep)
    arrival(1).wait_recv()
    transform(1, 1, functools.partial(finish, 1))
    x_first(distant)
    x_second(0, native)
    hear(2)
    x_second(1, distant)
    z_first(0, native)
    z_first(1, distant)
    values = z_last(0)
    values = values + z_last(1)
    for column in range(4):
        position = jnp.full((8, NG), lax.rem(order_ref[column] + 4 - 2 * b, 4), jnp.int32)
        value = values[3]
        for at in range(3):
            value = jnp.where(position == at, values[at], value)
        out_ref[pl.ds(column, 8, stride=4), :] = value

    for copy in to_pair + to_other + native + distant:
        copy.wait_send()
    for chunk in range(2):
        z_wait(x_sum, chunk, z_send)


def local(left_bands, right_bands, sphere_index, right_order):
    along_x, along_y, trig = dft_tables()
    hbm = pl.BlockSpec(memory_space=pltpu.HBM)
    dma = pltpu.SemaphoreType.DMA
    result = pl.pallas_call(
        kernel,
        name="pair_sums",
        out_shape=jax.ShapeDtypeStruct((32, NG), F32),
        in_specs=[pl.BlockSpec(memory_space=pltpu.SMEM)] + [hbm] * 6,
        out_specs=pl.BlockSpec(memory_space=pltpu.VMEM),
        scratch_shapes=[
            pltpu.VMEM((2, 2, 4, NG, NX), F32),
            pltpu.VMEM((2, 2, 2, NG, NX), F32),
            pltpu.VMEM((2, 2, NG, NX), F32),
            pltpu.VMEM((NG, NG), jnp.int32),
            pltpu.VMEM((6 * NG, 2 * NG), BF16),
            pltpu.VMEM((2 * NG, 6 * NG), BF16),
            pltpu.VMEM((8, NG), F32),
            pltpu.VMEM((NG, NG), jnp.int32),
            pltpu.VMEM((NG, NG), jnp.int32),
            pltpu.VMEM((NG, NG), jnp.int32),
            pltpu.VMEM((2, 2, NG, NG), F32),
            pltpu.VMEM((8, NG, NG), F32),
            pltpu.VMEM((2, AX * QUARTER, NG), F32),
            pltpu.VMEM((2, 2, HALF, NG), F32),
            pltpu.VMEM((2, 2, HALF, NG), F32),
            pltpu.VMEM((2, 2, HALF, NG), F32),
            pltpu.VMEM((2, QUARTER, NG), F32),
            pltpu.VMEM((2, QUARTER, NG), F32),
            dma((7,)), dma((2,)), dma((2,)), dma((2,)), dma((2,)),
            dma((2, 6)), dma((2, 6)), dma((2,)), dma((2,)), pltpu.SemaphoreType.REGULAR((3,)),
        ],
        compiler_params=pltpu.CompilerParams(collective_id=0, has_side_effects=True),
    )(
        right_order,
        left_bands.reshape(2, 4, NG, NX),
        right_bands.reshape(2, 2, NG, NX),
        sphere_index.reshape(NG, NG),
        jnp.asarray(along_x),
        jnp.asarray(along_y),
        jnp.asarray(trig),
    )
    return result.reshape(2, 4, 4, NG)


def solution(mesh):
    placed = (P(None, "band", "grid", None, None), P(None, "band", "grid", None, None), P(), P())
    return jax.shard_map(
        local, mesh=mesh, in_specs=placed, out_specs=P(None, "band", None, "grid"), check_vma=False
    )
```

```python
import functools
import math

import jax
import jax.numpy as jnp
from jax import lax
from jax.experimental import pallas as pl
from jax.experimental.pallas import tpu as pltpu
from jax.sharding import PartitionSpec as P
import numpy as np

NG = 128
NX = 128
NGV = 16384
AX, AH, AZ, AC = 4, 2, 8, 2
SIDE = AH * AZ * AC
QUARTER = SIDE * 8
HALF = QUARTER // 2
MESH = pl.DeviceIdType.MESH
F32 = jnp.float32
BF16 = jnp.bfloat16


def split(value):
    high = value.astype(BF16)
    return high, (value - high.astype(F32)).astype(BF16)


def dft_tables():
    counter = np.arange(NG)
    angles = (counter[:, None] * counter[None, :] % NG) * (2.0 * math.pi / NG)
    cosine, sine = np.cos(angles), np.sin(angles)

    def halves(table):
        high = table.astype(np.float32).astype(BF16)
        low = (table - high.astype(np.float64)).astype(np.float32).astype(BF16)
        return high, low

    high, low = halves(np.block([[cosine, -sine], [sine, cosine]]))
    along_x = np.concatenate([high, high, low], axis=0)
    high, low = halves(np.block([[cosine, sine], [-sine, cosine]]))
    along_y = np.concatenate([high, low, high], axis=1)
    trig = np.zeros((8, NG), np.float32)
    trig[0], trig[1] = cosine[1], sine[1]
    return along_x, along_y, trig


def lanes(value, index):
    return jnp.take_along_axis(value, index, axis=1, mode="promise_in_bounds")


def kernel(
    order_ref, left_ref, right_ref, sphere_ref, along_x_ref, along_y_ref, trig_ref, out_ref,
    lefts, rights, own_right, sphere, along_x, along_y, trig,
    ky_t, val_t, kx_of, phase, acc, send, from_a, from_b, from_c, x_sum, tiles,
    order, load_sem, pair_send, pair_recv, y_send, y_recv, x_send, x_recv, z_send, z_recv, known,
):
    g = lax.axis_index("grid")
    b = lax.axis_index("band")
    c = lax.rem(g, AC)
    j = lax.rem(g, SIDE)
    x = lax.div(g, SIDE)
    up = lax.rem(x + 1, AX)
    down = lax.rem(x + AX - 1, AX)
    across = lax.rem(x + 2, AX)

    loads = [
        pltpu.make_async_copy(right_ref, own_right, load_sem.at[0]),
        pltpu.make_async_copy(left_ref, lefts.at[c], load_sem.at[1]),
        pltpu.make_async_copy(sphere_ref, sphere, load_sem.at[2]),
        pltpu.make_async_copy(trig_ref, trig, load_sem.at[3]),
        pltpu.make_async_copy(right_ref.at[:, c], rights.at[0, c], load_sem.at[4]),
        pltpu.make_async_copy(along_x_ref, along_x, load_sem.at[5]),
        pltpu.make_async_copy(along_y_ref, along_y, load_sem.at[6]),
        pltpu.make_async_copy(order_ref, order, load_sem.at[7]),
    ]
    for load in loads:
        load.start()

    grid_up = up * SIDE + j
    grid_down = down * SIDE + j
    pair = g + 1 - 2 * c
    h = lax.rem(lax.div(g, SIDE // 2), AH)
    z = lax.rem(lax.div(g, AC), AZ)
    opposite = g + SIDE // 2 - SIDE * h
    along_z = [g + AC * (lax.rem(z + step, AZ) - z) for step in (1, AZ - 1, 2, AZ - 2)]
    near = [(along_z[0], b), (along_z[1], b), (pair, b), (g, 1 - b), (opposite, 1 - b)]
    friends = [(grid, b) for grid in along_z + [opposite, pair]]
    barrier = pltpu.get_barrier_semaphore()

    def signal(sem, grid, band):
        pl.semaphore_signal(sem, inc=1, device_id=(grid, band), device_id_type=MESH)

    meet = near + [(pair, 1 - b), (grid_up, b), (grid_down, b)]
    for grid, band in meet:
        signal(barrier, grid, band)

    def tell(step):
        for grid, band in near if step == 0 else friends:
            signal(known.at[step], grid, band)

    def hear(step):
        pl.semaphore_wait(known.at[step], len(near if step == 0 else friends))

    def remote(source, target, sent, received, grid, band):
        return pltpu.make_async_remote_copy(
            src_ref=source, dst_ref=target, send_sem=sent, recv_sem=received,
            device_id=(grid, band), device_id_type=MESH,
        )

    to_other = [
        remote(own_right.at[:, m], rights.at[1, c], y_send.at[m], y_recv.at[c], g - c + m, 1 - b)
        for m in range(2)
    ]
    to_pair = [
        remote(lefts.at[c], lefts.at[c], pair_send.at[0], pair_recv.at[0], pair, b),
        remote(own_right.at[:, 1 - c], rights.at[0, c], pair_send.at[1], pair_recv.at[1], pair, b),
    ]
    loads[2].wait()
    loads[3].wait()
    flipped = sphere[...].T
    ky_t[...] = (flipped >> 7) & 127
    val_t[...] = ((flipped >> 14) << 7) | (flipped & 127)
    rows = lax.broadcasted_iota(jnp.int32, (NG, NG), 0)

    def place(p, table):
        return jnp.where(ky_t[pl.ds(p, 1), :] == rows, val_t[pl.ds(p, 1), :], table)

    table = lax.fori_loop(0, NG, place, jnp.zeros((NG, NG), jnp.int32), unroll=8)
    kx_of[...] = table & 127
    kz = table >> 7
    cosine = jnp.broadcast_to(trig[0:1, :], (NG, NG))
    sine = jnp.broadcast_to(trig[1:2, :], (NG, NG))
    for core in range(2):
        angle = (kz * (g - c + core)) & 127
        phase[core, 0] = lanes(cosine, angle)
        phase[core, 1] = lanes(sine, angle)

    loads[0].wait()
    loads[1].wait()
    pl.semaphore_wait(barrier, len(meet))
    for copy in to_other + to_pair:
        copy.start()
    tell(0)

    def transform(chunk, plane, combine):
        right_real = rights[chunk, plane, 0]
        right_imag = rights[chunk, plane, 1]
        index = kx_of[...]
        for half in range(2):
            columns = []
            for n in (2 * half, 2 * half + 1):
                left_real = lefts[plane, 0, n]
                left_imag = lefts[plane, 1, n]
                field = jnp.concatenate(
                    [
                        left_real * right_real + left_imag * right_imag,
                        left_real * right_imag - left_imag * right_real,
                    ],
                    axis=1,
                )
                high, low = split(field)
                moved = jnp.dot(
                    jnp.concatenate([high, low, high], axis=1),
                    along_x[...],
                    preferred_element_type=F32,
                )
                columns.append(jnp.concatenate([moved[:, :NX], moved[:, NX:]], axis=0))
            high, low = split(jnp.concatenate(columns, axis=1))
            plane_waves = jnp.dot(
                along_y[...],
                jnp.concatenate([high, high, low], axis=0),
                preferred_element_type=F32,
            )
            for at, n in enumerate((2 * half, 2 * half + 1)):
                real = lanes(plane_waves[:NG, at * NX : (at + 1) * NX], index)
                imag = lanes(plane_waves[NG:, at * NX : (at + 1) * NX], index)
                cosines, sines = phase[plane, 0], phase[plane, 1]
                combine(n, real * cosines + imag * sines)
                combine(n + 4, imag * cosines - real * sines)

    def keep(channel, value):
        acc[channel] = value

    def finish(chunk, channel, value):
        send[chunk, pl.ds(channel, NG, stride=8), :] = (acc[channel] + value).T

    for load in loads[4:7]:
        load.wait()
    transform(0, c, keep)
    for copy in to_pair:
        copy.wait_recv()
    transform(0, 1 - c, functools.partial(finish, 0))

    def part(chunk, quarter, half):
        start = pl.multiple_of(quarter * QUARTER + half * HALF, HALF)
        return send.at[chunk, pl.ds(start, HALF)]

    def x_copies(chunk):
        sent, received = x_send.at[chunk], x_recv.at[chunk]
        return [
            remote(part(chunk, across, 0), from_a.at[chunk, 0], sent.at[0], received.at[0], grid_up, b),
            remote(part(chunk, across, 1), from_a.at[chunk, 1], sent.at[1], received.at[1], grid_down, b),
            remote(part(chunk, up, 1), from_b.at[chunk, 0], sent.at[2], received.at[2], grid_up, b),
            remote(part(chunk, down, 0), from_b.at[chunk, 1], sent.at[3], received.at[3], grid_down, b),
            remote(part(chunk, up, 0), from_c.at[chunk, 0], sent.at[4], received.at[4], grid_up, b),
            remote(part(chunk, down, 1), from_c.at[chunk, 1], sent.at[5], received.at[5], grid_down, b),
        ]

    def x_first(copies):
        for copy in copies[:4]:
            copy.start()

    def x_second(chunk, copies):
        for way, quarter in enumerate((up, down)):
            copies[way].wait_recv()
            ref = part(chunk, quarter, way)
            ref[...] = ref[...] + from_a[chunk, way]
            copies[4 + way].start()

    def z_first(chunk, copies):
        for copy in copies[2:]:
            copy.wait_recv()
        for half in range(2):
            x_sum[chunk, pl.ds(half * HALF, HALF)] = (
                part(chunk, x, half)[...] + from_c[chunk, half] + from_b[chunk, 1 - half]
            )
        mine = pl.ds(pl.multiple_of(j * 8, 8), 8)
        tiles[chunk, mine] = x_sum[chunk, mine]

        for away_z in (4, 3, 5, 2, 6, 1, 7, 0):
            for away in (2, 3, 0, 1):
                if (away_z, away) == (0, 0):
                    continue
                to = (
                    lax.rem(h + away // 2, AH) * AZ * AC
                    + lax.rem(z + away_z, AZ) * AC
                    + lax.rem(c + away % 2, AC)
                )
                theirs = pl.ds(pl.multiple_of(to * 8, 8), 8)
                remote(
                    x_sum.at[chunk, theirs], tiles.at[chunk, mine],
                    z_send.at[chunk], z_recv.at[chunk], x * SIDE + to, b,
                ).start()

    def z_wait(buffer, chunk, sem):
        many = buffer.at[chunk, pl.ds(0, (SIDE - 1) * 8)]
        pltpu.make_async_copy(many, many, sem.at[chunk]).wait()

    index = jnp.broadcast_to((sphere[pl.ds(g, 1), :] >> 7) & 127, (8, NG))
    factor = 1.0 / (NG * NG * NX) ** 0.5

    def z_last(chunk):
        z_wait(tiles, chunk, z_recv)
        values = []
        for core in range(2):
            total = tiles[chunk, pl.ds(core * 8, 8)]
            for chip in range(1, SIDE // 2):
                total = total + tiles[chunk, pl.ds((2 * chip + core) * 8, 8)]
            values.append(lanes(total, index) * factor)
        return values

    native = x_copies(0)
    distant = x_copies(1)
    x_first(native)
    hear(0)
    tell(1)

    @pl.when(c == 1)
    def _():
        x_second(0, native)

    def arrival(core):
        return remote(
            own_right.at[:, 0], rights.at[1, core], y_send.at[0], y_recv.at[core], g, 1 - b
        )

    arrival(0).wait_recv()
    transform(1, 0, keep)
    hear(1)
    tell(2)
    arrival(1).wait_recv()
    transform(1, 1, functools.partial(finish, 1))
    x_first(distant)
    @pl.when(c == 0)
    def _():
        x_second(0, native)

    hear(2)
    z_first(0, native)
    x_second(1, distant)
    z_first(1, distant)
    values = z_last(0)
    values = values + z_last(1)
    loads[7].wait()
    for column in range(4):
        position = jnp.full((8, NG), lax.rem(order[column] + 4 - 2 * b, 4), jnp.int32)
        value = values[3]
        for at in range(3):
            value = jnp.where(position == at, values[at], value)
        out_ref[pl.ds(column, 8, stride=4), :] = value

    for copy in to_pair + to_other + native + distant:
        copy.wait_send()
    for chunk in range(2):
        z_wait(x_sum, chunk, z_send)


def local(left_bands, right_bands, sphere_index, right_order):
    along_x, along_y, trig = dft_tables()
    hbm = pl.BlockSpec(memory_space=pltpu.HBM)
    dma = pltpu.SemaphoreType.DMA
    result = pl.pallas_call(
        kernel,
        name="pair_sums",
        out_shape=pltpu.VMEM((32, NG), F32),
        in_specs=[hbm] * 7,
        out_specs=pl.BlockSpec(memory_space=pltpu.VMEM),
        scratch_shapes=[
            pltpu.VMEM((2, 2, 4, NG, NX), F32),
            pltpu.VMEM((2, 2, 2, NG, NX), F32),
            pltpu.VMEM((2, 2, NG, NX), F32),
            pltpu.VMEM((NG, NG), jnp.int32),
            pltpu.VMEM((6 * NG, 2 * NG), BF16),
            pltpu.VMEM((2 * NG, 6 * NG), BF16),
            pltpu.VMEM((8, NG), F32),
            pltpu.VMEM((NG, NG), jnp.int32),
            pltpu.VMEM((NG, NG), jnp.int32),
            pltpu.VMEM((NG, NG), jnp.int32),
            pltpu.VMEM((2, 2, NG, NG), F32),
            pltpu.VMEM((8, NG, NG), F32),
            pltpu.VMEM((2, AX * QUARTER, NG), F32),
            pltpu.VMEM((2, 2, HALF, NG), F32),
            pltpu.VMEM((2, 2, HALF, NG), F32),
            pltpu.VMEM((2, 2, HALF, NG), F32),
            pltpu.VMEM((2, QUARTER, NG), F32),
            pltpu.VMEM((2, QUARTER, NG), F32),
            pltpu.SMEM((4,), jnp.int32),
            dma((8,)), dma((2,)), dma((2,)), dma((2,)), dma((2,)),
            dma((2, 6)), dma((2, 6)), dma((2,)), dma((2,)), pltpu.SemaphoreType.REGULAR((3,)),
        ],
        compiler_params=pltpu.CompilerParams(collective_id=0, has_side_effects=True),
    )(
        right_order,
        left_bands.reshape(2, 4, NG, NX),
        right_bands.reshape(2, 2, NG, NX),
        sphere_index.reshape(NG, NG),
        jnp.asarray(along_x),
        jnp.asarray(along_y),
        jnp.asarray(trig),
    )
    return result.reshape(2, 4, 4, NG)


def solution(mesh):
    placed = (P(None, "band", "grid", None, None), P(None, "band", "grid", None, None), P(), P())
    return jax.shard_map(
        local, mesh=mesh, in_specs=placed, out_specs=P(None, "band", None, "grid"), check_vma=False
    )
```

```python
import functools
import math

import jax
import jax.numpy as jnp
from jax import lax
from jax.experimental import pallas as pl
from jax.experimental.pallas import tpu as pltpu
from jax.sharding import PartitionSpec as P
import numpy as np

NG = 128
NX = 128
NGV = 16384
AX, AH, AZ, AC = 4, 2, 8, 2
SIDE = AH * AZ * AC
QUARTER = SIDE * 8
HALF = QUARTER // 2
MESH = pl.DeviceIdType.MESH
F32 = jnp.float32
BF16 = jnp.bfloat16


def split(value):
    high = value.astype(BF16)
    return high, (value - high.astype(F32)).astype(BF16)


def dft_tables():
    counter = np.arange(NG)
    angles = (counter[:, None] * counter[None, :] % NG) * (2.0 * math.pi / NG)
    cosine, sine = np.cos(angles), np.sin(angles)

    def halves(table):
        high = table.astype(np.float32).astype(BF16)
        low = (table - high.astype(np.float64)).astype(np.float32).astype(BF16)
        return high, low

    high, low = halves(np.block([[cosine, -sine], [sine, cosine]]))
    along_x = np.concatenate([high, high, low], axis=0)
    high, low = halves(np.block([[cosine, sine], [-sine, cosine]]))
    along_y = np.concatenate([high, low, high], axis=1)
    trig = np.zeros((8, NG), np.float32)
    trig[0], trig[1] = cosine[1], sine[1]
    return along_x, along_y, trig


def lanes(value, index):
    return jnp.take_along_axis(value, index, axis=1, mode="promise_in_bounds")


def kernel(
    order_ref, left_ref, right_ref, sphere_ref, along_x_ref, along_y_ref, trig_ref, out_ref,
    lefts, rights, own_right, sphere, along_x, along_y, trig,
    ky_t, val_t, kx_of, phase, acc, send, from_a, from_b, from_c, x_sum, tiles,
    order, load_sem, pair_send, pair_recv, y_send, y_recv, x_send, x_recv, z_send, z_recv, known,
):
    g = lax.axis_index("grid")
    b = lax.axis_index("band")
    c = lax.rem(g, AC)
    j = lax.rem(g, SIDE)
    x = lax.div(g, SIDE)
    up = lax.rem(x + 1, AX)
    down = lax.rem(x + AX - 1, AX)
    across = lax.rem(x + 2, AX)

    loads = [
        pltpu.make_async_copy(right_ref, own_right, load_sem.at[0]),
        pltpu.make_async_copy(left_ref, lefts.at[c], load_sem.at[1]),
        pltpu.make_async_copy(sphere_ref, sphere, load_sem.at[2]),
        pltpu.make_async_copy(trig_ref, trig, load_sem.at[3]),
        pltpu.make_async_copy(right_ref.at[:, c], rights.at[0, c], load_sem.at[4]),
        pltpu.make_async_copy(along_x_ref, along_x, load_sem.at[5]),
        pltpu.make_async_copy(along_y_ref, along_y, load_sem.at[6]),
        pltpu.make_async_copy(order_ref, order, load_sem.at[7]),
    ]
    for load in loads:
        load.start()

    grid_up = up * SIDE + j
    grid_down = down * SIDE + j
    pair = g + 1 - 2 * c
    h = lax.rem(lax.div(g, SIDE // 2), AH)
    z = lax.rem(lax.div(g, AC), AZ)
    opposite = g + SIDE // 2 - SIDE * h
    along_z = [g + AC * (lax.rem(z + step, AZ) - z) for step in (1, AZ - 1, 2, AZ - 2)]
    near = [(along_z[0], b), (along_z[1], b), (pair, b), (g, 1 - b), (opposite, 1 - b)]
    friends = [(grid, b) for grid in along_z + [opposite, pair]]
    barrier = pltpu.get_barrier_semaphore()

    def signal(sem, grid, band):
        pl.semaphore_signal(sem, inc=1, device_id=(grid, band), device_id_type=MESH)

    meet = near + [(pair, 1 - b), (grid_up, b), (grid_down, b)]
    for grid, band in meet:
        signal(barrier, grid, band)

    def tell(step):
        for grid, band in near if step == 0 else friends:
            signal(known.at[step], grid, band)

    def hear(step):
        pl.semaphore_wait(known.at[step], len(near if step == 0 else friends))

    def remote(source, target, sent, received, grid, band):
        return pltpu.make_async_remote_copy(
            src_ref=source, dst_ref=target, send_sem=sent, recv_sem=received,
            device_id=(grid, band), device_id_type=MESH,
        )

    to_other = [
        remote(own_right.at[:, m], rights.at[1, c], y_send.at[m], y_recv.at[c], g - c + m, 1 - b)
        for m in range(2)
    ]
    to_pair = [
        remote(lefts.at[c], lefts.at[c], pair_send.at[0], pair_recv.at[0], pair, b),
        remote(own_right.at[:, 1 - c], rights.at[0, c], pair_send.at[1], pair_recv.at[1], pair, b),
    ]
    loads[0].wait()
    pl.semaphore_wait(barrier, len(meet))
    for copy in to_other:
        copy.start()
    loads[1].wait()
    for copy in to_pair:
        copy.start()
    tell(0)

    loads[2].wait()
    loads[3].wait()
    flipped = sphere[...].T
    ky_t[...] = (flipped >> 7) & 127
    val_t[...] = ((flipped >> 14) << 7) | (flipped & 127)
    rows = lax.broadcasted_iota(jnp.int32, (NG, NG), 0)

    def place(p, table):
        return jnp.where(ky_t[pl.ds(p, 1), :] == rows, val_t[pl.ds(p, 1), :], table)

    table = lax.fori_loop(0, NG, place, jnp.zeros((NG, NG), jnp.int32), unroll=8)
    kx_of[...] = table & 127
    kz = table >> 7
    cosine = jnp.broadcast_to(trig[0:1, :], (NG, NG))
    sine = jnp.broadcast_to(trig[1:2, :], (NG, NG))
    for core in range(2):
        angle = (kz * (g - c + core)) & 127
        phase[core, 0] = lanes(cosine, angle)
        phase[core, 1] = lanes(sine, angle)

    def transform(chunk, plane, combine):
        right_real = rights[chunk, plane, 0]
        right_imag = rights[chunk, plane, 1]
        index = kx_of[...]
        for half in range(2):
            columns = []
            for n in (2 * half, 2 * half + 1):
                left_real = lefts[plane, 0, n]
                left_imag = lefts[plane, 1, n]
                field = jnp.concatenate(
                    [
                        left_real * right_real + left_imag * right_imag,
                        left_real * right_imag - left_imag * right_real,
                    ],
                    axis=1,
                )
                high, low = split(field)
                moved = jnp.dot(
                    jnp.concatenate([high, low, high], axis=1),
                    along_x[...],
                    preferred_element_type=F32,
                )
                columns.append(jnp.concatenate([moved[:, :NX], moved[:, NX:]], axis=0))
            high, low = split(jnp.concatenate(columns, axis=1))
            plane_waves = jnp.dot(
                along_y[...],
                jnp.concatenate([high, high, low], axis=0),
                preferred_element_type=F32,
            )
            for at, n in enumerate((2 * half, 2 * half + 1)):
                real = lanes(plane_waves[:NG, at * NX : (at + 1) * NX], index)
                imag = lanes(plane_waves[NG:, at * NX : (at + 1) * NX], index)
                cosines, sines = phase[plane, 0], phase[plane, 1]
                combine(n, real * cosines + imag * sines)
                combine(n + 4, imag * cosines - real * sines)

    def keep(channel, value):
        acc[channel] = value

    def finish(chunk, channel, value):
        send[chunk, pl.ds(channel, NG, stride=8), :] = (acc[channel] + value).T

    for load in loads[4:7]:
        load.wait()
    transform(0, c, keep)
    for copy in to_pair:
        copy.wait_recv()
    transform(0, 1 - c, functools.partial(finish, 0))

    def part(chunk, quarter, half):
        start = pl.multiple_of(quarter * QUARTER + half * HALF, HALF)
        return send.at[chunk, pl.ds(start, HALF)]

    def x_copies(chunk):
        sent, received = x_send.at[chunk], x_recv.at[chunk]
        return [
            remote(part(chunk, across, 0), from_a.at[chunk, 0], sent.at[0], received.at[0], grid_up, b),
            remote(part(chunk, across, 1), from_a.at[chunk, 1], sent.at[1], received.at[1], grid_down, b),
            remote(part(chunk, up, 1), from_b.at[chunk, 0], sent.at[2], received.at[2], grid_up, b),
            remote(part(chunk, down, 0), from_b.at[chunk, 1], sent.at[3], received.at[3], grid_down, b),
            remote(part(chunk, up, 0), from_c.at[chunk, 0], sent.at[4], received.at[4], grid_up, b),
            remote(part(chunk, down, 1), from_c.at[chunk, 1], sent.at[5], received.at[5], grid_down, b),
        ]

    def x_first(copies):
        for copy in copies[:4]:
            copy.start()

    def x_second(chunk, copies):
        for way, quarter in enumerate((up, down)):
            copies[way].wait_recv()
            ref = part(chunk, quarter, way)
            ref[...] = ref[...] + from_a[chunk, way]
            copies[4 + way].start()

    def z_first(chunk, copies):
        for copy in copies[2:]:
            copy.wait_recv()
        for half in range(2):
            x_sum[chunk, pl.ds(half * HALF, HALF)] = (
                part(chunk, x, half)[...] + from_c[chunk, half] + from_b[chunk, 1 - half]
            )
        mine = pl.ds(pl.multiple_of(j * 8, 8), 8)
        tiles[chunk, mine] = x_sum[chunk, mine]

        for away_z in (4, 3, 5, 2, 6, 1, 7, 0):
            for away in (2, 3, 0, 1):
                if (away_z, away) == (0, 0):
                    continue
                to = (
                    lax.rem(h + away // 2, AH) * AZ * AC
                    + lax.rem(z + away_z, AZ) * AC
                    + lax.rem(c + away % 2, AC)
                )
                theirs = pl.ds(pl.multiple_of(to * 8, 8), 8)
                remote(
                    x_sum.at[chunk, theirs], tiles.at[chunk, mine],
                    z_send.at[chunk], z_recv.at[chunk], x * SIDE + to, b,
                ).start()

    def z_wait(buffer, chunk, sem):
        many = buffer.at[chunk, pl.ds(0, (SIDE - 1) * 8)]
        pltpu.make_async_copy(many, many, sem.at[chunk]).wait()

    index = jnp.broadcast_to((sphere[pl.ds(g, 1), :] >> 7) & 127, (8, NG))
    factor = 1.0 / (NG * NG * NX) ** 0.5

    def z_last(chunk):
        z_wait(tiles, chunk, z_recv)
        values = []
        for core in range(2):
            total = tiles[chunk, pl.ds(core * 8, 8)]
            for chip in range(1, SIDE // 2):
                total = total + tiles[chunk, pl.ds((2 * chip + core) * 8, 8)]
            values.append(lanes(total, index) * factor)
        return values

    native = x_copies(0)
    distant = x_copies(1)
    x_first(native)
    hear(0)
    tell(1)

    @pl.when(c == 1)
    def _():
        x_second(0, native)

    def arrival(core):
        return remote(
            own_right.at[:, 0], rights.at[1, core], y_send.at[0], y_recv.at[core], g, 1 - b
        )

    arrival(0).wait_recv()
    transform(1, 0, keep)
    hear(1)
    tell(2)
    arrival(1).wait_recv()

    @pl.when(c == 0)
    def _():
        x_second(0, native)

    transform(1, 1, functools.partial(finish, 1))
    x_first(distant)
    hear(2)
    z_first(0, native)
    x_second(1, distant)
    z_first(1, distant)
    values = z_last(0)
    values = values + z_last(1)
    loads[7].wait()
    for column in range(4):
        position = jnp.full((8, NG), lax.rem(order[column] + 4 - 2 * b, 4), jnp.int32)
        value = values[3]
        for at in range(3):
            value = jnp.where(position == at, values[at], value)
        out_ref[pl.ds(column, 8, stride=4), :] = value

    for copy in to_pair + to_other + native + distant:
        copy.wait_send()
    for chunk in range(2):
        z_wait(x_sum, chunk, z_send)


def local(left_bands, right_bands, sphere_index, right_order):
    along_x, along_y, trig = dft_tables()
    hbm = pl.BlockSpec(memory_space=pltpu.HBM)
    dma = pltpu.SemaphoreType.DMA
    result = pl.pallas_call(
        kernel,
        name="pair_sums",
        out_shape=pltpu.VMEM((32, NG), F32),
        in_specs=[hbm] * 7,
        out_specs=pl.BlockSpec(memory_space=pltpu.VMEM),
        scratch_shapes=[
            pltpu.VMEM((2, 2, 4, NG, NX), F32),
            pltpu.VMEM((2, 2, 2, NG, NX), F32),
            pltpu.VMEM((2, 2, NG, NX), F32),
            pltpu.VMEM((NG, NG), jnp.int32),
            pltpu.VMEM((6 * NG, 2 * NG), BF16),
            pltpu.VMEM((2 * NG, 6 * NG), BF16),
            pltpu.VMEM((8, NG), F32),
            pltpu.VMEM((NG, NG), jnp.int32),
            pltpu.VMEM((NG, NG), jnp.int32),
            pltpu.VMEM((NG, NG), jnp.int32),
            pltpu.VMEM((2, 2, NG, NG), F32),
            pltpu.VMEM((8, NG, NG), F32),
            pltpu.VMEM((2, AX * QUARTER, NG), F32),
            pltpu.VMEM((2, 2, HALF, NG), F32),
            pltpu.VMEM((2, 2, HALF, NG), F32),
            pltpu.VMEM((2, 2, HALF, NG), F32),
            pltpu.VMEM((2, QUARTER, NG), F32),
            pltpu.VMEM((2, QUARTER, NG), F32),
            pltpu.SMEM((4,), jnp.int32),
            dma((8,)), dma((2,)), dma((2,)), dma((2,)), dma((2,)),
            dma((2, 6)), dma((2, 6)), dma((2,)), dma((2,)), pltpu.SemaphoreType.REGULAR((3,)),
        ],
        compiler_params=pltpu.CompilerParams(collective_id=0, has_side_effects=True),
    )(
        right_order,
        left_bands.reshape(2, 4, NG, NX),
        right_bands.reshape(2, 2, NG, NX),
        sphere_index.reshape(NG, NG),
        jnp.asarray(along_x),
        jnp.asarray(along_y),
        jnp.asarray(trig),
    )
    return result.reshape(2, 4, 4, NG)


def solution(mesh):
    placed = (P(None, "band", "grid", None, None), P(None, "band", "grid", None, None), P(), P())
    return jax.shard_map(
        local, mesh=mesh, in_specs=placed, out_specs=P(None, "band", None, "grid"), check_vma=False
    )
```

```python
import functools
import math

import jax
import jax.numpy as jnp
from jax import lax
from jax.experimental import pallas as pl
from jax.experimental.pallas import tpu as pltpu
from jax.sharding import PartitionSpec as P
import numpy as np

NG = 128
NX = 128
NGV = 16384
AX, AH, AZ, AC = 4, 2, 8, 2
SIDE = AH * AZ * AC
QUARTER = SIDE * 8
HALF = QUARTER // 2
MESH = pl.DeviceIdType.MESH
F32 = jnp.float32
BF16 = jnp.bfloat16


def split(value):
    high = value.astype(BF16)
    return high, (value - high.astype(F32)).astype(BF16)


def dft_tables():
    counter = np.arange(NG)
    angles = (counter[:, None] * counter[None, :] % NG) * (2.0 * math.pi / NG)
    cosine, sine = np.cos(angles), np.sin(angles)

    def halves(table):
        high = table.astype(np.float32).astype(BF16)
        low = (table - high.astype(np.float64)).astype(np.float32).astype(BF16)
        return high, low

    high, low = halves(np.block([[cosine, -sine], [sine, cosine]]))
    along_x = np.concatenate([high, high, low], axis=0)
    high, low = halves(np.block([[cosine, sine], [-sine, cosine]]))
    along_y = np.concatenate([high, low, high], axis=1)
    trig = np.zeros((8, NG), np.float32)
    trig[0], trig[1] = cosine[1], sine[1]
    return along_x, along_y, trig


def lanes(value, index):
    return jnp.take_along_axis(value, index, axis=1, mode="promise_in_bounds")


def kernel(
    order_ref, left_ref, right_ref, sphere_ref, along_x_ref, along_y_ref, trig_ref, out_ref,
    lefts, rights, own_right, sphere, along_x, along_y, trig,
    ky_t, val_t, kx_of, phase, acc, send, from_a, from_b, from_c, x_sum, tiles,
    order, load_sem, pair_send, pair_recv, y_send, y_recv, x_send, x_recv, z_send, z_recv, known,
):
    g = lax.axis_index("grid")
    b = lax.axis_index("band")
    c = lax.rem(g, AC)
    j = lax.rem(g, SIDE)
    x = lax.div(g, SIDE)
    up = lax.rem(x + 1, AX)
    down = lax.rem(x + AX - 1, AX)
    across = lax.rem(x + 2, AX)

    loads = [
        pltpu.make_async_copy(right_ref, own_right, load_sem.at[0]),
        pltpu.make_async_copy(left_ref, lefts.at[c], load_sem.at[1]),
        pltpu.make_async_copy(sphere_ref, sphere, load_sem.at[2]),
        pltpu.make_async_copy(trig_ref, trig, load_sem.at[3]),
        pltpu.make_async_copy(right_ref.at[:, c], rights.at[0, c], load_sem.at[4]),
        pltpu.make_async_copy(along_x_ref, along_x, load_sem.at[5]),
        pltpu.make_async_copy(along_y_ref, along_y, load_sem.at[6]),
        pltpu.make_async_copy(order_ref, order, load_sem.at[7]),
    ]
    for load in loads:
        load.start()

    grid_up = up * SIDE + j
    grid_down = down * SIDE + j
    pair = g + 1 - 2 * c
    h = lax.rem(lax.div(g, SIDE // 2), AH)
    z = lax.rem(lax.div(g, AC), AZ)
    opposite = g + SIDE // 2 - SIDE * h
    along_z = [g + AC * (lax.rem(z + step, AZ) - z) for step in (1, AZ - 1, 2, AZ - 2)]
    near = [(along_z[0], b), (along_z[1], b), (pair, b), (g, 1 - b), (opposite, 1 - b)]
    friends = [(grid, b) for grid in along_z + [opposite, pair]]
    barrier = pltpu.get_barrier_semaphore()

    def signal(sem, grid, band):
        pl.semaphore_signal(sem, inc=1, device_id=(grid, band), device_id_type=MESH)

    meet = near + [(pair, 1 - b), (grid_up, b), (grid_down, b)]
    for grid, band in meet:
        signal(barrier, grid, band)

    def tell(step):
        for grid, band in near if step == 0 else friends:
            signal(known.at[step], grid, band)

    def hear(step):
        pl.semaphore_wait(known.at[step], len(near if step == 0 else friends))

    def remote(source, target, sent, received, grid, band):
        return pltpu.make_async_remote_copy(
            src_ref=source, dst_ref=target, send_sem=sent, recv_sem=received,
            device_id=(grid, band), device_id_type=MESH,
        )

    to_other = [
        remote(own_right.at[:, m], rights.at[1, c], y_send.at[m], y_recv.at[c], g - c + m, 1 - b)
        for m in range(2)
    ]
    to_pair = [
        remote(lefts.at[c], lefts.at[c], pair_send.at[0], pair_recv.at[0], pair, b),
        remote(own_right.at[:, 1 - c], rights.at[0, c], pair_send.at[1], pair_recv.at[1], pair, b),
    ]
    loads[0].wait()
    pl.semaphore_wait(barrier, len(meet))
    for copy in to_other:
        copy.start()
    loads[1].wait()
    for copy in to_pair:
        copy.start()
    tell(0)

    loads[2].wait()
    loads[3].wait()
    flipped = sphere[...].T
    ky_t[...] = (flipped >> 7) & 127
    val_t[...] = ((flipped >> 14) << 7) | (flipped & 127)
    rows = lax.broadcasted_iota(jnp.int32, (NG, NG), 0)

    def place(p, table):
        return jnp.where(ky_t[pl.ds(p, 1), :] == rows, val_t[pl.ds(p, 1), :], table)

    table = lax.fori_loop(0, NG, place, jnp.zeros((NG, NG), jnp.int32), unroll=8)
    kx_of[...] = table & 127
    kz = table >> 7
    cosine = jnp.broadcast_to(trig[0:1, :], (NG, NG))
    sine = jnp.broadcast_to(trig[1:2, :], (NG, NG))
    for core in range(2):
        angle = (kz * (g - c + core)) & 127
        phase[core, 0] = lanes(cosine, angle)
        phase[core, 1] = lanes(sine, angle)

    def along_rows(chunk, plane, half):
        right_real = rights[chunk, plane, 0]
        right_imag = rights[chunk, plane, 1]
        columns = []
        for n in (2 * half, 2 * half + 1):
            left_real = lefts[plane, 0, n]
            left_imag = lefts[plane, 1, n]
            field = jnp.concatenate(
                [
                    left_real * right_real + left_imag * right_imag,
                    left_real * right_imag - left_imag * right_real,
                ],
                axis=1,
            )
            high, low = split(field)
            moved = jnp.dot(
                jnp.concatenate([high, low, high], axis=1),
                along_x[...],
                preferred_element_type=F32,
            )
            columns.append(jnp.concatenate([moved[:, :NX], moved[:, NX:]], axis=0))
        return split(jnp.concatenate(columns, axis=1))

    def along_columns(rows):
        high, low = rows
        return jnp.dot(
            along_y[...], jnp.concatenate([high, high, low], axis=0), preferred_element_type=F32
        )

    def pick(plane, waves, half):
        index = kx_of[...]
        cosines, sines = phase[plane, 0], phase[plane, 1]
        picked = {}
        for at in range(2):
            real = lanes(waves[:NG, at * NX : (at + 1) * NX], index)
            imag = lanes(waves[NG:, at * NX : (at + 1) * NX], index)
            n = 2 * half + at
            picked[n] = real * cosines + imag * sines
            picked[n + 4] = imag * cosines - real * sines
        return picked

    def ship(chunk, channel, value):
        send[chunk, pl.ds(channel, NG, stride=8), :] = value.T

    def native_first(plane):
        for half in range(2):
            picked = pick(plane, along_columns(along_rows(0, plane, half)), half)
            for channel, value in picked.items():
                acc[channel] = value

    def native_second(plane):
        for half in range(2):
            picked = pick(plane, along_columns(along_rows(0, plane, half)), half)
            for channel, value in picked.items():
                ship(0, channel, acc[channel] + value)

    def distant_both():
        def total(half, waves):
            first, second = (pick(plane, waves[plane], half) for plane in range(2))
            for channel in first:
                ship(1, channel, first[channel] + second[channel])

        rows = [along_rows(1, plane, 0) for plane in range(2)]
        waves = [along_columns(value) for value in rows]
        rows = [along_rows(1, plane, 1) for plane in range(2)]
        total(0, waves)
        waves = [along_columns(value) for value in rows]
        total(1, waves)

    for load in loads[4:7]:
        load.wait()
    native_first(c)
    for copy in to_pair:
        copy.wait_recv()
    native_second(1 - c)

    def part(chunk, quarter, half):
        start = pl.multiple_of(quarter * QUARTER + half * HALF, HALF)
        return send.at[chunk, pl.ds(start, HALF)]

    def x_copies(chunk):
        sent, received = x_send.at[chunk], x_recv.at[chunk]
        return [
            remote(part(chunk, across, 0), from_a.at[chunk, 0], sent.at[0], received.at[0], grid_up, b),
            remote(part(chunk, across, 1), from_a.at[chunk, 1], sent.at[1], received.at[1], grid_down, b),
            remote(part(chunk, up, 1), from_b.at[chunk, 0], sent.at[2], received.at[2], grid_up, b),
            remote(part(chunk, down, 0), from_b.at[chunk, 1], sent.at[3], received.at[3], grid_down, b),
            remote(part(chunk, up, 0), from_c.at[chunk, 0], sent.at[4], received.at[4], grid_up, b),
            remote(part(chunk, down, 1), from_c.at[chunk, 1], sent.at[5], received.at[5], grid_down, b),
        ]

    def x_first(copies):
        for copy in copies[:2]:
            copy.start()

    def x_direct(copies):
        for copy in copies[2:4]:
            copy.start()

    def x_second(chunk, copies):
        for way, quarter in enumerate((up, down)):
            copies[way].wait_recv()
            ref = part(chunk, quarter, way)
            ref[...] = ref[...] + from_a[chunk, way]
            copies[4 + way].start()

    def z_first(chunk, copies):
        for copy in copies[2:]:
            copy.wait_recv()
        for half in range(2):
            x_sum[chunk, pl.ds(half * HALF, HALF)] = (
                part(chunk, x, half)[...] + from_c[chunk, half] + from_b[chunk, 1 - half]
            )
        mine = pl.ds(pl.multiple_of(j * 8, 8), 8)
        tiles[chunk, mine] = x_sum[chunk, mine]

        for away_z in (4, 3, 5, 2, 6, 1, 7, 0):
            for away in (2, 3, 0, 1):
                if (away_z, away) == (0, 0):
                    continue
                to = (
                    lax.rem(h + away // 2, AH) * AZ * AC
                    + lax.rem(z + away_z, AZ) * AC
                    + lax.rem(c + away % 2, AC)
                )
                theirs = pl.ds(pl.multiple_of(to * 8, 8), 8)
                remote(
                    x_sum.at[chunk, theirs], tiles.at[chunk, mine],
                    z_send.at[chunk], z_recv.at[chunk], x * SIDE + to, b,
                ).start()

    def z_wait(buffer, chunk, sem):
        many = buffer.at[chunk, pl.ds(0, (SIDE - 1) * 8)]
        pltpu.make_async_copy(many, many, sem.at[chunk]).wait()

    index = jnp.broadcast_to((sphere[pl.ds(g, 1), :] >> 7) & 127, (8, NG))
    factor = 1.0 / (NG * NG * NX) ** 0.5

    def z_last(chunk):
        z_wait(tiles, chunk, z_recv)
        values = []
        for core in range(2):
            total = tiles[chunk, pl.ds(core * 8, 8)]
            for chip in range(1, SIDE // 2):
                total = total + tiles[chunk, pl.ds((2 * chip + core) * 8, 8)]
            values.append(lanes(total, index) * factor)
        return values

    native = x_copies(0)
    distant = x_copies(1)
    x_first(native)
    x_direct(native)
    hear(0)
    tell(1)

    @pl.when(c == 1)
    def _():
        x_second(0, native)

    def arrival(core):
        return remote(
            own_right.at[:, 0], rights.at[1, core], y_send.at[0], y_recv.at[core], g, 1 - b
        )

    arrival(0).wait_recv()
    arrival(1).wait_recv()
    distant_both()
    x_first(distant)
    hear(1)
    tell(2)

    @pl.when(c == 0)
    def _():
        x_second(0, native)
        x_direct(distant)
        x_second(1, distant)

    @pl.when(c == 1)
    def _():
        x_direct(distant)

    hear(2)
    z_first(0, native)

    @pl.when(c == 1)
    def _():
        x_second(1, distant)

    z_first(1, distant)
    values = z_last(0)
    values = values + z_last(1)
    loads[7].wait()
    for column in range(4):
        position = jnp.full((8, NG), lax.rem(order[column] + 4 - 2 * b, 4), jnp.int32)
        value = values[3]
        for at in range(3):
            value = jnp.where(position == at, values[at], value)
        out_ref[pl.ds(column, 8, stride=4), :] = value

    for copy in to_pair + to_other + native + distant:
        copy.wait_send()
    for chunk in range(2):
        z_wait(x_sum, chunk, z_send)


def local(left_bands, right_bands, sphere_index, right_order):
    along_x, along_y, trig = dft_tables()
    hbm = pl.BlockSpec(memory_space=pltpu.HBM)
    dma = pltpu.SemaphoreType.DMA
    result = pl.pallas_call(
        kernel,
        name="pair_sums",
        out_shape=pltpu.VMEM((32, NG), F32),
        in_specs=[hbm] * 7,
        out_specs=pl.BlockSpec(memory_space=pltpu.VMEM),
        scratch_shapes=[
            pltpu.VMEM((2, 2, 4, NG, NX), F32),
            pltpu.VMEM((2, 2, 2, NG, NX), F32),
            pltpu.VMEM((2, 2, NG, NX), F32),
            pltpu.VMEM((NG, NG), jnp.int32),
            pltpu.VMEM((6 * NG, 2 * NG), BF16),
            pltpu.VMEM((2 * NG, 6 * NG), BF16),
            pltpu.VMEM((8, NG), F32),
            pltpu.VMEM((NG, NG), jnp.int32),
            pltpu.VMEM((NG, NG), jnp.int32),
            pltpu.VMEM((NG, NG), jnp.int32),
            pltpu.VMEM((2, 2, NG, NG), F32),
            pltpu.VMEM((8, NG, NG), F32),
            pltpu.VMEM((2, AX * QUARTER, NG), F32),
            pltpu.VMEM((2, 2, HALF, NG), F32),
            pltpu.VMEM((2, 2, HALF, NG), F32),
            pltpu.VMEM((2, 2, HALF, NG), F32),
            pltpu.VMEM((2, QUARTER, NG), F32),
            pltpu.VMEM((2, QUARTER, NG), F32),
            pltpu.SMEM((4,), jnp.int32),
            dma((8,)), dma((2,)), dma((2,)), dma((2,)), dma((2,)),
            dma((2, 6)), dma((2, 6)), dma((2,)), dma((2,)), pltpu.SemaphoreType.REGULAR((3,)),
        ],
        compiler_params=pltpu.CompilerParams(collective_id=0, has_side_effects=True),
    )(
        right_order,
        left_bands.reshape(2, 4, NG, NX),
        right_bands.reshape(2, 2, NG, NX),
        sphere_index.reshape(NG, NG),
        jnp.asarray(along_x),
        jnp.asarray(along_y),
        jnp.asarray(trig),
    )
    return result.reshape(2, 4, 4, NG)


def solution(mesh):
    placed = (P(None, "band", "grid", None, None), P(None, "band", "grid", None, None), P(), P())
    return jax.shard_map(
        local, mesh=mesh, in_specs=placed, out_specs=P(None, "band", None, "grid"), check_vma=False
    )
```

```python
import functools
import math

import jax
import jax.numpy as jnp
from jax import lax
from jax.experimental import pallas as pl
from jax.experimental.pallas import tpu as pltpu
from jax.sharding import PartitionSpec as P
import numpy as np

NG = 128
NX = 128
NGV = 16384
AX, AH, AZ, AC = 4, 2, 8, 2
SIDE = AH * AZ * AC
QUARTER = SIDE * 8
HALF = QUARTER // 2
PIECE = HALF // 2
PLACE = (0, 2, 1, 3)
MESH = pl.DeviceIdType.MESH
F32 = jnp.float32
BF16 = jnp.bfloat16


def split(value):
    high = value.astype(BF16)
    return high, (value - high.astype(F32)).astype(BF16)


def dft_tables():
    counter = np.arange(NG)
    angles = (counter[:, None] * counter[None, :] % NG) * (2.0 * math.pi / NG)
    cosine, sine = np.cos(angles), np.sin(angles)

    def halves(table):
        high = table.astype(np.float32).astype(BF16)
        low = (table - high.astype(np.float64)).astype(np.float32).astype(BF16)
        return high, low

    high, low = halves(np.block([[cosine, -sine], [sine, cosine]]))
    along_x = np.concatenate([high, high, low], axis=0)
    high, low = halves(np.block([[cosine, sine], [-sine, cosine]]))
    along_y = np.concatenate([high, low, high], axis=1)
    trig = np.zeros((8, NG), np.float32)
    trig[0], trig[1] = cosine[1], sine[1]
    return along_x, along_y, trig


def lanes(value, index):
    return jnp.take_along_axis(value, index, axis=1, mode="promise_in_bounds")


def kernel(
    order_ref, left_ref, right_ref, sphere_ref, along_x_ref, along_y_ref, trig_ref, out_ref,
    lefts, rights, own_right, sphere, along_x, along_y, trig,
    ky_t, val_t, kx_of, phase, acc, send, from_a, from_b, from_c, x_sum, tiles,
    order, load_sem, pair_send, pair_recv, y_send, y_recv, x_send, x_recv, z_send, z_recv, known,
):
    g = lax.axis_index("grid")
    b = lax.axis_index("band")
    c = lax.rem(g, AC)
    j = lax.rem(g, SIDE)
    x = lax.div(g, SIDE)
    up = lax.rem(x + 1, AX)
    down = lax.rem(x + AX - 1, AX)
    across = lax.rem(x + 2, AX)

    loads = [
        pltpu.make_async_copy(right_ref, own_right, load_sem.at[0]),
        pltpu.make_async_copy(left_ref, lefts.at[c], load_sem.at[1]),
        pltpu.make_async_copy(trig_ref, trig, load_sem.at[2]),
        pltpu.make_async_copy(right_ref.at[:, c], rights.at[0, c], load_sem.at[3]),
        pltpu.make_async_copy(along_x_ref, along_x, load_sem.at[4]),
        pltpu.make_async_copy(along_y_ref, along_y, load_sem.at[5]),
        pltpu.make_async_copy(order_ref, order, load_sem.at[6]),
    ]
    loads += [
        pltpu.make_async_copy(
            sphere_ref.at[:, at], sphere.at[:, PLACE[at]], load_sem.at[8 + at]
        )
        for at in range(4)
    ]
    for load in loads:
        load.start()

    grid_up = up * SIDE + j
    grid_down = down * SIDE + j
    pair = g + 1 - 2 * c
    h = lax.rem(lax.div(g, SIDE // 2), AH)
    z = lax.rem(lax.div(g, AC), AZ)
    q = lax.div(z, 4) * 16 + h * 8 + lax.rem(z, 4) * AC + c
    opposite = g + SIDE // 2 - SIDE * h
    along_z = [g + AC * (lax.rem(z + step, AZ) - z) for step in (1, AZ - 1, 2, AZ - 2)]
    near = [(along_z[0], b), (along_z[1], b), (pair, b), (g, 1 - b), (opposite, 1 - b)]
    friends = [(grid, b) for grid in along_z + [opposite, pair]]
    barrier = pltpu.get_barrier_semaphore()

    def signal(sem, grid, band):
        pl.semaphore_signal(sem, inc=1, device_id=(grid, band), device_id_type=MESH)

    meet = near + [(pair, 1 - b), (grid_up, b), (grid_down, b)]
    for grid, band in meet:
        signal(barrier, grid, band)

    def tell(step):
        for grid, band in near if step == 0 else friends:
            signal(known.at[step], grid, band)

    def hear(step):
        pl.semaphore_wait(known.at[step], len(near if step == 0 else friends))

    def remote(source, target, sent, received, grid, band):
        return pltpu.make_async_remote_copy(
            src_ref=source, dst_ref=target, send_sem=sent, recv_sem=received,
            device_id=(grid, band), device_id_type=MESH,
        )

    to_other = [
        remote(own_right.at[:, m], rights.at[1, c], y_send.at[m], y_recv.at[c], g - c + m, 1 - b)
        for m in range(2)
    ]
    to_pair = [
        remote(lefts.at[c], lefts.at[c], pair_send.at[0], pair_recv.at[0], pair, b),
        remote(own_right.at[:, 1 - c], rights.at[0, c], pair_send.at[1], pair_recv.at[1], pair, b),
    ]
    loads[0].wait()
    pl.semaphore_wait(barrier, len(meet))
    for copy in to_other:
        copy.start()
    loads[1].wait()
    for copy in to_pair:
        copy.start()
    tell(0)

    for load in loads[7:]:
        load.wait()
    loads[2].wait()
    flipped = sphere[...].reshape(NG, NG).T
    ky_t[...] = (flipped >> 7) & 127
    val_t[...] = ((flipped >> 14) << 7) | (flipped & 127)
    rows = lax.broadcasted_iota(jnp.int32, (NG, NG), 0)

    def place(p, table):
        return jnp.where(ky_t[pl.ds(p, 1), :] == rows, val_t[pl.ds(p, 1), :], table)

    table = lax.fori_loop(0, NG, place, jnp.zeros((NG, NG), jnp.int32), unroll=8)
    kx_of[...] = table & 127
    kz = table >> 7
    cosine = jnp.broadcast_to(trig[0:1, :], (NG, NG))
    sine = jnp.broadcast_to(trig[1:2, :], (NG, NG))
    for core in range(2):
        angle = (kz * (g - c + core)) & 127
        phase[core, 0] = lanes(cosine, angle)
        phase[core, 1] = lanes(sine, angle)

    def along_rows(chunk, plane, half):
        right_real = rights[chunk, plane, 0]
        right_imag = rights[chunk, plane, 1]
        columns = []
        for n in (2 * half, 2 * half + 1):
            left_real = lefts[plane, 0, n]
            left_imag = lefts[plane, 1, n]
            field = jnp.concatenate(
                [
                    left_real * right_real + left_imag * right_imag,
                    left_real * right_imag - left_imag * right_real,
                ],
                axis=1,
            )
            high, low = split(field)
            moved = jnp.dot(
                jnp.concatenate([high, low, high], axis=1),
                along_x[...],
                preferred_element_type=F32,
            )
            columns.append(jnp.concatenate([moved[:, :NX], moved[:, NX:]], axis=0))
        return split(jnp.concatenate(columns, axis=1))

    def along_columns(rows):
        high, low = rows
        return jnp.dot(
            along_y[...], jnp.concatenate([high, high, low], axis=0), preferred_element_type=F32
        )

    def pick(plane, waves, half):
        index = kx_of[...]
        cosines, sines = phase[plane, 0], phase[plane, 1]
        picked = {}
        for at in range(2):
            real = lanes(waves[:NG, at * NX : (at + 1) * NX], index)
            imag = lanes(waves[NG:, at * NX : (at + 1) * NX], index)
            n = 2 * half + at
            picked[n] = real * cosines + imag * sines
            picked[n + 4] = imag * cosines - real * sines
        return picked

    def ship(chunk, channel, value):
        send[chunk, pl.ds(channel, NG, stride=8), :] = value.T

    def native_first(plane):
        for half in range(2):
            picked = pick(plane, along_columns(along_rows(0, plane, half)), half)
            for channel, value in picked.items():
                acc[channel] = value

    def native_second(plane):
        for half in range(2):
            picked = pick(plane, along_columns(along_rows(0, plane, half)), half)
            for channel, value in picked.items():
                ship(0, channel, acc[channel] + value)

    def distant_both():
        def total(half, waves):
            first, second = (pick(plane, waves[plane], half) for plane in range(2))
            for channel in first:
                ship(1, channel, first[channel] + second[channel])

        rows = [along_rows(1, plane, 0) for plane in range(2)]
        waves = [along_columns(value) for value in rows]
        rows = [along_rows(1, plane, 1) for plane in range(2)]
        total(0, waves)
        waves = [along_columns(value) for value in rows]
        total(1, waves)

    for load in loads[3:6]:
        load.wait()
    native_first(c)
    hear(0)
    tell(1)
    for copy in to_pair:
        copy.wait_recv()
    native_second(1 - c)

    def part(chunk, quarter, late, way):
        start = pl.multiple_of(quarter * QUARTER + late * HALF + way * PIECE, PIECE)
        return send.at[chunk, pl.ds(start, PIECE)]

    class Hop:
        def __init__(self, chunk, late):
            self.at = chunk, late
            sent, received = x_send.at[chunk, late], x_recv.at[chunk, late]
            self.buffers = [ref.at[chunk, late] for ref in (from_a, from_b, from_c)]
            routes = (
                (across, 0, 0, grid_up), (across, 1, 0, grid_down),
                (up, 1, 1, grid_up), (down, 0, 1, grid_down),
                (up, 0, 2, grid_up), (down, 1, 2, grid_down),
            )
            self.copies = [
                remote(
                    part(chunk, quarter, late, way), self.buffers[kind].at[number % 2],
                    sent.at[number], received.at[number], to, b,
                )
                for number, (quarter, way, kind, to) in enumerate(routes)
            ]

        def first(self):
            for copy in self.copies[:2]:
                copy.start()

        def direct(self):
            for copy in self.copies[2:4]:
                copy.start()

        def second(self):
            for way, quarter in enumerate((up, down)):
                self.copies[way].wait_recv()
                ref = part(self.at[0], quarter, self.at[1], way)
                ref[...] = ref[...] + self.buffers[0][way]
                self.copies[4 + way].start()

        def spread(self):
            chunk, late = self.at
            for copy in self.copies[2:]:
                copy.wait_recv()
            for way in range(2):
                x_sum[chunk, pl.ds(late * HALF + way * PIECE, PIECE)] = (
                    part(chunk, x, late, way)[...]
                    + self.buffers[2][way]
                    + self.buffers[1][1 - way]
                )
            mine = pl.ds(pl.multiple_of(q * 8, 8), 8)
            for owner_z in ((0, 1, 2, 3), (4, 7, 5, 6))[late]:
                for owner_h in range(2):
                    for owner_c in (1, 0):
                        to = late * 16 + owner_h * 8 + owner_z % 4 * 2 + owner_c
                        theirs = pl.ds(to * 8, 8)
                        owner = x * SIDE + (owner_h * AZ + owner_z) * AC + owner_c

                        @pl.when(q != to)
                        def _(theirs=theirs, owner=owner):
                            remote(
                                x_sum.at[chunk, theirs], tiles.at[chunk, mine],
                                z_send.at[chunk], z_recv.at[chunk], owner, b,
                            ).start()

            @pl.when(lax.div(z, 4) == late)
            def _():
                tiles[chunk, mine] = x_sum[chunk, mine]

    def z_wait(buffer, chunk, sem):
        many = buffer.at[chunk, pl.ds(0, (SIDE - 1) * 8)]
        pltpu.make_async_copy(many, many, sem.at[chunk]).wait()

    own = sphere[x, lax.div(z, 4) * 2 + h, pl.ds(lax.rem(z, 4) * AC + c, 1), :]
    index = jnp.broadcast_to((own >> 7) & 127, (8, NG))
    factor = 1.0 / (NG * NG * NX) ** 0.5

    def z_last(chunk):
        z_wait(tiles, chunk, z_recv)
        values = []
        for core in range(2):
            total = tiles[chunk, pl.ds(core * 8, 8)]
            for chip in range(1, SIDE // 2):
                total = total + tiles[chunk, pl.ds((2 * chip + core) * 8, 8)]
            values.append(lanes(total, index) * factor)
        return values

    (native, native_late), (distant, distant_late) = (
        [Hop(chunk, late) for late in range(2)] for chunk in range(2)
    )
    native.first()
    native_late.first()
    native.direct()
    native_late.direct()

    @pl.when(c == 1)
    def _():
        native.second()
        native_late.second()
        hear(1)
        tell(2)

    def arrival(core):
        return remote(
            own_right.at[:, 0], rights.at[1, core], y_send.at[0], y_recv.at[core], g, 1 - b
        )

    arrival(0).wait_recv()
    arrival(1).wait_recv()

    @pl.when(c == 0)
    def _():
        hear(1)
        tell(2)

    distant_both()
    distant.first()

    @pl.when(c == 0)
    def _():
        native.second()
        native_late.second()

    distant.direct()
    distant_late.first()
    distant.second()
    distant_late.direct()
    hear(2)
    native.spread()
    distant_late.second()
    native_late.spread()
    distant.spread()
    distant_late.spread()
    values = z_last(0)
    values = values + z_last(1)
    loads[6].wait()
    for column in range(4):
        position = jnp.full((8, NG), lax.rem(order[column] + 4 - 2 * b, 4), jnp.int32)
        value = values[3]
        for at in range(3):
            value = jnp.where(position == at, values[at], value)
        out_ref[pl.ds(column, 8, stride=4), :] = value

    for copy in to_pair + to_other:
        copy.wait_send()
    for hop in (native, native_late, distant, distant_late):
        for copy in hop.copies:
            copy.wait_send()
    for chunk in range(2):
        z_wait(x_sum, chunk, z_send)


def local(left_bands, right_bands, sphere_index, right_order):
    along_x, along_y, trig = dft_tables()
    hbm = pl.BlockSpec(memory_space=pltpu.HBM)
    dma = pltpu.SemaphoreType.DMA
    result = pl.pallas_call(
        kernel,
        name="pair_sums",
        out_shape=pltpu.VMEM((32, NG), F32),
        in_specs=[hbm] * 7,
        out_specs=pl.BlockSpec(memory_space=pltpu.VMEM),
        scratch_shapes=[
            pltpu.VMEM((2, 2, 4, NG, NX), F32),
            pltpu.VMEM((2, 2, 2, NG, NX), F32),
            pltpu.VMEM((2, 2, NG, NX), F32),
            pltpu.VMEM((4, 4, 8, NG), jnp.int32),
            pltpu.VMEM((6 * NG, 2 * NG), BF16),
            pltpu.VMEM((2 * NG, 6 * NG), BF16),
            pltpu.VMEM((8, NG), F32),
            pltpu.VMEM((NG, NG), jnp.int32),
            pltpu.VMEM((NG, NG), jnp.int32),
            pltpu.VMEM((NG, NG), jnp.int32),
            pltpu.VMEM((2, 2, NG, NG), F32),
            pltpu.VMEM((8, NG, NG), F32),
            pltpu.VMEM((2, AX * QUARTER, NG), F32),
            pltpu.VMEM((2, 2, 2, PIECE, NG), F32),
            pltpu.VMEM((2, 2, 2, PIECE, NG), F32),
            pltpu.VMEM((2, 2, 2, PIECE, NG), F32),
            pltpu.VMEM((2, QUARTER, NG), F32),
            pltpu.VMEM((2, QUARTER, NG), F32),
            pltpu.SMEM((4,), jnp.int32),
            dma((12,)), dma((2,)), dma((2,)), dma((2,)), dma((2,)),
            dma((2, 2, 6)), dma((2, 2, 6)), dma((2,)), dma((2,)), pltpu.SemaphoreType.REGULAR((3,)),
        ],
        compiler_params=pltpu.CompilerParams(collective_id=0, has_side_effects=True),
    )(
        right_order,
        left_bands.reshape(2, 4, NG, NX),
        right_bands.reshape(2, 2, NG, NX),
        sphere_index.reshape(4, 4, 8, NG),
        jnp.asarray(along_x),
        jnp.asarray(along_y),
        jnp.asarray(trig),
    )
    return result.reshape(2, 4, 4, NG)


def solution(mesh):
    placed = (P(None, "band", "grid", None, None), P(None, "band", "grid", None, None), P(), P())
    return jax.shard_map(
        local, mesh=mesh, in_specs=placed, out_specs=P(None, "band", None, "grid"), check_vma=False
    )
```

```python
import functools
import math

import jax
import jax.numpy as jnp
from jax import lax
from jax.experimental import pallas as pl
from jax.experimental.pallas import tpu as pltpu
from jax.sharding import PartitionSpec as P
import numpy as np

NG = 128
NX = 128
NGV = 16384
AX, AH, AZ, AC = 4, 2, 8, 2
SIDE = AH * AZ * AC
QUARTER = SIDE * 8
HALF = QUARTER // 2
PIECE = HALF // 2
PLACE = (0, 2, 1, 3)
MESH = pl.DeviceIdType.MESH
F32 = jnp.float32
BF16 = jnp.bfloat16


def split(value):
    high = value.astype(BF16)
    return high, (value - high.astype(F32)).astype(BF16)


def dft_tables():
    counter = np.arange(NG)
    angles = (counter[:, None] * counter[None, :] % NG) * (2.0 * math.pi / NG)
    cosine, sine = np.cos(angles), np.sin(angles)

    def halves(table):
        high = table.astype(np.float32).astype(BF16)
        low = (table - high.astype(np.float64)).astype(np.float32).astype(BF16)
        return high, low

    high, low = halves(np.block([[cosine, -sine], [sine, cosine]]))
    along_x = np.concatenate([high, high, low], axis=0)
    high, low = halves(np.block([[cosine, sine], [-sine, cosine]]))
    along_y = np.concatenate([high, low, high], axis=1)
    trig = np.zeros((8, NG), np.float32)
    trig[0], trig[1] = cosine[1], sine[1]
    return along_x, along_y, trig


def lanes(value, index):
    return jnp.take_along_axis(value, index, axis=1, mode="promise_in_bounds")


def kernel(
    order_ref, left_ref, right_ref, sphere_ref, along_x_ref, along_y_ref, trig_ref, out_ref,
    lefts, rights, own_right, sphere, along_x, along_y, trig,
    ky_t, val_t, kx_of, phase, acc, send, from_a, from_b, from_c, x_sum, tiles,
    order, load_sem, pair_send, pair_recv, y_send, y_recv, x_send, x_recv, z_send, z_recv, known,
):
    g = lax.axis_index("grid")
    b = lax.axis_index("band")
    c = lax.rem(g, AC)
    j = lax.rem(g, SIDE)
    x = lax.div(g, SIDE)
    up = lax.rem(x + 1, AX)
    down = lax.rem(x + AX - 1, AX)
    across = lax.rem(x + 2, AX)

    loads = [
        pltpu.make_async_copy(right_ref, own_right, load_sem.at[0]),
        pltpu.make_async_copy(left_ref, lefts.at[c], load_sem.at[1]),
        pltpu.make_async_copy(trig_ref, trig, load_sem.at[2]),
        pltpu.make_async_copy(right_ref.at[:, c], rights.at[0, c], load_sem.at[3]),
        pltpu.make_async_copy(along_x_ref, along_x, load_sem.at[4]),
        pltpu.make_async_copy(along_y_ref, along_y, load_sem.at[5]),
        pltpu.make_async_copy(order_ref, order, load_sem.at[6]),
    ]
    loads += [
        pltpu.make_async_copy(
            sphere_ref.at[:, at], sphere.at[:, PLACE[at]], load_sem.at[8 + at]
        )
        for at in range(4)
    ]
    for load in loads:
        load.start()

    grid_up = up * SIDE + j
    grid_down = down * SIDE + j
    pair = g + 1 - 2 * c
    h = lax.rem(lax.div(g, SIDE // 2), AH)
    z = lax.rem(lax.div(g, AC), AZ)
    q = lax.div(z, 4) * 16 + h * 8 + lax.rem(z, 4) * AC + c
    opposite = g + SIDE // 2 - SIDE * h
    along_z = [(g + AC * (lax.rem(z + step, AZ) - z), b) for step in (1, AZ - 1, 2, AZ - 2)]
    close = [(pair, b), (g, 1 - b), (pair, 1 - b)]
    near = along_z[:2] + [(grid_up, b), (grid_down, b), (opposite, 1 - b)]
    barrier = pltpu.get_barrier_semaphore()

    def signal(sem, devices):
        for grid, band in devices:
            pl.semaphore_signal(sem, inc=1, device_id=(grid, band), device_id_type=MESH)

    signal(barrier, close)

    @pl.when(c == 1)
    def _():
        signal(barrier, near)

    def tell(step):
        others = near + [(g, 1 - b)] if step == 0 else along_z + [(opposite, b)]

        @pl.when(c == 1)
        def _():
            signal(known.at[step], [(pair, b)] + others)

    def hear(step):
        pl.semaphore_wait(known.at[step], jnp.where(c == 1, 6 if step == 0 else 5, 1))

    def remote(source, target, sent, received, grid, band):
        return pltpu.make_async_remote_copy(
            src_ref=source, dst_ref=target, send_sem=sent, recv_sem=received,
            device_id=(grid, band), device_id_type=MESH,
        )

    to_other = [
        remote(own_right.at[:, m], rights.at[1, c], y_send.at[m], y_recv.at[c], g - c + m, 1 - b)
        for m in range(2)
    ]
    to_pair = [
        remote(lefts.at[c], lefts.at[c], pair_send.at[0], pair_recv.at[0], pair, b),
        remote(own_right.at[:, 1 - c], rights.at[0, c], pair_send.at[1], pair_recv.at[1], pair, b),
    ]
    loads[0].wait()
    pl.semaphore_wait(barrier, jnp.where(c == 1, len(close) + len(near), len(close)))
    for copy in to_other:
        copy.start()
    loads[1].wait()
    for copy in to_pair:
        copy.start()
    tell(0)

    for load in loads[7:]:
        load.wait()
    loads[2].wait()
    flipped = sphere[...].reshape(NG, NG).T
    ky_t[...] = (flipped >> 7) & 127
    val_t[...] = ((flipped >> 14) << 7) | (flipped & 127)
    rows = lax.broadcasted_iota(jnp.int32, (NG, NG), 0)

    def place(p, table):
        return jnp.where(ky_t[pl.ds(p, 1), :] == rows, val_t[pl.ds(p, 1), :], table)

    table = lax.fori_loop(0, NG, place, jnp.zeros((NG, NG), jnp.int32), unroll=8)
    kx_of[...] = table & 127
    kz = table >> 7
    cosine = jnp.broadcast_to(trig[0:1, :], (NG, NG))
    sine = jnp.broadcast_to(trig[1:2, :], (NG, NG))
    for core in range(2):
        angle = (kz * (g - c + core)) & 127
        phase[core, 0] = lanes(cosine, angle)
        phase[core, 1] = lanes(sine, angle)

    def along_rows(chunk, plane, half):
        right_real = rights[chunk, plane, 0]
        right_imag = rights[chunk, plane, 1]
        columns = []
        for n in (2 * half, 2 * half + 1):
            left_real = lefts[plane, 0, n]
            left_imag = lefts[plane, 1, n]
            field = jnp.concatenate(
                [
                    left_real * right_real + left_imag * right_imag,
                    left_real * right_imag - left_imag * right_real,
                ],
                axis=1,
            )
            high, low = split(field)
            moved = jnp.dot(
                jnp.concatenate([high, low, high], axis=1),
                along_x[...],
                preferred_element_type=F32,
            )
            columns.append(jnp.concatenate([moved[:, :NX], moved[:, NX:]], axis=0))
        return split(jnp.concatenate(columns, axis=1))

    def along_columns(rows):
        high, low = rows
        return jnp.dot(
            along_y[...], jnp.concatenate([high, high, low], axis=0), preferred_element_type=F32
        )

    def pick(plane, waves, half):
        index = kx_of[...]
        cosines, sines = phase[plane, 0], phase[plane, 1]
        picked = {}
        for at in range(2):
            real = lanes(waves[:NG, at * NX : (at + 1) * NX], index)
            imag = lanes(waves[NG:, at * NX : (at + 1) * NX], index)
            n = 2 * half + at
            picked[n] = real * cosines + imag * sines
            picked[n + 4] = imag * cosines - real * sines
        return picked

    def ship(chunk, channel, value):
        send[chunk, pl.ds(channel, NG, stride=8), :] = value.T

    def native_first(plane):
        for half in range(2):
            picked = pick(plane, along_columns(along_rows(0, plane, half)), half)
            for channel, value in picked.items():
                acc[channel] = value

    def native_second(plane):
        for half in range(2):
            picked = pick(plane, along_columns(along_rows(0, plane, half)), half)
            for channel, value in picked.items():
                ship(0, channel, acc[channel] + value)

    def distant_both():
        def total(half, waves):
            first, second = (pick(plane, waves[plane], half) for plane in range(2))
            for channel in first:
                ship(1, channel, first[channel] + second[channel])

        rows = [along_rows(1, plane, 0) for plane in range(2)]
        waves = [along_columns(value) for value in rows]
        rows = [along_rows(1, plane, 1) for plane in range(2)]
        total(0, waves)
        waves = [along_columns(value) for value in rows]
        total(1, waves)

    for load in loads[3:6]:
        load.wait()
    native_first(c)
    hear(0)
    tell(1)
    for copy in to_pair:
        copy.wait_recv()
    native_second(1 - c)

    def part(chunk, quarter, late, way):
        start = pl.multiple_of(quarter * QUARTER + late * HALF + way * PIECE, PIECE)
        return send.at[chunk, pl.ds(start, PIECE)]

    class Hop:
        def __init__(self, chunk, late):
            self.at = chunk, late
            sent, received = x_send.at[chunk, late], x_recv.at[chunk, late]
            self.buffers = [ref.at[chunk, late] for ref in (from_a, from_b, from_c)]
            routes = (
                (across, 0, 0, grid_up), (across, 1, 0, grid_down),
                (up, 1, 1, grid_up), (down, 0, 1, grid_down),
                (up, 0, 2, grid_up), (down, 1, 2, grid_down),
            )
            self.copies = [
                remote(
                    part(chunk, quarter, late, way), self.buffers[kind].at[number % 2],
                    sent.at[number], received.at[number], to, b,
                )
                for number, (quarter, way, kind, to) in enumerate(routes)
            ]

        def first(self):
            for copy in self.copies[:2]:
                copy.start()

        def direct(self):
            for copy in self.copies[2:4]:
                copy.start()

        def second(self):
            for way, quarter in enumerate((up, down)):
                self.copies[way].wait_recv()
                ref = part(self.at[0], quarter, self.at[1], way)
                ref[...] = ref[...] + self.buffers[0][way]
                self.copies[4 + way].start()

        def spread(self):
            chunk, late = self.at
            for copy in self.copies[2:]:
                copy.wait_recv()
            for way in range(2):
                x_sum[chunk, pl.ds(late * HALF + way * PIECE, PIECE)] = (
                    part(chunk, x, late, way)[...]
                    + self.buffers[2][way]
                    + self.buffers[1][1 - way]
                )
            mine = pl.ds(pl.multiple_of(q * 8, 8), 8)
            for owner_z in ((0, 1, 2, 3), (4, 7, 5, 6))[late]:
                for owner_h in range(2):
                    for owner_c in (1, 0):
                        to = late * 16 + owner_h * 8 + owner_z % 4 * 2 + owner_c
                        theirs = pl.ds(to * 8, 8)
                        owner = x * SIDE + (owner_h * AZ + owner_z) * AC + owner_c

                        @pl.when(q != to)
                        def _(theirs=theirs, owner=owner):
                            remote(
                                x_sum.at[chunk, theirs], tiles.at[chunk, mine],
                                z_send.at[chunk], z_recv.at[chunk], owner, b,
                            ).start()

            @pl.when(lax.div(z, 4) == late)
            def _():
                tiles[chunk, mine] = x_sum[chunk, mine]

    def z_wait(buffer, chunk, sem):
        many = buffer.at[chunk, pl.ds(0, (SIDE - 1) * 8)]
        pltpu.make_async_copy(many, many, sem.at[chunk]).wait()

    own = sphere[x, lax.div(z, 4) * 2 + h, pl.ds(lax.rem(z, 4) * AC + c, 1), :]
    index = jnp.broadcast_to((own >> 7) & 127, (8, NG))
    factor = 1.0 / (NG * NG * NX) ** 0.5

    def z_last(chunk):
        z_wait(tiles, chunk, z_recv)
        values = []
        for core in range(2):
            total = tiles[chunk, pl.ds(core * 8, 8)]
            for chip in range(1, SIDE // 2):
                total = total + tiles[chunk, pl.ds((2 * chip + core) * 8, 8)]
            values.append(lanes(total, index) * factor)
        return values

    (native, native_late), (distant, distant_late) = (
        [Hop(chunk, late) for late in range(2)] for chunk in range(2)
    )

    @pl.when(c == 0)
    def _():
        hear(1)

    native.first()
    native_late.first()
    native.direct()
    native_late.direct()

    @pl.when(c == 1)
    def _():
        hear(1)
        tell(2)
        native.second()
        native_late.second()

    def arrival(core):
        return remote(
            own_right.at[:, 0], rights.at[1, core], y_send.at[0], y_recv.at[core], g, 1 - b
        )

    arrival(0).wait_recv()
    arrival(1).wait_recv()
    @pl.when(c == 1)
    def _():
        hear(2)
        tell(3)

    distant_both()
    distant.first()

    @pl.when(c == 0)
    def _():
        native.second()
        native_late.second()
        distant_late.first()
        distant.direct()
        hear(2)
        distant.second()
        hear(3)
        native.spread()
        native_late.spread()

    @pl.when(c == 1)
    def _():
        hear(3)
        native.spread()
        distant_late.first()
        distant.direct()
        native_late.spread()
        distant.second()

    distant.spread()
    distant_late.direct()
    distant_late.second()
    distant_late.spread()
    values = z_last(0)
    values = values + z_last(1)
    loads[6].wait()
    for column in range(4):
        position = jnp.full((8, NG), lax.rem(order[column] + 4 - 2 * b, 4), jnp.int32)
        value = values[3]
        for at in range(3):
            value = jnp.where(position == at, values[at], value)
        out_ref[pl.ds(column, 8, stride=4), :] = value

    for copy in to_pair + to_other:
        copy.wait_send()
    for hop in (native, native_late, distant, distant_late):
        for copy in hop.copies:
            copy.wait_send()
    for chunk in range(2):
        z_wait(x_sum, chunk, z_send)


def local(left_bands, right_bands, sphere_index, right_order):
    along_x, along_y, trig = dft_tables()
    hbm = pl.BlockSpec(memory_space=pltpu.HBM)
    dma = pltpu.SemaphoreType.DMA
    result = pl.pallas_call(
        kernel,
        name="pair_sums",
        out_shape=pltpu.VMEM((32, NG), F32),
        in_specs=[hbm] * 7,
        out_specs=pl.BlockSpec(memory_space=pltpu.VMEM),
        scratch_shapes=[
            pltpu.VMEM((2, 2, 4, NG, NX), F32),
            pltpu.VMEM((2, 2, 2, NG, NX), F32),
            pltpu.VMEM((2, 2, NG, NX), F32),
            pltpu.VMEM((4, 4, 8, NG), jnp.int32),
            pltpu.VMEM((6 * NG, 2 * NG), BF16),
            pltpu.VMEM((2 * NG, 6 * NG), BF16),
            pltpu.VMEM((8, NG), F32),
            pltpu.VMEM((NG, NG), jnp.int32),
            pltpu.VMEM((NG, NG), jnp.int32),
            pltpu.VMEM((NG, NG), jnp.int32),
            pltpu.VMEM((2, 2, NG, NG), F32),
            pltpu.VMEM((8, NG, NG), F32),
            pltpu.VMEM((2, AX * QUARTER, NG), F32),
            pltpu.VMEM((2, 2, 2, PIECE, NG), F32),
            pltpu.VMEM((2, 2, 2, PIECE, NG), F32),
            pltpu.VMEM((2, 2, 2, PIECE, NG), F32),
            pltpu.VMEM((2, QUARTER, NG), F32),
            pltpu.VMEM((2, QUARTER, NG), F32),
            pltpu.SMEM((4,), jnp.int32),
            dma((12,)), dma((2,)), dma((2,)), dma((2,)), dma((2,)),
            dma((2, 2, 6)), dma((2, 2, 6)), dma((2,)), dma((2,)), pltpu.SemaphoreType.REGULAR((4,)),
        ],
        compiler_params=pltpu.CompilerParams(collective_id=0, has_side_effects=True),
    )(
        right_order,
        left_bands.reshape(2, 4, NG, NX),
        right_bands.reshape(2, 2, NG, NX),
        sphere_index.reshape(4, 4, 8, NG),
        jnp.asarray(along_x),
        jnp.asarray(along_y),
        jnp.asarray(trig),
    )
    return result.reshape(2, 4, 4, NG)


def solution(mesh):
    placed = (P(None, "band", "grid", None, None), P(None, "band", "grid", None, None), P(), P())
    return jax.shard_map(
        local, mesh=mesh, in_specs=placed, out_specs=P(None, "band", None, "grid"), check_vma=False
    )
```

```python
import functools
import math

import jax
import jax.numpy as jnp
from jax import lax
from jax.experimental import pallas as pl
from jax.experimental.pallas import tpu as pltpu
from jax.sharding import PartitionSpec as P
import numpy as np

NG = 128
NX = 128
NGV = 16384
AX, AH, AZ, AC = 4, 2, 8, 2
SIDE = AH * AZ * AC
QUARTER = SIDE * 8
HALF = QUARTER // 2
PIECE = HALF // 2
PLACE = (0, 2, 1, 3)
MESH = pl.DeviceIdType.MESH
F32 = jnp.float32
BF16 = jnp.bfloat16


def split(value):
    high = value.astype(BF16)
    return high, (value - high.astype(F32)).astype(BF16)


def dft_tables():
    counter = np.arange(NG)
    angles = (counter[:, None] * counter[None, :] % NG) * (2.0 * math.pi / NG)
    cosine, sine = np.cos(angles), np.sin(angles)

    def halves(table):
        high = table.astype(np.float32).astype(BF16)
        low = (table - high.astype(np.float64)).astype(np.float32).astype(BF16)
        return high, low

    high, low = halves(np.block([[cosine, -sine], [sine, cosine]]))
    along_x = np.concatenate([high, high, low], axis=0)
    high, low = halves(np.block([[cosine, sine], [-sine, cosine]]))
    along_y = np.concatenate([high, low, high], axis=1)
    trig = np.zeros((8, NG), np.float32)
    trig[0], trig[1] = cosine[1], sine[1]
    return along_x, along_y, trig


def lanes(value, index):
    return jnp.take_along_axis(value, index, axis=1, mode="promise_in_bounds")


def kernel(
    order_ref, left_ref, right_ref, sphere_ref, along_x_ref, along_y_ref, trig_ref, out_ref,
    lefts, rights, own_right, sphere, along_x, along_y, trig,
    ky_t, val_t, kx_of, phase, acc, send, from_a, from_b, from_c, from_all, x_sum, tiles,
    order, load_sem, pair_send, pair_recv, y_send, y_recv, x_send, x_recv, z_send, z_recv, known,
):
    g = lax.axis_index("grid")
    b = lax.axis_index("band")
    c = lax.rem(g, AC)
    j = lax.rem(g, SIDE)
    x = lax.div(g, SIDE)
    up = lax.rem(x + 1, AX)
    down = lax.rem(x + AX - 1, AX)
    across = lax.rem(x + 2, AX)

    loads = [
        pltpu.make_async_copy(right_ref, own_right, load_sem.at[0]),
        pltpu.make_async_copy(left_ref, lefts.at[c], load_sem.at[1]),
        pltpu.make_async_copy(trig_ref, trig, load_sem.at[2]),
        pltpu.make_async_copy(right_ref.at[:, c], rights.at[0, c], load_sem.at[3]),
        pltpu.make_async_copy(along_x_ref, along_x, load_sem.at[4]),
        pltpu.make_async_copy(along_y_ref, along_y, load_sem.at[5]),
        pltpu.make_async_copy(order_ref, order, load_sem.at[6]),
    ]
    loads += [
        pltpu.make_async_copy(
            sphere_ref.at[:, at], sphere.at[:, PLACE[at]], load_sem.at[8 + at]
        )
        for at in range(4)
    ]
    for load in loads:
        load.start()

    grid_up = up * SIDE + j
    grid_down = down * SIDE + j
    pair = g + 1 - 2 * c
    h = lax.rem(lax.div(g, SIDE // 2), AH)
    z = lax.rem(lax.div(g, AC), AZ)
    q = lax.div(z, 4) * 16 + h * 8 + lax.rem(z, 4) * AC + c
    opposite = g + SIDE // 2 - SIDE * h
    along_z = [(g + AC * (lax.rem(z + step, AZ) - z), b) for step in (1, AZ - 1, 2, AZ - 2)]
    close = [(pair, b), (g, 1 - b), (pair, 1 - b)]
    near = along_z[:2] + [(grid_up, b), (grid_down, b), (opposite, 1 - b)]
    barrier = pltpu.get_barrier_semaphore()

    def signal(sem, devices):
        for grid, band in devices:
            pl.semaphore_signal(sem, inc=1, device_id=(grid, band), device_id_type=MESH)

    signal(barrier, close)

    @pl.when(c == 1)
    def _():
        signal(barrier, near)

    def tell(step):
        others = near + [(g, 1 - b)] if step == 0 else along_z + near[2:4] + [(opposite, b)]

        @pl.when(c == 1)
        def _():
            signal(known.at[step], [(pair, b)] + others)

    def hear(step):
        pl.semaphore_wait(known.at[step], jnp.where(c == 1, 6 if step == 0 else 7, 1))

    def remote(source, target, sent, received, grid, band):
        return pltpu.make_async_remote_copy(
            src_ref=source, dst_ref=target, send_sem=sent, recv_sem=received,
            device_id=(grid, band), device_id_type=MESH,
        )

    to_other = [
        remote(own_right.at[:, m], rights.at[1, c], y_send.at[m], y_recv.at[c], g - c + m, 1 - b)
        for m in range(2)
    ]
    to_pair = [
        remote(lefts.at[c], lefts.at[c], pair_send.at[0], pair_recv.at[0], pair, b),
        remote(own_right.at[:, 1 - c], rights.at[0, c], pair_send.at[1], pair_recv.at[1], pair, b),
    ]
    loads[0].wait()
    pl.semaphore_wait(barrier, jnp.where(c == 1, len(close) + len(near), len(close)))
    for copy in to_other:
        copy.start()
    loads[1].wait()
    for copy in to_pair:
        copy.start()
    tell(0)

    for load in loads[7:]:
        load.wait()
    loads[2].wait()
    flipped = sphere[...].reshape(NG, NG).T
    ky_t[...] = (flipped >> 7) & 127
    val_t[...] = ((flipped >> 14) << 7) | (flipped & 127)
    rows = lax.broadcasted_iota(jnp.int32, (NG, NG), 0)

    def place(p, table):
        return jnp.where(ky_t[pl.ds(p, 1), :] == rows, val_t[pl.ds(p, 1), :], table)

    table = lax.fori_loop(0, NG, place, jnp.zeros((NG, NG), jnp.int32), unroll=8)
    kx_of[...] = table & 127
    kz = table >> 7
    cosine = jnp.broadcast_to(trig[0:1, :], (NG, NG))
    sine = jnp.broadcast_to(trig[1:2, :], (NG, NG))
    for core in range(2):
        angle = (kz * (g - c + core)) & 127
        phase[core, 0] = lanes(cosine, angle)
        phase[core, 1] = lanes(sine, angle)

    def along_rows(chunk, plane, half):
        right_real = rights[chunk, plane, 0]
        right_imag = rights[chunk, plane, 1]
        columns = []
        for n in (2 * half, 2 * half + 1):
            left_real = lefts[plane, 0, n]
            left_imag = lefts[plane, 1, n]
            field = jnp.concatenate(
                [
                    left_real * right_real + left_imag * right_imag,
                    left_real * right_imag - left_imag * right_real,
                ],
                axis=1,
            )
            high, low = split(field)
            moved = jnp.dot(
                jnp.concatenate([high, low, high], axis=1),
                along_x[...],
                preferred_element_type=F32,
            )
            columns.append(jnp.concatenate([moved[:, :NX], moved[:, NX:]], axis=0))
        return split(jnp.concatenate(columns, axis=1))

    def along_columns(rows):
        high, low = rows
        return jnp.dot(
            along_y[...], jnp.concatenate([high, high, low], axis=0), preferred_element_type=F32
        )

    def pick(plane, waves, half):
        index = kx_of[...]
        cosines, sines = phase[plane, 0], phase[plane, 1]
        picked = {}
        for at in range(2):
            real = lanes(waves[:NG, at * NX : (at + 1) * NX], index)
            imag = lanes(waves[NG:, at * NX : (at + 1) * NX], index)
            n = 2 * half + at
            picked[n] = real * cosines + imag * sines
            picked[n + 4] = imag * cosines - real * sines
        return picked

    def ship(chunk, channel, value):
        send[chunk, pl.ds(channel, NG, stride=8), :] = value.T

    def native_first(plane):
        for half in range(2):
            picked = pick(plane, along_columns(along_rows(0, plane, half)), half)
            for channel, value in picked.items():
                acc[channel] = value

    def native_second(plane):
        for half in range(2):
            picked = pick(plane, along_columns(along_rows(0, plane, half)), half)
            for channel, value in picked.items():
                ship(0, channel, acc[channel] + value)

    def distant_both():
        def total(half, waves):
            first, second = (pick(plane, waves[plane], half) for plane in range(2))
            for channel in first:
                ship(1, channel, first[channel] + second[channel])

        rows = [along_rows(1, plane, 0) for plane in range(2)]
        waves = [along_columns(value) for value in rows]
        rows = [along_rows(1, plane, 1) for plane in range(2)]
        total(0, waves)
        waves = [along_columns(value) for value in rows]
        total(1, waves)

    for load in loads[3:6]:
        load.wait()
    native_first(c)
    hear(0)
    tell(1)
    for copy in to_pair:
        copy.wait_recv()
    native_second(1 - c)

    def part(chunk, quarter, late, way):
        start = pl.multiple_of(quarter * QUARTER + late * HALF + way * PIECE, PIECE)
        return send.at[chunk, pl.ds(start, PIECE)]

    def whole(quarter, late):
        start = pl.multiple_of(quarter * QUARTER + late * HALF, HALF)
        return send.at[1, pl.ds(start, HALF)]

    def send_tiles(chunk, late):
        mine = pl.ds(pl.multiple_of(q * 8, 8), 8)
        for owner_z in ((0, 1, 2, 3), (4, 7, 5, 6))[late]:
            for owner_h in range(2):
                for owner_c in (1, 0):
                    to = late * 16 + owner_h * 8 + owner_z % 4 * 2 + owner_c
                    theirs = pl.ds(to * 8, 8)
                    owner = x * SIDE + (owner_h * AZ + owner_z) * AC + owner_c

                    @pl.when(q != to)
                    def _(theirs=theirs, owner=owner):
                        remote(
                            x_sum.at[chunk, theirs], tiles.at[chunk, mine],
                            z_send.at[chunk], z_recv.at[chunk], owner, b,
                        ).start()

        @pl.when(lax.div(z, 4) == late)
        def _():
            tiles[chunk, mine] = x_sum[chunk, mine]

    class Relay:
        def __init__(self, late):
            self.late = late
            sent, received = x_send.at[0, late], x_recv.at[0, late]
            self.buffers = [ref.at[late] for ref in (from_a, from_b, from_c)]
            routes = (
                (across, 0, 0, grid_up), (across, 1, 0, grid_down),
                (up, 1, 1, grid_up), (down, 0, 1, grid_down),
                (up, 0, 2, grid_up), (down, 1, 2, grid_down),
            )
            self.copies = [
                remote(
                    part(0, quarter, late, way), self.buffers[kind].at[number % 2],
                    sent.at[number], received.at[number], to, b,
                )
                for number, (quarter, way, kind, to) in enumerate(routes)
            ]

        def first(self):
            for copy in self.copies[:2]:
                copy.start()

        def direct(self):
            for copy in self.copies[2:4]:
                copy.start()

        def second(self):
            for way, quarter in enumerate((up, down)):
                self.copies[way].wait_recv()
                ref = part(0, quarter, self.late, way)
                ref[...] = ref[...] + self.buffers[0][way]
                self.copies[4 + way].start()

        def spread(self):
            for copy in self.copies[2:]:
                copy.wait_recv()
            for way in range(2):
                x_sum[0, pl.ds(self.late * HALF + way * PIECE, PIECE)] = (
                    part(0, x, self.late, way)[...]
                    + self.buffers[2][way]
                    + self.buffers[1][1 - way]
                )
            send_tiles(0, self.late)

    class Direct:
        def __init__(self, late):
            self.late = late
            routes = ((across, across * SIDE + j), (up, grid_up), (down, grid_down))
            self.copies = [
                remote(
                    whole(quarter, late), from_all.at[late, number],
                    x_send.at[1, late, number], x_recv.at[1, late, number], to, b,
                )
                for number, (quarter, to) in enumerate(routes)
            ]

        def start(self):
            for copy in self.copies:
                copy.start()

        def spread(self):
            for copy in self.copies:
                copy.wait_recv()
            x_sum[1, pl.ds(self.late * HALF, HALF)] = (
                whole(x, self.late)[...]
                + from_all[self.late, 0]
                + (from_all[self.late, 1] + from_all[self.late, 2])
            )
            send_tiles(1, self.late)

    def z_wait(buffer, chunk, sem):
        many = buffer.at[chunk, pl.ds(0, (SIDE - 1) * 8)]
        pltpu.make_async_copy(many, many, sem.at[chunk]).wait()

    own = sphere[x, lax.div(z, 4) * 2 + h, pl.ds(lax.rem(z, 4) * AC + c, 1), :]
    index = jnp.broadcast_to((own >> 7) & 127, (8, NG))
    factor = 1.0 / (NG * NG * NX) ** 0.5

    def z_last(chunk):
        z_wait(tiles, chunk, z_recv)
        values = []
        for core in range(2):
            total = tiles[chunk, pl.ds(core * 8, 8)]
            for chip in range(1, SIDE // 2):
                total = total + tiles[chunk, pl.ds((2 * chip + core) * 8, 8)]
            values.append(lanes(total, index) * factor)
        return values

    native, native_late = Relay(0), Relay(1)
    distant, distant_late = Direct(0), Direct(1)

    @pl.when(c == 0)
    def _():
        hear(1)

    native.first()
    native_late.first()
    native.direct()
    native_late.direct()

    @pl.when(c == 1)
    def _():
        hear(1)
        tell(2)
        native.second()
        native_late.second()

    def arrival(core):
        return remote(
            own_right.at[:, 0], rights.at[1, core], y_send.at[0], y_recv.at[core], g, 1 - b
        )

    arrival(0).wait_recv()
    arrival(1).wait_recv()
    @pl.when(c == 1)
    def _():
        hear(2)
        tell(3)

    distant_both()

    @pl.when(c == 0)
    def _():
        hear(2)

    @pl.when(c == 0)
    def _():
        native.second()
        distant.start()
        native_late.second()

    @pl.when(c == 1)
    def _():
        distant.start()

    hear(3)
    native.spread()

    @pl.when(c == 1)
    def _():
        native_late.spread()

    distant.spread()
    distant_late.start()

    @pl.when(c == 0)
    def _():
        native_late.spread()

    distant_late.spread()
    values = z_last(0)
    values = values + z_last(1)
    loads[6].wait()
    for column in range(4):
        position = jnp.full((8, NG), lax.rem(order[column] + 4 - 2 * b, 4), jnp.int32)
        value = values[3]
        for at in range(3):
            value = jnp.where(position == at, values[at], value)
        out_ref[pl.ds(column, 8, stride=4), :] = value

    for copy in to_pair + to_other:
        copy.wait_send()
    for hop in (native, native_late, distant, distant_late):
        for copy in hop.copies:
            copy.wait_send()
    for chunk in range(2):
        z_wait(x_sum, chunk, z_send)


def local(left_bands, right_bands, sphere_index, right_order):
    along_x, along_y, trig = dft_tables()
    hbm = pl.BlockSpec(memory_space=pltpu.HBM)
    dma = pltpu.SemaphoreType.DMA
    result = pl.pallas_call(
        kernel,
        name="pair_sums",
        out_shape=pltpu.VMEM((32, NG), F32),
        in_specs=[hbm] * 7,
        out_specs=pl.BlockSpec(memory_space=pltpu.VMEM),
        scratch_shapes=[
            pltpu.VMEM((2, 2, 4, NG, NX), F32),
            pltpu.VMEM((2, 2, 2, NG, NX), F32),
            pltpu.VMEM((2, 2, NG, NX), F32),
            pltpu.VMEM((4, 4, 8, NG), jnp.int32),
            pltpu.VMEM((6 * NG, 2 * NG), BF16),
            pltpu.VMEM((2 * NG, 6 * NG), BF16),
            pltpu.VMEM((8, NG), F32),
            pltpu.VMEM((NG, NG), jnp.int32),
            pltpu.VMEM((NG, NG), jnp.int32),
            pltpu.VMEM((NG, NG), jnp.int32),
            pltpu.VMEM((2, 2, NG, NG), F32),
            pltpu.VMEM((8, NG, NG), F32),
            pltpu.VMEM((2, AX * QUARTER, NG), F32),
            pltpu.VMEM((2, 2, PIECE, NG), F32),
            pltpu.VMEM((2, 2, PIECE, NG), F32),
            pltpu.VMEM((2, 2, PIECE, NG), F32),
            pltpu.VMEM((2, 3, HALF, NG), F32),
            pltpu.VMEM((2, QUARTER, NG), F32),
            pltpu.VMEM((2, QUARTER, NG), F32),
            pltpu.SMEM((4,), jnp.int32),
            dma((12,)), dma((2,)), dma((2,)), dma((2,)), dma((2,)),
            dma((2, 2, 6)), dma((2, 2, 6)), dma((2,)), dma((2,)), pltpu.SemaphoreType.REGULAR((4,)),
        ],
        compiler_params=pltpu.CompilerParams(collective_id=0, has_side_effects=True),
    )(
        right_order,
        left_bands.reshape(2, 4, NG, NX),
        right_bands.reshape(2, 2, NG, NX),
        sphere_index.reshape(4, 4, 8, NG),
        jnp.asarray(along_x),
        jnp.asarray(along_y),
        jnp.asarray(trig),
    )
    return result.reshape(2, 4, 4, NG)


def solution(mesh):
    placed = (P(None, "band", "grid", None, None), P(None, "band", "grid", None, None), P(), P())
    return jax.shard_map(
        local, mesh=mesh, in_specs=placed, out_specs=P(None, "band", None, "grid"), check_vma=False
    )
```

```python
import functools
import math

import jax
import jax.numpy as jnp
from jax import lax
from jax.experimental import pallas as pl
from jax.experimental.pallas import tpu as pltpu
from jax.sharding import PartitionSpec as P
import numpy as np

NG = 128
NX = 128
NGV = 16384
AX, AH, AZ, AC = 4, 2, 8, 2
SIDE = AH * AZ * AC
QUARTER = SIDE * 8
HALF = QUARTER // 2
PIECE = HALF // 2
PLACE = (0, 2, 1, 3)
Y_ROWS = (6 * NG, 8 * NG, 10 * NG)
MESH = pl.DeviceIdType.MESH
F32 = jnp.float32
BF16 = jnp.bfloat16


def split(value):
    high = value.astype(BF16)
    return high, (value - high.astype(F32)).astype(BF16)


def dft_tables():
    counter = np.arange(NG)
    angles = (counter[:, None] * counter[None, :] % NG) * (2.0 * math.pi / NG)
    cosine, sine = np.cos(angles), np.sin(angles)

    def halves(table):
        high = table.astype(np.float32).astype(BF16)
        low = (table - high.astype(np.float64)).astype(np.float32).astype(BF16)
        return high, low

    high, low = halves(np.block([[cosine, -sine], [sine, cosine]]))
    along_x = np.concatenate([high, high, low], axis=0)
    high, low = halves(np.block([[cosine, sine], [-sine, cosine]]))
    along_y = np.concatenate([high, low, high], axis=0)
    trig = np.zeros((8, NG), np.float32)
    trig[0], trig[1] = cosine[1], sine[1]
    return np.concatenate([along_x, along_y], axis=0), trig


def lanes(value, index):
    return jnp.take_along_axis(value, index, axis=1, mode="promise_in_bounds")


def kernel(
    order_ref, left_ref, right_ref, sphere_ref, table_ref, trig_ref, out_ref,
    lefts, rights, own_right, sphere, dft, trig,
    ky_t, val_t, kx_of, phase, acc, send, from_a, from_bc, from_all, x_sum, tiles,
    order, load_sem, pair_send, pair_recv, y_send, y_recv, native_send, native_recv, distant_send, distant_recv,
    z_send, z_recv, known,
):
    g = lax.axis_index("grid")
    b = lax.axis_index("band")
    c = lax.rem(g, AC)
    j = lax.rem(g, SIDE)
    x = lax.div(g, SIDE)
    up = lax.rem(x + 1, AX)
    down = lax.rem(x + AX - 1, AX)
    across = lax.rem(x + 2, AX)

    loads = [
        pltpu.make_async_copy(right_ref, own_right, load_sem.at[0]),
        pltpu.make_async_copy(left_ref, lefts.at[c], load_sem.at[1]),
        pltpu.make_async_copy(trig_ref, trig, load_sem.at[2]),
        pltpu.make_async_copy(right_ref.at[:, c], rights.at[0, c], load_sem.at[3]),
        pltpu.make_async_copy(table_ref, dft, load_sem.at[4]),
        pltpu.make_async_copy(order_ref, order, load_sem.at[5]),
    ]
    sphere_loads = [
        pltpu.make_async_copy(sphere_ref.at[:, at], sphere.at[:, PLACE[at]], load_sem.at[6])
        for at in range(4)
    ]
    for load in loads[:1] + sphere_loads + loads[1:]:
        load.start()

    grid_up = up * SIDE + j
    grid_down = down * SIDE + j
    pair = g + 1 - 2 * c
    h = lax.rem(lax.div(g, SIDE // 2), AH)
    z = lax.rem(lax.div(g, AC), AZ)
    q = lax.div(z, 4) * 16 + h * 8 + lax.rem(z, 4) * AC + c
    opposite = g + SIDE // 2 - SIDE * h
    along_z = [(g + AC * (lax.rem(z + step, AZ) - z), b) for step in (1, AZ - 1, 2, AZ - 2)]
    close = [(pair, b), (g, 1 - b), (pair, 1 - b)]
    near = along_z[:2] + [(grid_up, b), (grid_down, b), (opposite, 1 - b)]
    barrier = pltpu.get_barrier_semaphore()

    def signal(sem, devices):
        for grid, band in devices:
            pl.semaphore_signal(sem, inc=1, device_id=(grid, band), device_id_type=MESH)

    signal(barrier, close)

    @pl.when(c == 1)
    def _():
        signal(barrier, near)

    def tell(step):
        others = near + [(g, 1 - b)] if step == 0 else along_z + near[2:4] + [(opposite, b)]

        @pl.when(c == 1)
        def _():
            signal(known.at[step], [(pair, b)] + others)

    def hear(step):
        pl.semaphore_wait(known.at[step], jnp.where(c == 1, 6 if step == 0 else 7, 1))

    def remote(source, target, sent, received, grid, band):
        return pltpu.make_async_remote_copy(
            src_ref=source, dst_ref=target, send_sem=sent, recv_sem=received,
            device_id=(grid, band), device_id_type=MESH,
        )

    to_other = [
        remote(own_right.at[:, m], rights.at[1, c], y_send, y_recv.at[c], g - c + m, 1 - b)
        for m in range(2)
    ]
    to_pair = [
        remote(lefts.at[c], lefts.at[c], pair_send.at[0], pair_recv.at[0], pair, b),
        remote(own_right.at[:, 1 - c], rights.at[0, c], pair_send.at[1], pair_recv.at[1], pair, b),
    ]
    loads[0].wait()
    pl.semaphore_wait(barrier, jnp.where(c == 1, len(close) + len(near), len(close)))
    for copy in to_other:
        copy.start()
    loads[1].wait()
    for copy in to_pair:
        copy.start()
    tell(0)

    pltpu.make_async_copy(sphere, sphere, load_sem.at[6]).wait()
    loads[2].wait()
    flipped = sphere[...].reshape(NG, NG).T
    ky_t[...] = (flipped >> 7) & 127
    val_t[...] = ((flipped >> 14) << 7) | (flipped & 127)
    rows = lax.broadcasted_iota(jnp.int32, (NG, NG), 0)

    def place(p, table):
        return jnp.where(ky_t[pl.ds(p, 1), :] == rows, val_t[pl.ds(p, 1), :], table)

    table = lax.fori_loop(0, NG, place, jnp.zeros((NG, NG), jnp.int32), unroll=8)
    kx_of[...] = table & 127
    kz = table >> 7
    cosine = jnp.broadcast_to(trig[0:1, :], (NG, NG))
    sine = jnp.broadcast_to(trig[1:2, :], (NG, NG))
    for core in range(2):
        angle = (kz * (g - c + core)) & 127
        phase[core, 0] = lanes(cosine, angle)
        phase[core, 1] = lanes(sine, angle)

    def along_rows(chunk, plane, half):
        right_real = rights[chunk, plane, 0]
        right_imag = rights[chunk, plane, 1]
        columns = []
        for n in (2 * half, 2 * half + 1):
            left_real = lefts[plane, 0, n]
            left_imag = lefts[plane, 1, n]
            field = jnp.concatenate(
                [
                    left_real * right_real + left_imag * right_imag,
                    left_real * right_imag - left_imag * right_real,
                ],
                axis=1,
            )
            high, low = split(field)
            moved = jnp.dot(
                jnp.concatenate([high, low, high], axis=1),
                dft[: 6 * NG, :],
                preferred_element_type=F32,
            )
            columns.append(jnp.concatenate([moved[:, :NX], moved[:, NX:]], axis=0))
        return split(jnp.concatenate(columns, axis=1))

    def along_columns(rows):
        high, low = rows
        return jnp.dot(
            jnp.concatenate([dft[start : start + 2 * NG, :] for start in Y_ROWS], axis=1),
            jnp.concatenate([high, high, low], axis=0),
            preferred_element_type=F32,
        )

    def pick(plane, waves, half):
        index = kx_of[...]
        cosines, sines = phase[plane, 0], phase[plane, 1]
        picked = {}
        for at in range(2):
            real = lanes(waves[:NG, at * NX : (at + 1) * NX], index)
            imag = lanes(waves[NG:, at * NX : (at + 1) * NX], index)
            n = 2 * half + at
            picked[n] = real * cosines + imag * sines
            picked[n + 4] = imag * cosines - real * sines
        return picked

    def ship(chunk, channel, value):
        send[chunk, pl.ds(channel, NG, stride=8), :] = value.T

    def native_first(plane):
        for half in range(2):
            picked = pick(plane, along_columns(along_rows(0, plane, half)), half)
            for channel, value in picked.items():
                acc[channel] = value

    def native_second(plane):
        for half in range(2):
            picked = pick(plane, along_columns(along_rows(0, plane, half)), half)
            for channel, value in picked.items():
                ship(0, channel, acc[channel] + value)

    def distant_both():
        def total(half, waves):
            first, second = (pick(plane, waves[plane], half) for plane in range(2))
            for channel in first:
                ship(1, channel, first[channel] + second[channel])

        rows = [along_rows(1, plane, 0) for plane in range(2)]
        waves = [along_columns(value) for value in rows]
        rows = [along_rows(1, plane, 1) for plane in range(2)]
        total(0, waves)
        waves = [along_columns(value) for value in rows]
        total(1, waves)

    for load in loads[3:5]:
        load.wait()
    native_first(c)
    hear(0)
    tell(1)
    for copy in to_pair:
        copy.wait_recv()
    native_second(1 - c)

    def part(chunk, quarter, late, way):
        start = pl.multiple_of(quarter * QUARTER + late * HALF + way * PIECE, PIECE)
        return send.at[chunk, pl.ds(start, PIECE)]

    def send_tiles(chunk, places):
        mine = pl.ds(pl.multiple_of(q * 8, 8), 8)
        for to in places:
            owner_z = to // 16 * 4 + to % 8 // AC
            theirs = pl.ds(to * 8, 8)
            owner = x * SIDE + (to % 16 // 8 * AZ + owner_z) * AC + to % AC

            @pl.when(q != to)
            def _(theirs=theirs, owner=owner):
                remote(
                    x_sum.at[chunk, theirs], tiles.at[chunk, mine],
                    z_send.at[chunk], z_recv.at[chunk], owner, b,
                ).start()

        @pl.when(functools.reduce(jnp.logical_or, [q == to for to in places]))
        def _():
            tiles[chunk, mine] = x_sum[chunk, mine]

    class Relay:
        def __init__(self, late):
            self.late = late
            self.added = from_a.at[late]
            self.last = from_bc.at[late]
            routes = (
                (across, 0, self.added.at[0], 0, grid_up),
                (across, 1, self.added.at[1], 1, grid_down),
                (up, 1, self.last.at[0], 2, grid_up),
                (down, 0, self.last.at[1], 2, grid_down),
                (up, 0, self.last.at[2], 2, grid_up),
                (down, 1, self.last.at[3], 2, grid_down),
            )
            self.copies = [
                remote(
                    part(0, quarter, late, way), target, native_send,
                    native_recv.at[late, number], to, b,
                )
                for quarter, way, target, number, to in routes
            ]

        def first(self):
            for copy in self.copies[:2]:
                copy.start()

        def direct(self):
            for copy in self.copies[2:4]:
                copy.start()

        def second(self):
            for way, quarter in enumerate((up, down)):
                self.copies[way].wait_recv()
                ref = part(0, quarter, self.late, way)
                ref[...] = ref[...] + self.added[way]
                self.copies[4 + way].start()

        def spread(self):
            pltpu.make_async_copy(self.last, self.last, native_recv.at[self.late, 2]).wait()
            for way in range(2):
                x_sum[0, pl.ds(self.late * HALF + way * PIECE, PIECE)] = (
                    part(0, x, self.late, way)[...] + self.last[2 + way] + self.last[1 - way]
                )
            send_tiles(
                0,
                [
                    self.late * 16 + way * 8 + AC * at + core
                    for at in range(4)
                    for way in range(2)
                    for core in (1, 0)
                ],
            )

    class Direct:
        def __init__(self, number, first, count):
            self.places = range(first, first + count)
            self.rows = pl.ds(first * 8, count * 8)
            self.received = distant_recv.at[number]

        def of_quarter(self, quarter):
            start = pl.multiple_of(quarter * QUARTER + self.rows.start, 8)
            return send.at[1, pl.ds(start, self.rows.size)]

        def start(self):
            for owner_x in (0, 1, 3, 2):

                @pl.when(x != owner_x)
                def _(owner_x=owner_x):
                    number = lax.rem(x - owner_x + AX, AX) - 1
                    remote(
                        self.of_quarter(owner_x), from_all.at[number, self.rows],
                        distant_send, self.received, owner_x * SIDE + j, b,
                    ).start()

        def spread(self):
            arrived = from_all.at[:, self.rows]
            pltpu.make_async_copy(arrived, arrived, self.received).wait()
            x_sum[1, self.rows] = (
                self.of_quarter(x)[...]
                + from_all[1, self.rows]
                + (from_all[0, self.rows] + from_all[2, self.rows])
            )
            send_tiles(1, self.places)

    def z_wait(buffer, chunk, sem):
        many = buffer.at[chunk, pl.ds(0, (SIDE - 1) * 8)]
        pltpu.make_async_copy(many, many, sem.at[chunk]).wait()

    own = sphere[x, lax.div(z, 4) * 2 + h, pl.ds(lax.rem(z, 4) * AC + c, 1), :]
    index = jnp.broadcast_to((own >> 7) & 127, (8, NG))
    factor = 1.0 / (NG * NG * NX) ** 0.5

    def z_last(chunk):
        z_wait(tiles, chunk, z_recv)
        values = []
        for core in range(2):
            total = tiles[chunk, pl.ds(core * 8, 8)]
            for chip in range(1, SIDE // 2):
                total = total + tiles[chunk, pl.ds((2 * chip + core) * 8, 8)]
            values.append(lanes(total, index) * factor)
        return values

    native, native_late = Relay(0), Relay(1)
    distant = [
        Direct(number, first, count)
        for number, (first, count) in enumerate(((0, 2), (2, 6), (8, 8), (16, 16)))
    ]

    @pl.when(c == 0)
    def _():
        hear(1)

    native.first()
    native_late.first()
    native.direct()
    native_late.direct()

    @pl.when(c == 1)
    def _():
        hear(1)
        tell(2)
        native.second()
        native_late.second()

    def arrival(core):
        return remote(
            own_right.at[:, 0], rights.at[1, core], y_send, y_recv.at[core], g, 1 - b
        )

    arrival(0).wait_recv()
    arrival(1).wait_recv()
    @pl.when(c == 1)
    def _():
        hear(2)
        tell(3)

    distant_both()

    @pl.when(c == 0)
    def _():
        hear(2)

    distant[0].start()

    @pl.when(c == 0)
    def _():
        native.second()
        distant[1].start()
        distant[2].start()
        native_late.second()

    @pl.when(c == 1)
    def _():
        distant[1].start()

    hear(3)
    native.spread()

    @pl.when(c == 1)
    def _():
        distant[2].start()
        native_late.spread()

    @pl.when(jnp.logical_or(c == 0, z < 4))
    def _():
        distant[3].start()

    distant[0].spread()
    distant[1].spread()
    distant[2].spread()

    @pl.when(jnp.logical_and(c == 1, z >= 4))
    def _():
        distant[3].start()

    @pl.when(c == 0)
    def _():
        native_late.spread()

    distant[3].spread()
    values = z_last(0)
    values = values + z_last(1)
    loads[5].wait()
    for column in range(4):
        position = jnp.full((8, NG), lax.rem(order[column] + 4 - 2 * b, 4), jnp.int32)
        value = values[3]
        for at in range(3):
            value = jnp.where(position == at, values[at], value)
        out_ref[pl.ds(column, 8, stride=4), :] = value

    for copy in to_pair:
        copy.wait_send()
    pltpu.make_async_copy(own_right, own_right, y_send).wait()
    for chunk, sem in enumerate((native_send, distant_send)):
        sent = send.at[chunk, pl.ds(0, 3 * QUARTER)]
        pltpu.make_async_copy(sent, sent, sem).wait()
    for chunk in range(2):
        z_wait(x_sum, chunk, z_send)


def local(left_bands, right_bands, sphere_index, right_order):
    table, trig = dft_tables()
    hbm = pl.BlockSpec(memory_space=pltpu.HBM)
    dma = pltpu.SemaphoreType.DMA
    result = pl.pallas_call(
        kernel,
        name="pair_sums",
        out_shape=pltpu.VMEM((32, NG), F32),
        in_specs=[hbm] * 6,
        out_specs=pl.BlockSpec(memory_space=pltpu.VMEM),
        scratch_shapes=[
            pltpu.VMEM((2, 2, 4, NG, NX), F32),
            pltpu.VMEM((2, 2, 2, NG, NX), F32),
            pltpu.VMEM((2, 2, NG, NX), F32),
            pltpu.VMEM((4, 4, 8, NG), jnp.int32),
            pltpu.VMEM((12 * NG, 2 * NG), BF16),
            pltpu.VMEM((8, NG), F32),
            pltpu.VMEM((NG, NG), jnp.int32),
            pltpu.VMEM((NG, NG), jnp.int32),
            pltpu.VMEM((NG, NG), jnp.int32),
            pltpu.VMEM((2, 2, NG, NG), F32),
            pltpu.VMEM((8, NG, NG), F32),
            pltpu.VMEM((2, AX * QUARTER, NG), F32),
            pltpu.VMEM((2, 2, PIECE, NG), F32),
            pltpu.VMEM((2, 4, PIECE, NG), F32),
            pltpu.VMEM((3, QUARTER, NG), F32),
            pltpu.VMEM((2, QUARTER, NG), F32),
            pltpu.VMEM((2, QUARTER, NG), F32),
            pltpu.SMEM((4,), jnp.int32),
            dma((7,)), dma((2,)), dma((2,)), dma, dma((2,)), dma, dma((2, 3)), dma, dma((4,)),
            dma((2,)), dma((2,)), pltpu.SemaphoreType.REGULAR((4,)),
        ],
        compiler_params=pltpu.CompilerParams(collective_id=0, has_side_effects=True),
    )(
        right_order,
        left_bands.reshape(2, 4, NG, NX),
        right_bands.reshape(2, 2, NG, NX),
        sphere_index.reshape(4, 4, 8, NG),
        jnp.asarray(table),
        jnp.asarray(trig),
    )
    return result.reshape(2, 4, 4, NG)


def solution(mesh):
    placed = (P(None, "band", "grid", None, None), P(None, "band", "grid", None, None), P(), P())
    return jax.shard_map(
        local, mesh=mesh, in_specs=placed, out_specs=P(None, "band", None, "grid"), check_vma=False
    )
```

```python
import functools
import math

import jax
import jax.numpy as jnp
from jax import lax
from jax.experimental import pallas as pl
from jax.experimental.pallas import tpu as pltpu
from jax.sharding import PartitionSpec as P
import numpy as np

NG = 128
NX = 128
NGV = 16384
AX, AH, AZ, AC = 4, 2, 8, 2
SIDE = AH * AZ * AC
QUARTER = SIDE * 8
HALF = QUARTER // 2
PIECE = HALF // 2
PLACE = (0, 2, 1, 3)
Y_ROWS = (6 * NG, 8 * NG, 10 * NG)
MESH = pl.DeviceIdType.MESH
F32 = jnp.float32
BF16 = jnp.bfloat16


def split(value):
    high = value.astype(BF16)
    return high, (value - high.astype(F32)).astype(BF16)


def dft_tables():
    counter = np.arange(NG)
    angles = (counter[:, None] * counter[None, :] % NG) * (2.0 * math.pi / NG)
    cosine, sine = np.cos(angles), np.sin(angles)

    def halves(table):
        high = table.astype(np.float32).astype(BF16)
        low = (table - high.astype(np.float64)).astype(np.float32).astype(BF16)
        return high, low

    high, low = halves(np.block([[cosine, -sine], [sine, cosine]]))
    along_x = np.concatenate([high, high, low], axis=0)
    high, low = halves(np.block([[cosine, sine], [-sine, cosine]]))
    along_y = np.concatenate([high, low, high], axis=0)
    trig = np.zeros((8, NG), np.float32)
    trig[0], trig[1] = cosine[1], sine[1]
    return np.concatenate([along_x, along_y], axis=0), trig


def lanes(value, index):
    return jnp.take_along_axis(value, index, axis=1, mode="promise_in_bounds")


def kernel(
    order_ref, left_ref, right_ref, sphere_ref, table_ref, trig_ref, out_ref,
    lefts, rights, own_right, sphere, dft, trig,
    ky_t, val_t, kx_of, phase, acc, send, from_a, from_bc, from_all, x_sum, tiles,
    order, load_sem, pair_send, pair_recv, y_send, y_recv, native_send, native_recv, distant_send, distant_recv,
    z_send, z_recv, known,
):
    g = lax.axis_index("grid")
    b = lax.axis_index("band")
    c = lax.rem(g, AC)
    j = lax.rem(g, SIDE)
    x = lax.div(g, SIDE)
    up = lax.rem(x + 1, AX)
    down = lax.rem(x + AX - 1, AX)
    across = lax.rem(x + 2, AX)

    loads = [
        pltpu.make_async_copy(right_ref, own_right, load_sem.at[0]),
        pltpu.make_async_copy(left_ref, lefts.at[c], load_sem.at[1]),
        pltpu.make_async_copy(trig_ref, trig, load_sem.at[2]),
        pltpu.make_async_copy(right_ref.at[:, c], rights.at[0, c], load_sem.at[3]),
        pltpu.make_async_copy(table_ref, dft, load_sem.at[4]),
        pltpu.make_async_copy(order_ref, order, load_sem.at[5]),
    ]
    sphere_loads = [
        pltpu.make_async_copy(sphere_ref.at[:, at], sphere.at[:, PLACE[at]], load_sem.at[6])
        for at in range(4)
    ]
    for load in loads[:1] + sphere_loads + loads[1:]:
        load.start()

    grid_up = up * SIDE + j
    grid_down = down * SIDE + j
    pair = g + 1 - 2 * c
    h = lax.rem(lax.div(g, SIDE // 2), AH)
    z = lax.rem(lax.div(g, AC), AZ)
    q = lax.div(z, 4) * 16 + h * 8 + lax.rem(z, 4) * AC + c
    opposite = g + SIDE // 2 - SIDE * h
    along_z = [(g + AC * (lax.rem(z + step, AZ) - z), b) for step in (1, AZ - 1, 2, AZ - 2)]
    close = [(pair, b), (g, 1 - b), (pair, 1 - b)]
    near = along_z[:2] + [(grid_up, b), (grid_down, b), (opposite, 1 - b)]
    barrier = pltpu.get_barrier_semaphore()

    def signal(sem, devices):
        for grid, band in devices:
            pl.semaphore_signal(sem, inc=1, device_id=(grid, band), device_id_type=MESH)

    signal(barrier, close)

    @pl.when(c == 1)
    def _():
        signal(barrier, near)

    def tell(step):
        others = near + [(g, 1 - b)] if step == 0 else along_z + near[2:4] + [(opposite, b)]

        @pl.when(c == 1)
        def _():
            signal(known.at[step], [(pair, b)] + others)

    def hear(step):
        pl.semaphore_wait(known.at[step], jnp.where(c == 1, 6 if step == 0 else 7, 1))

    def remote(source, target, sent, received, grid, band):
        return pltpu.make_async_remote_copy(
            src_ref=source, dst_ref=target, send_sem=sent, recv_sem=received,
            device_id=(grid, band), device_id_type=MESH,
        )

    to_other = [
        remote(own_right.at[:, m], rights.at[1, c], y_send, y_recv.at[c], g - c + m, 1 - b)
        for m in range(2)
    ]
    to_pair = [
        remote(lefts.at[c], lefts.at[c], pair_send.at[0], pair_recv.at[0], pair, b),
        remote(own_right.at[:, 1 - c], rights.at[0, c], pair_send.at[1], pair_recv.at[1], pair, b),
    ]
    loads[0].wait()
    pl.semaphore_wait(barrier, jnp.where(c == 1, len(close) + len(near), len(close)))
    for copy in to_other:
        copy.start()
    loads[1].wait()
    for copy in to_pair:
        copy.start()
    tell(0)

    pltpu.make_async_copy(sphere, sphere, load_sem.at[6]).wait()
    loads[2].wait()
    flipped = sphere[...].reshape(NG, NG).T
    ky_t[...] = (flipped >> 7) & 127
    val_t[...] = ((flipped >> 14) << 7) | (flipped & 127)
    rows = lax.broadcasted_iota(jnp.int32, (NG, NG), 0)

    def place(p, table):
        return jnp.where(ky_t[pl.ds(p, 1), :] == rows, val_t[pl.ds(p, 1), :], table)

    table = lax.fori_loop(0, NG, place, jnp.zeros((NG, NG), jnp.int32), unroll=8)
    kx_of[...] = table & 127
    kz = table >> 7
    cosine = jnp.broadcast_to(trig[0:1, :], (NG, NG))
    sine = jnp.broadcast_to(trig[1:2, :], (NG, NG))
    for core in range(2):
        angle = (kz * (g - c + core)) & 127
        phase[core, 0] = lanes(cosine, angle)
        phase[core, 1] = lanes(sine, angle)

    def along_rows(chunk, plane, half):
        right_real = rights[chunk, plane, 0]
        right_imag = rights[chunk, plane, 1]
        fields = []
        for n in (2 * half, 2 * half + 1):
            left_real = lefts[plane, 0, n]
            left_imag = lefts[plane, 1, n]
            fields.append(
                jnp.concatenate(
                    [
                        left_real * right_real + left_imag * right_imag,
                        left_real * right_imag - left_imag * right_real,
                    ],
                    axis=1,
                )
            )
        high, low = split(jnp.concatenate(fields, axis=0))
        moved = jnp.dot(
            jnp.concatenate([high, low, high], axis=1), dft[: 6 * NG, :], preferred_element_type=F32
        )
        columns = [
            jnp.concatenate([moved[start : start + NG, :NX], moved[start : start + NG, NX:]], axis=0)
            for start in (0, NG)
        ]
        return split(jnp.concatenate(columns, axis=1))

    def along_columns(rows):
        high, low = rows
        return jnp.dot(
            jnp.concatenate([dft[start : start + 2 * NG, :] for start in Y_ROWS], axis=1),
            jnp.concatenate([high, high, low], axis=0),
            preferred_element_type=F32,
        )

    def pick(plane, waves, half):
        index = kx_of[...]
        cosines, sines = phase[plane, 0], phase[plane, 1]
        picked = {}
        for at in range(2):
            real = lanes(waves[:NG, at * NX : (at + 1) * NX], index)
            imag = lanes(waves[NG:, at * NX : (at + 1) * NX], index)
            n = 2 * half + at
            picked[n] = real * cosines + imag * sines
            picked[n + 4] = imag * cosines - real * sines
        return picked

    def ship(chunk, channel, value):
        send[chunk, pl.ds(channel, NG, stride=8), :] = value.T

    def native_first(plane):
        for half in range(2):
            picked = pick(plane, along_columns(along_rows(0, plane, half)), half)
            for channel, value in picked.items():
                acc[channel] = value

    def native_second(plane):
        for half in range(2):
            picked = pick(plane, along_columns(along_rows(0, plane, half)), half)
            for channel, value in picked.items():
                ship(0, channel, acc[channel] + value)

    def distant_both():
        def total(half, waves):
            first, second = (pick(plane, waves[plane], half) for plane in range(2))
            for channel in first:
                ship(1, channel, first[channel] + second[channel])

        rows = [along_rows(1, plane, half) for half in range(2) for plane in range(2)]
        waves = [along_columns(value) for value in rows]
        total(0, waves[:2])
        total(1, waves[2:])

    for load in loads[3:5]:
        load.wait()
    native_first(c)
    hear(0)
    tell(1)
    for copy in to_pair:
        copy.wait_recv()
    native_second(1 - c)

    def part(chunk, quarter, late, way):
        start = pl.multiple_of(quarter * QUARTER + late * HALF + way * PIECE, PIECE)
        return send.at[chunk, pl.ds(start, PIECE)]

    def send_tiles(chunk, places):
        mine = pl.ds(pl.multiple_of(q * 8, 8), 8)
        for to in places:
            owner_z = to // 16 * 4 + to % 8 // AC
            theirs = pl.ds(to * 8, 8)
            owner = x * SIDE + (to % 16 // 8 * AZ + owner_z) * AC + to % AC

            @pl.when(q != to)
            def _(theirs=theirs, owner=owner):
                remote(
                    x_sum.at[chunk, theirs], tiles.at[chunk, mine],
                    z_send.at[chunk], z_recv.at[chunk], owner, b,
                ).start()

        @pl.when(functools.reduce(jnp.logical_or, [q == to for to in places]))
        def _():
            tiles[chunk, mine] = x_sum[chunk, mine]

    class Relay:
        def __init__(self, late):
            self.late = late
            self.added = from_a.at[late]
            self.last = from_bc.at[late]
            routes = (
                (across, 0, self.added.at[0], 0, grid_up),
                (across, 1, self.added.at[1], 1, grid_down),
                (up, 1, self.last.at[0], 2, grid_up),
                (down, 0, self.last.at[1], 2, grid_down),
                (up, 0, self.last.at[2], 2, grid_up),
                (down, 1, self.last.at[3], 2, grid_down),
            )
            self.copies = [
                remote(
                    part(0, quarter, late, way), target, native_send,
                    native_recv.at[late, number], to, b,
                )
                for quarter, way, target, number, to in routes
            ]

        def first(self):
            for copy in self.copies[:2]:
                copy.start()

        def direct(self):
            for copy in self.copies[2:4]:
                copy.start()

        def second(self):
            for way, quarter in enumerate((up, down)):
                self.copies[way].wait_recv()
                ref = part(0, quarter, self.late, way)
                ref[...] = ref[...] + self.added[way]
                self.copies[4 + way].start()

        def spread(self):
            pltpu.make_async_copy(self.last, self.last, native_recv.at[self.late, 2]).wait()
            for way in range(2):
                x_sum[0, pl.ds(self.late * HALF + way * PIECE, PIECE)] = (
                    part(0, x, self.late, way)[...] + self.last[2 + way] + self.last[1 - way]
                )
            send_tiles(
                0,
                [
                    self.late * 16 + way * 8 + AC * at + core
                    for at in range(4)
                    for way in range(2)
                    for core in (1, 0)
                ],
            )

    class Direct:
        def __init__(self, number, first, count):
            self.places = range(first, first + count)
            self.rows = pl.ds(first * 8, count * 8)
            self.received = distant_recv.at[number]

        def of_quarter(self, quarter):
            start = pl.multiple_of(quarter * QUARTER + self.rows.start, 8)
            return send.at[1, pl.ds(start, self.rows.size)]

        def start(self):
            for owner_x in (0, 1, 3, 2):

                @pl.when(x != owner_x)
                def _(owner_x=owner_x):
                    number = lax.rem(x - owner_x + AX, AX) - 1
                    remote(
                        self.of_quarter(owner_x), from_all.at[number, self.rows],
                        distant_send, self.received, owner_x * SIDE + j, b,
                    ).start()

        def spread(self):
            arrived = from_all.at[:, self.rows]
            pltpu.make_async_copy(arrived, arrived, self.received).wait()
            x_sum[1, self.rows] = (
                self.of_quarter(x)[...]
                + from_all[1, self.rows]
                + (from_all[0, self.rows] + from_all[2, self.rows])
            )
            send_tiles(1, self.places)

    def z_wait(buffer, chunk, sem):
        many = buffer.at[chunk, pl.ds(0, (SIDE - 1) * 8)]
        pltpu.make_async_copy(many, many, sem.at[chunk]).wait()

    own = sphere[x, lax.div(z, 4) * 2 + h, pl.ds(lax.rem(z, 4) * AC + c, 1), :]
    index = jnp.broadcast_to((own >> 7) & 127, (8, NG))
    factor = 1.0 / (NG * NG * NX) ** 0.5

    def z_last(chunk):
        z_wait(tiles, chunk, z_recv)
        values = []
        for core in range(2):
            total = tiles[chunk, pl.ds(core * 8, 8)]
            for chip in range(1, SIDE // 2):
                total = total + tiles[chunk, pl.ds((2 * chip + core) * 8, 8)]
            values.append(lanes(total, index) * factor)
        return values

    native, native_late = Relay(0), Relay(1)
    distant = [
        Direct(number, first, count)
        for number, (first, count) in enumerate(((0, 2), (2, 6), (8, 8), (16, 16)))
    ]

    @pl.when(c == 0)
    def _():
        hear(1)

    native.first()
    native_late.first()
    native.direct()
    native_late.direct()

    @pl.when(c == 1)
    def _():
        hear(1)
        tell(2)
        native.second()
        native_late.second()

    def arrival(core):
        return remote(
            own_right.at[:, 0], rights.at[1, core], y_send, y_recv.at[core], g, 1 - b
        )

    arrival(0).wait_recv()
    arrival(1).wait_recv()
    @pl.when(c == 1)
    def _():
        hear(2)
        tell(3)

    distant_both()

    @pl.when(c == 0)
    def _():
        hear(2)

    distant[0].start()

    @pl.when(c == 0)
    def _():
        native.second()
        distant[1].start()
        distant[2].start()
        native_late.second()

    @pl.when(c == 1)
    def _():
        distant[1].start()

    hear(3)
    native.spread()

    @pl.when(c == 1)
    def _():
        distant[2].start()

    distant[0].spread()

    @pl.when(jnp.logical_or(c == 0, z < 4))
    def _():
        distant[3].start()
    distant[1].spread()
    distant[2].spread()

    @pl.when(jnp.logical_and(c == 1, z >= 4))
    def _():
        distant[3].start()

    native_late.spread()
    distant[3].spread()
    values = z_last(0)
    values = values + z_last(1)
    loads[5].wait()
    for column in range(4):
        position = jnp.full((8, NG), lax.rem(order[column] + 4 - 2 * b, 4), jnp.int32)
        value = values[3]
        for at in range(3):
            value = jnp.where(position == at, values[at], value)
        out_ref[pl.ds(column, 8, stride=4), :] = value

    for copy in to_pair:
        copy.wait_send()
    pltpu.make_async_copy(own_right, own_right, y_send).wait()
    for chunk, sem in enumerate((native_send, distant_send)):
        sent = send.at[chunk, pl.ds(0, 3 * QUARTER)]
        pltpu.make_async_copy(sent, sent, sem).wait()
    for chunk in range(2):
        z_wait(x_sum, chunk, z_send)


def local(left_bands, right_bands, sphere_index, right_order):
    table, trig = dft_tables()
    hbm = pl.BlockSpec(memory_space=pltpu.HBM)
    dma = pltpu.SemaphoreType.DMA
    result = pl.pallas_call(
        kernel,
        name="pair_sums",
        out_shape=pltpu.VMEM((32, NG), F32),
        in_specs=[hbm] * 6,
        out_specs=pl.BlockSpec(memory_space=pltpu.VMEM),
        scratch_shapes=[
            pltpu.VMEM((2, 2, 4, NG, NX), F32),
            pltpu.VMEM((2, 2, 2, NG, NX), F32),
            pltpu.VMEM((2, 2, NG, NX), F32),
            pltpu.VMEM((4, 4, 8, NG), jnp.int32),
            pltpu.VMEM((12 * NG, 2 * NG), BF16),
            pltpu.VMEM((8, NG), F32),
            pltpu.VMEM((NG, NG), jnp.int32),
            pltpu.VMEM((NG, NG), jnp.int32),
            pltpu.VMEM((NG, NG), jnp.int32),
            pltpu.VMEM((2, 2, NG, NG), F32),
            pltpu.VMEM((8, NG, NG), F32),
            pltpu.VMEM((2, AX * QUARTER, NG), F32),
            pltpu.VMEM((2, 2, PIECE, NG), F32),
            pltpu.VMEM((2, 4, PIECE, NG), F32),
            pltpu.VMEM((3, QUARTER, NG), F32),
            pltpu.VMEM((2, QUARTER, NG), F32),
            pltpu.VMEM((2, QUARTER, NG), F32),
            pltpu.SMEM((4,), jnp.int32),
            dma((7,)), dma((2,)), dma((2,)), dma, dma((2,)), dma, dma((2, 3)), dma, dma((4,)),
            dma((2,)), dma((2,)), pltpu.SemaphoreType.REGULAR((4,)),
        ],
        compiler_params=pltpu.CompilerParams(collective_id=0, has_side_effects=True),
    )(
        right_order,
        left_bands.reshape(2, 4, NG, NX),
        right_bands.reshape(2, 2, NG, NX),
        sphere_index.reshape(4, 4, 8, NG),
        jnp.asarray(table),
        jnp.asarray(trig),
    )
    return result.reshape(2, 4, 4, NG)


def solution(mesh):
    placed = (P(None, "band", "grid", None, None), P(None, "band", "grid", None, None), P(), P())
    return jax.shard_map(
        local, mesh=mesh, in_specs=placed, out_specs=P(None, "band", None, "grid"), check_vma=False
    )
```

```python
import functools
import math

import jax
import jax.numpy as jnp
from jax import lax
from jax.experimental import pallas as pl
from jax.experimental.pallas import tpu as pltpu
from jax.sharding import PartitionSpec as P
import numpy as np

NG = 128
NX = 128
NGV = 16384
AX, AH, AZ, AC = 4, 2, 8, 2
SIDE = AH * AZ * AC
QUARTER = SIDE * 8
HALF = QUARTER // 2
PIECE = HALF // 2
PLACE = (0, 2, 1, 3)
Y_ROWS = (6 * NG, 8 * NG, 10 * NG)
MESH = pl.DeviceIdType.MESH
F32 = jnp.float32
BF16 = jnp.bfloat16


def split(value):
    high = value.astype(BF16)
    return high, (value - high.astype(F32)).astype(BF16)


def dft_tables():
    counter = np.arange(NG)
    angles = (counter[:, None] * counter[None, :] % NG) * (2.0 * math.pi / NG)
    cosine, sine = np.cos(angles), np.sin(angles)

    def halves(table):
        high = table.astype(np.float32).astype(BF16)
        low = (table - high.astype(np.float64)).astype(np.float32).astype(BF16)
        return high, low

    high, low = halves(np.block([[cosine, -sine], [sine, cosine]]))
    along_x = np.concatenate([high, high, low], axis=0)
    high, low = halves(np.block([[cosine, sine], [-sine, cosine]]))
    along_y = np.concatenate([high, low, high], axis=0)
    trig = np.zeros((8, NG), np.float32)
    trig[0], trig[1] = cosine[1], sine[1]
    return np.concatenate([along_x, along_y], axis=0), trig


def lanes(value, index):
    return jnp.take_along_axis(value, index, axis=1, mode="promise_in_bounds")


def kernel(
    order_ref, left_ref, right_ref, sphere_ref, table_ref, trig_ref, out_ref,
    lefts, rights, own_right, sphere, dft, trig,
    ky_t, val_t, kx_of, phase, acc, send, from_a, from_bc, from_all, x_sum, tiles,
    order, load_sem, early_send, pair_recv, y_recv, send_sem, native_recv, distant_recv, z_recv, known,
):
    g = lax.axis_index("grid")
    b = lax.axis_index("band")
    c = lax.rem(g, AC)
    j = lax.rem(g, SIDE)
    x = lax.div(g, SIDE)
    up = lax.rem(x + 1, AX)
    down = lax.rem(x + AX - 1, AX)
    across = lax.rem(x + 2, AX)

    loads = [
        pltpu.make_async_copy(right_ref, own_right, load_sem.at[0]),
        pltpu.make_async_copy(left_ref, lefts.at[c], load_sem.at[1]),
        pltpu.make_async_copy(trig_ref, trig, load_sem.at[2]),
        pltpu.make_async_copy(right_ref.at[:, c], rights.at[0, c], load_sem.at[3]),
        pltpu.make_async_copy(table_ref, dft, load_sem.at[4]),
        pltpu.make_async_copy(order_ref, order, load_sem.at[5]),
    ]
    sphere_loads = [
        pltpu.make_async_copy(sphere_ref.at[:, at], sphere.at[:, PLACE[at]], load_sem.at[6])
        for at in range(4)
    ]
    for load in loads[:1] + sphere_loads + loads[1:]:
        load.start()

    grid_up = up * SIDE + j
    grid_down = down * SIDE + j
    pair = g + 1 - 2 * c
    h = lax.rem(lax.div(g, SIDE // 2), AH)
    z = lax.rem(lax.div(g, AC), AZ)
    q = lax.div(z, 4) * 16 + h * 8 + lax.rem(z, 4) * AC + c
    opposite = g + SIDE // 2 - SIDE * h
    along_z = [(g + AC * (lax.rem(z + step, AZ) - z), b) for step in (1, AZ - 1, 2, AZ - 2)]
    close = [(pair, b), (g, 1 - b), (pair, 1 - b)]
    near = along_z[:2] + [(grid_up, b), (grid_down, b), (opposite, 1 - b)]
    barrier = pltpu.get_barrier_semaphore()

    def signal(sem, devices):
        for grid, band in devices:
            pl.semaphore_signal(sem, inc=1, device_id=(grid, band), device_id_type=MESH)

    signal(barrier, close)

    @pl.when(c == 1)
    def _():
        signal(barrier, near)

    def tell(step):
        others = near + [(g, 1 - b)] if step == 0 else along_z + near[2:4] + [(opposite, b)]

        @pl.when(c == 1)
        def _():
            signal(known.at[step], [(pair, b)] + others)

    def hear(step):
        pl.semaphore_wait(known.at[step], jnp.where(c == 1, 6 if step == 0 else 7, 1))

    def remote(source, target, sent, received, grid, band):
        return pltpu.make_async_remote_copy(
            src_ref=source, dst_ref=target, send_sem=sent, recv_sem=received,
            device_id=(grid, band), device_id_type=MESH,
        )

    to_other = [
        remote(own_right.at[:, m], rights.at[1, c], early_send, y_recv, g - c + m, 1 - b)
        for m in range(2)
    ]
    to_pair = [
        remote(lefts.at[c], lefts.at[c], early_send, pair_recv, pair, b),
        remote(own_right.at[:, 1 - c], rights.at[0, c], early_send, pair_recv, pair, b),
    ]
    loads[0].wait()
    pl.semaphore_wait(barrier, jnp.where(c == 1, len(close) + len(near), len(close)))
    for copy in to_other:
        copy.start()
    loads[1].wait()
    for copy in to_pair:
        copy.start()
    tell(0)

    pltpu.make_async_copy(sphere, sphere, load_sem.at[6]).wait()
    loads[2].wait()
    flipped = sphere[...].reshape(NG, NG).T
    ky_t[...] = (flipped >> 7) & 127
    val_t[...] = ((flipped >> 14) << 7) | (flipped & 127)
    rows = lax.broadcasted_iota(jnp.int32, (NG, NG), 0)

    def place(p, table):
        return jnp.where(ky_t[pl.ds(p, 1), :] == rows, val_t[pl.ds(p, 1), :], table)

    table = lax.fori_loop(0, NG, place, jnp.zeros((NG, NG), jnp.int32), unroll=8)
    kx_of[...] = table & 127
    kz = table >> 7
    cosine = jnp.broadcast_to(trig[0:1, :], (NG, NG))
    sine = jnp.broadcast_to(trig[1:2, :], (NG, NG))
    for core in range(2):
        angle = (kz * (g - c + core)) & 127
        phase[core, 0] = lanes(cosine, angle)
        phase[core, 1] = lanes(sine, angle)

    def along_rows(chunk, plane, half):
        right_real = rights[chunk, plane, 0]
        right_imag = rights[chunk, plane, 1]
        fields = []
        for n in (2 * half, 2 * half + 1):
            left_real = lefts[plane, 0, n]
            left_imag = lefts[plane, 1, n]
            fields.append(
                jnp.concatenate(
                    [
                        left_real * right_real + left_imag * right_imag,
                        left_real * right_imag - left_imag * right_real,
                    ],
                    axis=1,
                )
            )
        high, low = split(jnp.concatenate(fields, axis=0))
        moved = jnp.dot(
            jnp.concatenate([high, low, high], axis=1), dft[: 6 * NG, :], preferred_element_type=F32
        )
        columns = [
            jnp.concatenate([moved[start : start + NG, :NX], moved[start : start + NG, NX:]], axis=0)
            for start in (0, NG)
        ]
        return split(jnp.concatenate(columns, axis=1))

    def along_columns(rows):
        high, low = rows
        return jnp.dot(
            jnp.concatenate([dft[start : start + 2 * NG, :] for start in Y_ROWS], axis=1),
            jnp.concatenate([high, high, low], axis=0),
            preferred_element_type=F32,
        )

    def pick(plane, waves, half):
        index = kx_of[...]
        cosines, sines = phase[plane, 0], phase[plane, 1]
        picked = {}
        for at in range(2):
            real = lanes(waves[:NG, at * NX : (at + 1) * NX], index)
            imag = lanes(waves[NG:, at * NX : (at + 1) * NX], index)
            n = 2 * half + at
            picked[n] = real * cosines + imag * sines
            picked[n + 4] = imag * cosines - real * sines
        return picked

    def ship(chunk, channel, value):
        send[chunk, pl.ds(channel, NG, stride=8), :] = value.T

    def native_first(plane):
        for half in range(2):
            picked = pick(plane, along_columns(along_rows(0, plane, half)), half)
            for channel, value in picked.items():
                acc[channel] = value

    def native_second(plane):
        for half in range(2):
            picked = pick(plane, along_columns(along_rows(0, plane, half)), half)
            for channel, value in picked.items():
                ship(0, channel, acc[channel] + value)

    def distant_both():
        def total(half, waves):
            first, second = (pick(plane, waves[plane], half) for plane in range(2))
            for channel in first:
                ship(1, channel, first[channel] + second[channel])

        rows = [along_rows(1, plane, half) for half in range(2) for plane in range(2)]
        waves = [along_columns(value) for value in rows]
        total(0, waves[:2])
        total(1, waves[2:])

    for load in loads[3:5]:
        load.wait()
    native_first(c)
    hear(0)
    tell(1)
    both = send.at[:, pl.ds(0, 640)]
    pltpu.make_async_copy(both, both, pair_recv).wait()
    native_second(1 - c)

    def part(chunk, quarter, late, way):
        start = pl.multiple_of(quarter * QUARTER + late * HALF + way * PIECE, PIECE)
        return send.at[chunk, pl.ds(start, PIECE)]

    def send_tiles(chunk, places):
        mine = pl.ds(pl.multiple_of(q * 8, 8), 8)
        for to in places:
            owner_z = to // 16 * 4 + to % 8 // AC
            theirs = pl.ds(to * 8, 8)
            owner = x * SIDE + (to % 16 // 8 * AZ + owner_z) * AC + to % AC

            @pl.when(q != to)
            def _(theirs=theirs, owner=owner):
                remote(
                    x_sum.at[chunk, theirs], tiles.at[chunk, mine],
                    send_sem, z_recv.at[chunk], owner, b,
                ).start()

        @pl.when(functools.reduce(jnp.logical_or, [q == to for to in places]))
        def _():
            tiles[chunk, mine] = x_sum[chunk, mine]

    class Relay:
        def __init__(self, late):
            self.late = late
            self.added = from_a.at[late]
            self.last = from_bc.at[late]
            routes = (
                (across, 0, self.added.at[0], 0, grid_up),
                (across, 1, self.added.at[1], 0, grid_down),
                (up, 1, self.last.at[0], 1, grid_up),
                (down, 0, self.last.at[1], 1, grid_down),
                (up, 0, self.last.at[2], 1, grid_up),
                (down, 1, self.last.at[3], 1, grid_down),
            )
            self.copies = [
                remote(
                    part(0, quarter, late, way), target, send_sem,
                    native_recv.at[late, number], to, b,
                )
                for quarter, way, target, number, to in routes
            ]

        def first(self):
            for copy in self.copies[:2]:
                copy.start()

        def direct(self):
            for copy in self.copies[2:4]:
                copy.start()

        def second(self):
            pltpu.make_async_copy(self.added, self.added, native_recv.at[self.late, 0]).wait()
            for way, quarter in enumerate((up, down)):
                ref = part(0, quarter, self.late, way)
                ref[...] = ref[...] + self.added[way]
                self.copies[4 + way].start()

        def spread(self):
            pltpu.make_async_copy(self.last, self.last, native_recv.at[self.late, 1]).wait()
            for way in range(2):
                x_sum[0, pl.ds(self.late * HALF + way * PIECE, PIECE)] = (
                    part(0, x, self.late, way)[...] + self.last[2 + way] + self.last[1 - way]
                )
            send_tiles(
                0,
                [
                    self.late * 16 + way * 8 + AC * at + core
                    for at in range(4)
                    for way in range(2)
                    for core in (1, 0)
                ],
            )

    class Direct:
        def __init__(self, number, first, count):
            self.places = range(first, first + count)
            self.rows = pl.ds(first * 8, count * 8)
            self.received = distant_recv.at[number]

        def of_quarter(self, quarter):
            start = pl.multiple_of(quarter * QUARTER + self.rows.start, 8)
            return send.at[1, pl.ds(start, self.rows.size)]

        def start(self):
            for owner_x in (0, 1, 3, 2):

                @pl.when(x != owner_x)
                def _(owner_x=owner_x):
                    number = lax.rem(x - owner_x + AX, AX) - 1
                    remote(
                        self.of_quarter(owner_x), from_all.at[number, self.rows],
                        send_sem, self.received, owner_x * SIDE + j, b,
                    ).start()

        def spread(self):
            arrived = from_all.at[:, self.rows]
            pltpu.make_async_copy(arrived, arrived, self.received).wait()
            x_sum[1, self.rows] = (
                self.of_quarter(x)[...]
                + from_all[1, self.rows]
                + (from_all[0, self.rows] + from_all[2, self.rows])
            )
            send_tiles(1, self.places)

    def z_wait(chunk):
        many = tiles.at[chunk, pl.ds(0, (SIDE - 1) * 8)]
        pltpu.make_async_copy(many, many, z_recv.at[chunk]).wait()

    own = sphere[x, lax.div(z, 4) * 2 + h, pl.ds(lax.rem(z, 4) * AC + c, 1), :]
    index = jnp.broadcast_to((own >> 7) & 127, (8, NG))
    factor = 1.0 / (NG * NG * NX) ** 0.5

    def z_last(chunk):
        z_wait(chunk)
        values = []
        for core in range(2):
            total = tiles[chunk, pl.ds(core * 8, 8)]
            for chip in range(1, SIDE // 2):
                total = total + tiles[chunk, pl.ds((2 * chip + core) * 8, 8)]
            values.append(lanes(total, index) * factor)
        return values

    native, native_late = Relay(0), Relay(1)
    distant = [
        Direct(number, first, count)
        for number, (first, count) in enumerate(((0, 2), (2, 6), (8, 8), (16, 16)))
    ]

    @pl.when(c == 0)
    def _():
        hear(1)

    native.first()
    native_late.first()
    native.direct()
    native_late.direct()

    @pl.when(c == 1)
    def _():
        hear(1)
        tell(2)
        native.second()
        native_late.second()

    pltpu.make_async_copy(rights.at[1], rights.at[1], y_recv).wait()
    @pl.when(c == 1)
    def _():
        hear(2)
        tell(3)

    distant_both()

    @pl.when(c == 0)
    def _():
        hear(2)

    distant[0].start()

    @pl.when(c == 0)
    def _():
        native.second()
        distant[1].start()
        distant[2].start()
        native_late.second()

    @pl.when(c == 1)
    def _():
        distant[1].start()

    hear(3)
    native.spread()

    @pl.when(c == 1)
    def _():
        distant[2].start()

    distant[0].spread()

    @pl.when(jnp.logical_or(c == 0, z < 4))
    def _():
        distant[3].start()
    distant[1].spread()
    distant[2].spread()

    @pl.when(jnp.logical_and(c == 1, z >= 4))
    def _():
        distant[3].start()

    native_late.spread()
    distant[3].spread()
    values = z_last(0)
    values = values + z_last(1)
    loads[5].wait()
    for column in range(4):
        position = jnp.full((8, NG), lax.rem(order[column] + 4 - 2 * b, 4), jnp.int32)
        value = values[3]
        for at in range(3):
            value = jnp.where(position == at, values[at], value)
        out_ref[pl.ds(column, 8, stride=4), :] = value

    for sem, rows in ((early_send, 896), (send_sem, 1016)):
        sent = send.at[:, pl.ds(0, rows)]
        pltpu.make_async_copy(sent, sent, sem).wait()


def local(left_bands, right_bands, sphere_index, right_order):
    table, trig = dft_tables()
    hbm = pl.BlockSpec(memory_space=pltpu.HBM)
    dma = pltpu.SemaphoreType.DMA
    result = pl.pallas_call(
        kernel,
        name="pair_sums",
        out_shape=pltpu.VMEM((32, NG), F32),
        in_specs=[hbm] * 6,
        out_specs=pl.BlockSpec(memory_space=pltpu.VMEM),
        scratch_shapes=[
            pltpu.VMEM((2, 2, 4, NG, NX), F32),
            pltpu.VMEM((2, 2, 2, NG, NX), F32),
            pltpu.VMEM((2, 2, NG, NX), F32),
            pltpu.VMEM((4, 4, 8, NG), jnp.int32),
            pltpu.VMEM((12 * NG, 2 * NG), BF16),
            pltpu.VMEM((8, NG), F32),
            pltpu.VMEM((NG, NG), jnp.int32),
            pltpu.VMEM((NG, NG), jnp.int32),
            pltpu.VMEM((NG, NG), jnp.int32),
            pltpu.VMEM((2, 2, NG, NG), F32),
            pltpu.VMEM((8, NG, NG), F32),
            pltpu.VMEM((2, AX * QUARTER, NG), F32),
            pltpu.VMEM((2, 2, PIECE, NG), F32),
            pltpu.VMEM((2, 4, PIECE, NG), F32),
            pltpu.VMEM((3, QUARTER, NG), F32),
            pltpu.VMEM((2, QUARTER, NG), F32),
            pltpu.VMEM((2, QUARTER, NG), F32),
            pltpu.SMEM((4,), jnp.int32),
            dma((7,)), dma, dma, dma, dma, dma((2, 2)), dma((4,)), dma((2,)),
            pltpu.SemaphoreType.REGULAR((4,)),
        ],
        compiler_params=pltpu.CompilerParams(collective_id=0, has_side_effects=True),
    )(
        right_order,
        left_bands.reshape(2, 4, NG, NX),
        right_bands.reshape(2, 2, NG, NX),
        sphere_index.reshape(4, 4, 8, NG),
        jnp.asarray(table),
        jnp.asarray(trig),
    )
    return result.reshape(2, 4, 4, NG)


def solution(mesh):
    placed = (P(None, "band", "grid", None, None), P(None, "band", "grid", None, None), P(), P())
    return jax.shard_map(
        local, mesh=mesh, in_specs=placed, out_specs=P(None, "band", None, "grid"), check_vma=False
    )
```

```python
import functools
import math

import jax
import jax.numpy as jnp
from jax import lax
from jax.experimental import pallas as pl
from jax.experimental.pallas import tpu as pltpu
from jax.sharding import PartitionSpec as P
import numpy as np

NG = 128
NX = 128
NGV = 16384
AX, AH, AZ, AC = 4, 2, 8, 2
SIDE = AH * AZ * AC
QUARTER = SIDE * 8
HALF = QUARTER // 2
PIECE = HALF // 2
PLACE = (0, 2, 1, 3)
Y_ROWS = (6 * NG, 8 * NG, 10 * NG)
MESH = pl.DeviceIdType.MESH
F32 = jnp.float32
BF16 = jnp.bfloat16


def split(value):
    high = value.astype(BF16)
    return high, (value - high.astype(F32)).astype(BF16)


def dft_tables():
    counter = np.arange(NG)
    angles = (counter[:, None] * counter[None, :] % NG) * (2.0 * math.pi / NG)
    cosine, sine = np.cos(angles), np.sin(angles)

    def halves(table):
        high = table.astype(np.float32).astype(BF16)
        low = (table - high.astype(np.float64)).astype(np.float32).astype(BF16)
        return high, low

    high, low = halves(np.block([[cosine, -sine], [sine, cosine]]))
    along_x = np.concatenate([high, high, low], axis=0)
    high, low = halves(np.block([[cosine, sine], [-sine, cosine]]))
    along_y = np.concatenate([high, low, high], axis=0)
    trig = np.zeros((8, NG), np.float32)
    trig[0], trig[1] = cosine[1], sine[1]
    return np.concatenate([along_x, along_y], axis=0), trig


def lanes(value, index):
    return jnp.take_along_axis(value, index, axis=1, mode="promise_in_bounds")


def kernel(
    order_ref, left_ref, right_ref, sphere_ref, table_ref, trig_ref, out_ref,
    lefts, rights, own_right, sphere, dft, trig,
    ky_t, val_t, kx_of, phase, acc, send, from_a, from_bc, from_all, x_sum, tiles,
    order, load_sem, early_send, pair_recv, y_recv, send_sem, native_recv, distant_recv, z_recv, known,
):
    g = lax.axis_index("grid")
    b = lax.axis_index("band")
    c = lax.rem(g, AC)
    j = lax.rem(g, SIDE)
    x = lax.div(g, SIDE)
    up = lax.rem(x + 1, AX)
    down = lax.rem(x + AX - 1, AX)
    across = lax.rem(x + 2, AX)

    loads = [
        pltpu.make_async_copy(right_ref, own_right, load_sem.at[0]),
        pltpu.make_async_copy(left_ref, lefts.at[c], load_sem.at[1]),
        pltpu.make_async_copy(trig_ref, trig, load_sem.at[4]),
        pltpu.make_async_copy(right_ref.at[:, c], rights.at[0, c], load_sem.at[2]),
        pltpu.make_async_copy(table_ref, dft, load_sem.at[2]),
        pltpu.make_async_copy(order_ref, order, load_sem.at[3]),
    ]
    sphere_loads = [
        pltpu.make_async_copy(sphere_ref.at[:, at], sphere.at[:, PLACE[at]], load_sem.at[4])
        for at in range(4)
    ]
    for load in loads[:1] + sphere_loads + loads[1:]:
        load.start()

    grid_up = up * SIDE + j
    grid_down = down * SIDE + j
    pair = g + 1 - 2 * c
    h = lax.rem(lax.div(g, SIDE // 2), AH)
    z = lax.rem(lax.div(g, AC), AZ)
    q = lax.div(z, 4) * 16 + h * 8 + lax.rem(z, 4) * AC + c
    opposite = g + SIDE // 2 - SIDE * h
    along_z = [(g + AC * (lax.rem(z + step, AZ) - z), b) for step in (1, AZ - 1, 2, AZ - 2)]
    close = [(pair, b), (g, 1 - b), (pair, 1 - b)]
    near = along_z[:2] + [(grid_up, b), (grid_down, b), (opposite, 1 - b)]
    barrier = pltpu.get_barrier_semaphore()

    def signal(sem, devices):
        for grid, band in devices:
            pl.semaphore_signal(sem, inc=1, device_id=(grid, band), device_id_type=MESH)

    signal(barrier, close)

    @pl.when(c == 1)
    def _():
        signal(barrier, near)

    def tell(step):
        others = near + [(g, 1 - b)] if step == 0 else along_z + near[2:4] + [(opposite, b)]

        @pl.when(c == 1)
        def _():
            signal(known.at[step], [(pair, b)] + others)

    def hear(step):
        pl.semaphore_wait(known.at[step], jnp.where(c == 1, 6 if step == 0 else 7, 1))

    def remote(source, target, sent, received, grid, band):
        return pltpu.make_async_remote_copy(
            src_ref=source, dst_ref=target, send_sem=sent, recv_sem=received,
            device_id=(grid, band), device_id_type=MESH,
        )

    to_other = [
        remote(own_right.at[:, m], rights.at[1, c], early_send, y_recv, g - c + m, 1 - b)
        for m in range(2)
    ]
    to_pair = [
        remote(lefts.at[c], lefts.at[c], early_send, pair_recv, pair, b),
        remote(own_right.at[:, 1 - c], rights.at[0, c], early_send, pair_recv, pair, b),
    ]
    loads[0].wait()
    pl.semaphore_wait(barrier, jnp.where(c == 1, len(close) + len(near), len(close)))
    for copy in to_other:
        copy.start()
    loads[1].wait()
    for copy in to_pair:
        copy.start()
    tell(0)

    both = send.at[0, pl.ds(0, 136)]
    pltpu.make_async_copy(both, both, load_sem.at[4]).wait()
    flipped = sphere[...].reshape(NG, NG).T
    ky_t[...] = (flipped >> 7) & 127
    val_t[...] = ((flipped >> 14) << 7) | (flipped & 127)
    rows = lax.broadcasted_iota(jnp.int32, (NG, NG), 0)

    def place(p, table):
        return jnp.where(ky_t[pl.ds(p, 1), :] == rows, val_t[pl.ds(p, 1), :], table)

    table = lax.fori_loop(0, NG, place, jnp.zeros((NG, NG), jnp.int32), unroll=8)
    kx_of[...] = table & 127
    kz = table >> 7
    cosine = jnp.broadcast_to(trig[0:1, :], (NG, NG))
    sine = jnp.broadcast_to(trig[1:2, :], (NG, NG))
    for core in range(2):
        angle = (kz * (g - c + core)) & 127
        phase[core, 0] = lanes(cosine, angle)
        phase[core, 1] = lanes(sine, angle)

    def along_rows(chunk, plane, half):
        right_real = rights[chunk, plane, 0]
        right_imag = rights[chunk, plane, 1]
        fields = []
        for n in (2 * half, 2 * half + 1):
            left_real = lefts[plane, 0, n]
            left_imag = lefts[plane, 1, n]
            fields.append(
                jnp.concatenate(
                    [
                        left_real * right_real + left_imag * right_imag,
                        left_real * right_imag - left_imag * right_real,
                    ],
                    axis=1,
                )
            )
        high, low = split(jnp.concatenate(fields, axis=0))
        moved = jnp.dot(
            jnp.concatenate([high, low, high], axis=1), dft[: 6 * NG, :], preferred_element_type=F32
        )
        columns = [
            jnp.concatenate([moved[start : start + NG, :NX], moved[start : start + NG, NX:]], axis=0)
            for start in (0, NG)
        ]
        return split(jnp.concatenate(columns, axis=1))

    def along_columns(rows):
        high, low = rows
        return jnp.dot(
            jnp.concatenate([dft[start : start + 2 * NG, :] for start in Y_ROWS], axis=1),
            jnp.concatenate([high, high, low], axis=0),
            preferred_element_type=F32,
        )

    def pick(plane, waves, half):
        index = kx_of[...]
        cosines, sines = phase[plane, 0], phase[plane, 1]
        picked = {}
        for at in range(2):
            real = lanes(waves[:NG, at * NX : (at + 1) * NX], index)
            imag = lanes(waves[NG:, at * NX : (at + 1) * NX], index)
            n = 2 * half + at
            picked[n] = real * cosines + imag * sines
            picked[n + 4] = imag * cosines - real * sines
        return picked

    def ship(chunk, channel, value):
        send[chunk, pl.ds(channel, NG, stride=8), :] = value.T

    def native_first(plane):
        for half in range(2):
            picked = pick(plane, along_columns(along_rows(0, plane, half)), half)
            for channel, value in picked.items():
                acc[channel] = value

    def native_second(plane):
        for half in range(2):
            picked = pick(plane, along_columns(along_rows(0, plane, half)), half)
            for channel, value in picked.items():
                ship(0, channel, acc[channel] + value)

    def distant_both():
        def total(half, waves):
            first, second = (pick(plane, waves[plane], half) for plane in range(2))
            for channel in first:
                ship(1, channel, first[channel] + second[channel])

        rows = [along_rows(1, plane, half) for half in range(2) for plane in range(2)]
        waves = [along_columns(value) for value in rows]
        total(0, waves[:2])
        total(1, waves[2:])

    both = send.at[:, pl.ds(0, 896)]
    pltpu.make_async_copy(both, both, load_sem.at[2]).wait()
    native_first(c)
    hear(0)
    tell(1)
    both = send.at[:, pl.ds(0, 640)]
    pltpu.make_async_copy(both, both, pair_recv).wait()
    native_second(1 - c)

    def part(chunk, quarter, late, way):
        start = pl.multiple_of(quarter * QUARTER + late * HALF + way * PIECE, PIECE)
        return send.at[chunk, pl.ds(start, PIECE)]

    def send_tiles(chunk, places):
        mine = pl.ds(pl.multiple_of(q * 8, 8), 8)
        for to in places:
            owner_z = to // 16 * 4 + to % 8 // AC
            theirs = pl.ds(to * 8, 8)
            owner = x * SIDE + (to % 16 // 8 * AZ + owner_z) * AC + to % AC

            @pl.when(q != to)
            def _(theirs=theirs, owner=owner):
                remote(
                    x_sum.at[chunk, theirs], tiles.at[chunk, mine],
                    send_sem, z_recv.at[chunk], owner, b,
                ).start()

        @pl.when(functools.reduce(jnp.logical_or, [q == to for to in places]))
        def _():
            tiles[chunk, mine] = x_sum[chunk, mine]

    class Relay:
        def __init__(self, late):
            self.late = late
            self.added = from_a.at[late]
            self.last = from_bc.at[late]
            routes = (
                (across, 0, self.added.at[0], 0, grid_up),
                (across, 1, self.added.at[1], 0, grid_down),
                (up, 1, self.last.at[0], 1, grid_up),
                (down, 0, self.last.at[1], 1, grid_down),
                (up, 0, self.last.at[2], 1, grid_up),
                (down, 1, self.last.at[3], 1, grid_down),
            )
            self.copies = [
                remote(
                    part(0, quarter, late, way), target, send_sem,
                    native_recv.at[late, number], to, b,
                )
                for quarter, way, target, number, to in routes
            ]

        def first(self):
            for copy in self.copies[:2]:
                copy.start()

        def direct(self):
            for copy in self.copies[2:4]:
                copy.start()

        def second(self):
            pltpu.make_async_copy(self.added, self.added, native_recv.at[self.late, 0]).wait()
            for way, quarter in enumerate((up, down)):
                ref = part(0, quarter, self.late, way)
                ref[...] = ref[...] + self.added[way]
                self.copies[4 + way].start()

        def spread(self):
            pltpu.make_async_copy(self.last, self.last, native_recv.at[self.late, 1]).wait()
            for way in range(2):
                x_sum[0, pl.ds(self.late * HALF + way * PIECE, PIECE)] = (
                    part(0, x, self.late, way)[...] + self.last[2 + way] + self.last[1 - way]
                )
            send_tiles(
                0,
                [
                    self.late * 16 + way * 8 + AC * at + core
                    for at in range(4)
                    for way in range(2)
                    for core in (1, 0)
                ],
            )

    class Direct:
        def __init__(self, number, first, count):
            self.places = range(first, first + count)
            self.rows = pl.ds(first * 8, count * 8)
            self.received = distant_recv.at[number]

        def of_quarter(self, quarter):
            start = pl.multiple_of(quarter * QUARTER + self.rows.start, 8)
            return send.at[1, pl.ds(start, self.rows.size)]

        def start(self):
            for owner_x in (0, 1, 3, 2):

                @pl.when(x != owner_x)
                def _(owner_x=owner_x):
                    number = lax.rem(x - owner_x + AX, AX) - 1
                    remote(
                        self.of_quarter(owner_x), from_all.at[number, self.rows],
                        send_sem, self.received, owner_x * SIDE + j, b,
                    ).start()

        def spread(self):
            arrived = from_all.at[:, self.rows]
            pltpu.make_async_copy(arrived, arrived, self.received).wait()
            x_sum[1, self.rows] = (
                self.of_quarter(x)[...]
                + from_all[1, self.rows]
                + (from_all[0, self.rows] + from_all[2, self.rows])
            )
            send_tiles(1, self.places)

    def z_wait(chunk):
        many = tiles.at[chunk, pl.ds(0, (SIDE - 1) * 8)]
        pltpu.make_async_copy(many, many, z_recv.at[chunk]).wait()

    own = sphere[x, lax.div(z, 4) * 2 + h, pl.ds(lax.rem(z, 4) * AC + c, 1), :]
    index = jnp.broadcast_to((own >> 7) & 127, (8, NG))
    factor = 1.0 / (NG * NG * NX) ** 0.5

    def z_last(chunk):
        z_wait(chunk)
        values = []
        for core in range(2):
            total = tiles[chunk, pl.ds(core * 8, 8)]
            for chip in range(1, SIDE // 2):
                total = total + tiles[chunk, pl.ds((2 * chip + core) * 8, 8)]
            values.append(lanes(total, index) * factor)
        return values

    native, native_late = Relay(0), Relay(1)
    distant = [
        Direct(number, first, count)
        for number, (first, count) in enumerate(((0, 2), (2, 6), (8, 8), (16, 16)))
    ]

    @pl.when(c == 0)
    def _():
        hear(1)

    native.first()
    native_late.first()
    native.direct()
    native_late.direct()

    @pl.when(c == 1)
    def _():
        hear(1)
        tell(2)
        native.second()
        native_late.second()

    pltpu.make_async_copy(rights.at[1], rights.at[1], y_recv).wait()
    @pl.when(c == 1)
    def _():
        hear(2)
        tell(3)

    distant_both()

    @pl.when(c == 0)
    def _():
        hear(2)

    distant[0].start()

    @pl.when(c == 0)
    def _():
        native.second()
        distant[1].start()
        distant[2].start()
        native_late.second()

    @pl.when(c == 1)
    def _():
        distant[1].start()

    hear(3)
    native.spread()

    @pl.when(c == 1)
    def _():
        distant[2].start()

    distant[0].spread()

    @pl.when(jnp.logical_or(c == 0, z < 4))
    def _():
        distant[3].start()
    distant[1].spread()
    distant[2].spread()

    @pl.when(jnp.logical_and(c == 1, z >= 4))
    def _():
        distant[3].start()

    native_late.spread()
    distant[3].spread()
    values = z_last(0)
    values = values + z_last(1)
    loads[5].wait()
    for column in range(4):
        position = jnp.full((8, NG), lax.rem(order[column] + 4 - 2 * b, 4), jnp.int32)
        value = values[3]
        for at in range(3):
            value = jnp.where(position == at, values[at], value)
        out_ref[pl.ds(column, 8, stride=4), :] = value

    for sem, rows in ((early_send, 896), (send_sem, 1016)):
        sent = send.at[:, pl.ds(0, rows)]
        pltpu.make_async_copy(sent, sent, sem).wait()


def local(left_bands, right_bands, sphere_index, right_order):
    table, trig = dft_tables()
    hbm = pl.BlockSpec(memory_space=pltpu.HBM)
    dma = pltpu.SemaphoreType.DMA
    result = pl.pallas_call(
        kernel,
        name="pair_sums",
        out_shape=pltpu.VMEM((32, NG), F32),
        in_specs=[hbm] * 6,
        out_specs=pl.BlockSpec(memory_space=pltpu.VMEM),
        scratch_shapes=[
            pltpu.VMEM((2, 2, 4, NG, NX), F32),
            pltpu.VMEM((2, 2, 2, NG, NX), F32),
            pltpu.VMEM((2, 2, NG, NX), F32),
            pltpu.VMEM((4, 4, 8, NG), jnp.int32),
            pltpu.VMEM((12 * NG, 2 * NG), BF16),
            pltpu.VMEM((8, NG), F32),
            pltpu.VMEM((NG, NG), jnp.int32),
            pltpu.VMEM((NG, NG), jnp.int32),
            pltpu.VMEM((NG, NG), jnp.int32),
            pltpu.VMEM((2, 2, NG, NG), F32),
            pltpu.VMEM((8, NG, NG), F32),
            pltpu.VMEM((2, AX * QUARTER, NG), F32),
            pltpu.VMEM((2, 2, PIECE, NG), F32),
            pltpu.VMEM((2, 4, PIECE, NG), F32),
            pltpu.VMEM((3, QUARTER, NG), F32),
            pltpu.VMEM((2, QUARTER, NG), F32),
            pltpu.VMEM((2, QUARTER, NG), F32),
            pltpu.SMEM((4,), jnp.int32),
            dma((5,)), dma, dma, dma, dma, dma((2, 2)), dma((4,)), dma((2,)),
            pltpu.SemaphoreType.REGULAR((4,)),
        ],
        compiler_params=pltpu.CompilerParams(collective_id=0, has_side_effects=True),
    )(
        right_order,
        left_bands.reshape(2, 4, NG, NX),
        right_bands.reshape(2, 2, NG, NX),
        sphere_index.reshape(4, 4, 8, NG),
        jnp.asarray(table),
        jnp.asarray(trig),
    )
    return result.reshape(2, 4, 4, NG)


def solution(mesh):
    placed = (P(None, "band", "grid", None, None), P(None, "band", "grid", None, None), P(), P())
    return jax.shard_map(
        local, mesh=mesh, in_specs=placed, out_specs=P(None, "band", None, "grid"), check_vma=False
    )
```

```python
import functools
import math

import jax
import jax.numpy as jnp
from jax import lax
from jax.experimental import pallas as pl
from jax.experimental.pallas import tpu as pltpu
from jax.sharding import PartitionSpec as P
import numpy as np

NG = 128
NX = 128
NGV = 16384
AX, AH, AZ, AC = 4, 2, 8, 2
SIDE = AH * AZ * AC
QUARTER = SIDE * 8
HALF = QUARTER // 2
PIECE = HALF // 2
PLACE = (0, 2, 1, 3)
Y_ROWS = (6 * NG, 8 * NG, 10 * NG)
MESH = pl.DeviceIdType.MESH
F32 = jnp.float32
BF16 = jnp.bfloat16


def split(value):
    high = value.astype(BF16)
    return high, (value - high.astype(F32)).astype(BF16)


def dft_tables():
    counter = np.arange(NG)
    angles = (counter[:, None] * counter[None, :] % NG) * (2.0 * math.pi / NG)
    cosine, sine = np.cos(angles), np.sin(angles)

    def halves(table):
        high = table.astype(np.float32).astype(BF16)
        low = (table - high.astype(np.float64)).astype(np.float32).astype(BF16)
        return high, low

    high, low = halves(np.block([[cosine, -sine], [sine, cosine]]))
    along_x = np.concatenate([high, high, low], axis=0)
    high, low = halves(np.block([[cosine, sine], [-sine, cosine]]))
    along_y = np.concatenate([high, low, high], axis=0)
    trig = np.zeros((8, NG), np.float32)
    trig[0], trig[1] = cosine[1], sine[1]
    return np.concatenate([along_x, along_y], axis=0), trig


def lanes(value, index):
    return jnp.take_along_axis(value, index, axis=1, mode="promise_in_bounds")


def kernel(
    order_ref, left_ref, right_ref, sphere_ref, table_ref, trig_ref, out_ref,
    lefts, rights, own_right, sphere, dft, trig,
    ky_t, val_t, kx_of, phase, acc, send, from_a, from_bc, from_all, x_sum, tiles,
    order, load_sem, early_send, pair_recv, y_recv, send_sem, native_recv, distant_recv, z_recv, known,
):
    g = lax.axis_index("grid")
    b = lax.axis_index("band")
    c = lax.rem(g, AC)
    j = lax.rem(g, SIDE)
    x = lax.div(g, SIDE)
    up = lax.rem(x + 1, AX)
    down = lax.rem(x + AX - 1, AX)
    across = lax.rem(x + 2, AX)

    loads = [
        pltpu.make_async_copy(right_ref, own_right, load_sem.at[0]),
        pltpu.make_async_copy(left_ref, lefts.at[c], load_sem.at[1]),
        pltpu.make_async_copy(trig_ref, trig, load_sem.at[4]),
        pltpu.make_async_copy(right_ref.at[:, c], rights.at[0, c], load_sem.at[2]),
        pltpu.make_async_copy(table_ref, dft, load_sem.at[2]),
        pltpu.make_async_copy(order_ref, order, load_sem.at[3]),
    ]
    sphere_loads = [
        pltpu.make_async_copy(sphere_ref.at[:, at], sphere.at[:, PLACE[at]], load_sem.at[4])
        for at in range(4)
    ]
    for load in loads[:1] + sphere_loads + loads[1:]:
        load.start()

    grid_up = up * SIDE + j
    grid_down = down * SIDE + j
    pair = g + 1 - 2 * c
    h = lax.rem(lax.div(g, SIDE // 2), AH)
    z = lax.rem(lax.div(g, AC), AZ)
    q = lax.div(z, 4) * 16 + h * 8 + lax.rem(z, 4) * AC + c
    opposite = g + SIDE // 2 - SIDE * h
    along_z = [(g + AC * (lax.rem(z + step, AZ) - z), b) for step in (1, AZ - 1, 2, AZ - 2)]
    close = [(pair, b), (g, 1 - b), (pair, 1 - b)]
    near = along_z[:2] + [(grid_up, b), (grid_down, b), (opposite, 1 - b)]
    barrier = pltpu.get_barrier_semaphore()

    def signal(sem, devices):
        for grid, band in devices:
            pl.semaphore_signal(sem, inc=1, device_id=(grid, band), device_id_type=MESH)

    signal(barrier, close)

    @pl.when(c == 1)
    def _():
        signal(barrier, near)

    def tell(step):
        others = near + [(g, 1 - b)] if step == 0 else along_z + near[2:4] + [(opposite, b)]

        @pl.when(c == 1)
        def _():
            signal(known.at[step], [(pair, b)] + others)

    def hear(step):
        pl.semaphore_wait(known.at[step], jnp.where(c == 1, 6 if step == 0 else 7, 1))

    def remote(source, target, sent, received, grid, band):
        return pltpu.make_async_remote_copy(
            src_ref=source, dst_ref=target, send_sem=sent, recv_sem=received,
            device_id=(grid, band), device_id_type=MESH,
        )

    to_other = [
        remote(own_right.at[:, m], rights.at[1, c], early_send, y_recv, g - c + m, 1 - b)
        for m in range(2)
    ]
    to_pair = [
        remote(lefts.at[c], lefts.at[c], early_send, pair_recv, pair, b),
        remote(own_right.at[:, 1 - c], rights.at[0, c], early_send, pair_recv, pair, b),
    ]
    loads[0].wait()
    pl.semaphore_wait(barrier, jnp.where(c == 1, len(close) + len(near), len(close)))
    for copy in to_other:
        copy.start()
    loads[1].wait()
    for copy in to_pair:
        copy.start()
    tell(0)

    both = send.at[0, pl.ds(0, 136)]
    pltpu.make_async_copy(both, both, load_sem.at[4]).wait()
    flipped = sphere[...].reshape(NG, NG).T
    ky_t[...] = (flipped >> 7) & 127
    val_t[...] = ((flipped >> 14) << 7) | (flipped & 127)
    rows = lax.broadcasted_iota(jnp.int32, (NG, NG), 0)

    def place(p, table):
        return jnp.where(ky_t[pl.ds(p, 1), :] == rows, val_t[pl.ds(p, 1), :], table)

    table = lax.fori_loop(0, NG, place, jnp.zeros((NG, NG), jnp.int32), unroll=8)
    kx_of[...] = table & 127
    kz = table >> 7
    cosine = jnp.broadcast_to(trig[0:1, :], (NG, NG))
    sine = jnp.broadcast_to(trig[1:2, :], (NG, NG))
    for core in range(2):
        angle = (kz * (g - c + core)) & 127
        phase[core, 0] = lanes(cosine, angle)
        phase[core, 1] = lanes(sine, angle)

    def along_rows(chunk, plane, half):
        right_real = rights[chunk, plane, 0]
        right_imag = rights[chunk, plane, 1]
        fields = []
        for n in (2 * half, 2 * half + 1):
            left_real = lefts[plane, 0, n]
            left_imag = lefts[plane, 1, n]
            fields.append(
                jnp.concatenate(
                    [
                        left_real * right_real + left_imag * right_imag,
                        left_real * right_imag - left_imag * right_real,
                    ],
                    axis=1,
                )
            )
        high, low = split(jnp.concatenate(fields, axis=0))
        moved = jnp.dot(
            jnp.concatenate([high, low, high], axis=1), dft[: 6 * NG, :], preferred_element_type=F32
        )
        columns = [
            jnp.concatenate([moved[start : start + NG, :NX], moved[start : start + NG, NX:]], axis=0)
            for start in (0, NG)
        ]
        return split(jnp.concatenate(columns, axis=1))

    def along_columns(rows):
        high, low = rows
        return jnp.dot(
            jnp.concatenate([dft[start : start + 2 * NG, :] for start in Y_ROWS], axis=1),
            jnp.concatenate([high, high, low], axis=0),
            preferred_element_type=F32,
        )

    def pick(plane, waves, half):
        index = kx_of[...]
        cosines, sines = phase[plane, 0], phase[plane, 1]
        picked = {}
        for at in range(2):
            real = lanes(waves[:NG, at * NX : (at + 1) * NX], index)
            imag = lanes(waves[NG:, at * NX : (at + 1) * NX], index)
            n = 2 * half + at
            picked[n] = real * cosines + imag * sines
            picked[n + 4] = imag * cosines - real * sines
        return picked

    def ship(chunk, channel, value):
        send[chunk, pl.ds(channel, NG, stride=8), :] = value.T

    def native_first(plane):
        for half in range(2):
            picked = pick(plane, along_columns(along_rows(0, plane, half)), half)
            for channel, value in picked.items():
                acc[channel] = value

    def native_second(plane):
        for half in range(2):
            picked = pick(plane, along_columns(along_rows(0, plane, half)), half)
            for channel, value in picked.items():
                ship(0, channel, acc[channel] + value)

    def distant_both():
        def total(half, waves):
            first, second = (pick(plane, waves[plane], half) for plane in range(2))
            for channel in first:
                ship(1, channel, first[channel] + second[channel])

        rows = [along_rows(1, plane, half) for half in range(2) for plane in range(2)]
        waves = [along_columns(value) for value in rows]
        total(0, waves[:2])
        total(1, waves[2:])

    both = send.at[:, pl.ds(0, 896)]
    pltpu.make_async_copy(both, both, load_sem.at[2]).wait()
    native_first(c)
    hear(0)
    tell(1)
    both = send.at[:, pl.ds(0, 640)]
    pltpu.make_async_copy(both, both, pair_recv).wait()
    native_second(1 - c)

    def part(chunk, quarter, late, way):
        start = pl.multiple_of(quarter * QUARTER + late * HALF + way * PIECE, PIECE)
        return send.at[chunk, pl.ds(start, PIECE)]

    def send_tiles(chunk, places):
        mine = pl.ds(pl.multiple_of(q * 8, 8), 8)
        for to in places:
            owner_z = to // 16 * 4 + to % 8 // AC
            theirs = pl.ds(to * 8, 8)
            owner = x * SIDE + (to % 16 // 8 * AZ + owner_z) * AC + to % AC

            @pl.when(q != to)
            def _(theirs=theirs, owner=owner):
                remote(
                    x_sum.at[chunk, theirs], tiles.at[chunk, mine],
                    send_sem, z_recv.at[chunk], owner, b,
                ).start()

        @pl.when(functools.reduce(jnp.logical_or, [q == to for to in places]))
        def _():
            tiles[chunk, mine] = x_sum[chunk, mine]

    class Relay:
        def __init__(self, late):
            self.late = late
            self.added = from_a.at[late]
            self.last = from_bc.at[late]
            routes = (
                (across, 0, self.added.at[0], 0, grid_up),
                (across, 1, self.added.at[1], 0, grid_down),
                (up, 1, self.last.at[0], 1, grid_up),
                (down, 0, self.last.at[1], 1, grid_down),
                (up, 0, self.last.at[2], 1, grid_up),
                (down, 1, self.last.at[3], 1, grid_down),
            )
            self.copies = [
                remote(
                    part(0, quarter, late, way), target, send_sem,
                    native_recv.at[late, number], to, b,
                )
                for quarter, way, target, number, to in routes
            ]

        def first(self):
            for copy in self.copies[:2]:
                copy.start()

        def direct(self):
            for copy in self.copies[2:4]:
                copy.start()

        def second(self):
            pltpu.make_async_copy(self.added, self.added, native_recv.at[self.late, 0]).wait()
            for way, quarter in enumerate((up, down)):
                ref = part(0, quarter, self.late, way)
                ref[...] = ref[...] + self.added[way]
                self.copies[4 + way].start()

        def spread(self):
            pltpu.make_async_copy(self.last, self.last, native_recv.at[self.late, 1]).wait()
            for way in range(2):
                x_sum[0, pl.ds(self.late * HALF + way * PIECE, PIECE)] = (
                    part(0, x, self.late, way)[...] + self.last[2 + way] + self.last[1 - way]
                )
            send_tiles(
                0,
                [
                    self.late * 16 + way * 8 + AC * at + core
                    for at in range(4)
                    for way in range(2)
                    for core in (1, 0)
                ],
            )

    class Direct:
        def __init__(self, number, first, count):
            self.places = range(first, first + count)
            self.rows = pl.ds(first * 8, count * 8)
            self.received = distant_recv.at[number]

        def of_quarter(self, quarter):
            start = pl.multiple_of(quarter * QUARTER + self.rows.start, 8)
            return send.at[1, pl.ds(start, self.rows.size)]

        def start(self):
            for owner_x in (0, 1, 3, 2):

                @pl.when(x != owner_x)
                def _(owner_x=owner_x):
                    number = lax.rem(x - owner_x + AX, AX) - 1
                    remote(
                        self.of_quarter(owner_x), from_all.at[number, self.rows],
                        send_sem, self.received, owner_x * SIDE + j, b,
                    ).start()

        def spread(self):
            arrived = from_all.at[:, self.rows]
            pltpu.make_async_copy(arrived, arrived, self.received).wait()
            x_sum[1, self.rows] = (
                self.of_quarter(x)[...]
                + from_all[1, self.rows]
                + (from_all[0, self.rows] + from_all[2, self.rows])
            )
            send_tiles(1, self.places)

    def z_wait(chunk):
        many = tiles.at[chunk, pl.ds(0, (SIDE - 1) * 8)]
        pltpu.make_async_copy(many, many, z_recv.at[chunk]).wait()

    own = sphere[x, lax.div(z, 4) * 2 + h, pl.ds(lax.rem(z, 4) * AC + c, 1), :]
    index = jnp.broadcast_to((own >> 7) & 127, (8, NG))
    factor = 1.0 / (NG * NG * NX) ** 0.5

    def z_last(chunk):
        z_wait(chunk)
        values = []
        for core in range(2):
            total = tiles[chunk, pl.ds(core * 8, 8)]
            for chip in range(1, SIDE // 2):
                total = total + tiles[chunk, pl.ds((2 * chip + core) * 8, 8)]
            values.append(lanes(total, index) * factor)
        return values

    native, native_late = Relay(0), Relay(1)
    distant = [
        Direct(number, first, count)
        for number, (first, count) in enumerate(((0, 2), (2, 6), (8, 8), (16, 16)))
    ]

    @pl.when(c == 0)
    def _():
        hear(1)

    native.first()
    native_late.first()
    native.direct()
    native_late.direct()

    @pl.when(c == 1)
    def _():
        hear(1)
        tell(2)
        native.second()
        native_late.second()

    pltpu.make_async_copy(rights.at[1], rights.at[1], y_recv).wait()
    @pl.when(c == 1)
    def _():
        hear(2)
        tell(3)

    distant_both()

    @pl.when(c == 0)
    def _():
        hear(2)

    distant[0].start()

    @pl.when(c == 0)
    def _():
        native.second()
        distant[1].start()
        distant[2].start()
        native_late.second()


    hear(3)
    native.spread()

    @pl.when(c == 1)
    def _():
        distant[1].start()
        distant[2].start()

    distant[0].spread()

    @pl.when(jnp.logical_or(c == 0, z < 4))
    def _():
        distant[3].start()
    distant[1].spread()
    distant[2].spread()

    @pl.when(jnp.logical_and(c == 1, z >= 4))
    def _():
        distant[3].start()

    native_late.spread()
    distant[3].spread()
    values = z_last(0)
    values = values + z_last(1)
    loads[5].wait()
    for column in range(4):
        position = jnp.full((8, NG), lax.rem(order[column] + 4 - 2 * b, 4), jnp.int32)
        value = values[3]
        for at in range(3):
            value = jnp.where(position == at, values[at], value)
        out_ref[pl.ds(column, 8, stride=4), :] = value

    for sem, rows in ((early_send, 896), (send_sem, 1016)):
        sent = send.at[:, pl.ds(0, rows)]
        pltpu.make_async_copy(sent, sent, sem).wait()


def local(left_bands, right_bands, sphere_index, right_order):
    table, trig = dft_tables()
    hbm = pl.BlockSpec(memory_space=pltpu.HBM)
    dma = pltpu.SemaphoreType.DMA
    result = pl.pallas_call(
        kernel,
        name="pair_sums",
        out_shape=pltpu.VMEM((32, NG), F32),
        in_specs=[hbm] * 6,
        out_specs=pl.BlockSpec(memory_space=pltpu.VMEM),
        scratch_shapes=[
            pltpu.VMEM((2, 2, 4, NG, NX), F32),
            pltpu.VMEM((2, 2, 2, NG, NX), F32),
            pltpu.VMEM((2, 2, NG, NX), F32),
            pltpu.VMEM((4, 4, 8, NG), jnp.int32),
            pltpu.VMEM((12 * NG, 2 * NG), BF16),
            pltpu.VMEM((8, NG), F32),
            pltpu.VMEM((NG, NG), jnp.int32),
            pltpu.VMEM((NG, NG), jnp.int32),
            pltpu.VMEM((NG, NG), jnp.int32),
            pltpu.VMEM((2, 2, NG, NG), F32),
            pltpu.VMEM((8, NG, NG), F32),
            pltpu.VMEM((2, AX * QUARTER, NG), F32),
            pltpu.VMEM((2, 2, PIECE, NG), F32),
            pltpu.VMEM((2, 4, PIECE, NG), F32),
            pltpu.VMEM((3, QUARTER, NG), F32),
            pltpu.VMEM((2, QUARTER, NG), F32),
            pltpu.VMEM((2, QUARTER, NG), F32),
            pltpu.SMEM((4,), jnp.int32),
            dma((5,)), dma, dma, dma, dma, dma((2, 2)), dma((4,)), dma((2,)),
            pltpu.SemaphoreType.REGULAR((4,)),
        ],
        compiler_params=pltpu.CompilerParams(collective_id=0, has_side_effects=True),
    )(
        right_order,
        left_bands.reshape(2, 4, NG, NX),
        right_bands.reshape(2, 2, NG, NX),
        sphere_index.reshape(4, 4, 8, NG),
        jnp.asarray(table),
        jnp.asarray(trig),
    )
    return result.reshape(2, 4, 4, NG)


def solution(mesh):
    placed = (P(None, "band", "grid", None, None), P(None, "band", "grid", None, None), P(), P())
    return jax.shard_map(
        local, mesh=mesh, in_specs=placed, out_specs=P(None, "band", None, "grid"), check_vma=False
    )
```
